128 devices in a mesh: dp: 32 (over y, x, z_hi), mp: 4 (over z_lo, core).
Axes of the slice: x: 4, y: 4, z: 4 (z_hi: 2, z_lo: 2; z = z_hi * 2 + z_lo), core: 2. Of those that a mesh axis runs over, the one named last changes fastest.
Arguments:
- page_pool: bfloat16 [2048, 128, 512], P('dp'), may hold values from -6 to 6
- move_count: int32 [32, 32], P('dp'), may hold values from 0 to 2, as said below
- send_slots: int32 [1024, 2], P('dp'), may hold values from 0 to 63, as said below
- page_table: int32 [2048, 16], P('dp'), may hold values from 0 to 127, as said below
- history_len: int32 [2048], P('dp'), may hold values from 1 to 2048, as said below
- queries: bfloat16 [2048, 8, 256], P('dp', 'mp'), may hold values from -6 to 6
- new_entry: bfloat16 [2048, 512], P('dp'), may hold values from -6 to 6
- residual: bfloat16 [2048, 2048], P('dp'), may hold values from -30 to 30
- out_proj: bfloat16 [2048, 2048], P('mp'), may hold values from -0.125 to 0.125
- ffn_gain: float32 [2048], replicated, may hold values from -0.5 to 0.5
- gate_proj: bfloat16 [2048, 16384], P(None, ('dp', 'mp')), may hold values from -0.125 to 0.125
- up_proj: bfloat16 [2048, 16384], P(None, ('dp', 'mp')), may hold values from -0.125 to 0.125
- down_proj: bfloat16 [16384, 2048], P(('dp', 'mp')), may hold values from -0.046875 to 0.046875
Outputs:
- arrived: bfloat16 [2048, 128, 512], P('dp')
- layer_out: bfloat16 [2048, 2048], P('dp')
The draws below stay inside these ranges and needn't reach their ends.
Inputs may be any that keep to these rules, and one draw needn't show every extreme that they name: `move_count`: zero on the diagonal; in every draw one device receives exactly 2 pages from every other device. `send_slots`: only the first move_count[s, d] entries of row s * 32 + d are sent. `page_table`: for a game of device d, an entry e >= 64 equals 64 + s * 2 + c with c < move_count[s, d]. `history_len`: some game of some device reaches 2048 in every draw.
All inputs are finite; a program needn't handle non-finite values.
Results may differ from the reference program's by a relative error of at most 0.0075.
Values may be sent and summed in bfloat16 or wider, within the bound.
No kernel may reach another device: no remote copies, remote signals or barrier semaphores. Data moves between devices by JAX's collectives and lax.ppermute only.
A program may use at most 128 MiB of HBM per device.

```python
import math
import jax
import jax.numpy as jnp
from jax import lax

D = 2048
HEADS = 8
HD = 256
FF = 16384
PAGE = 128
MAXP = 16
CAP = 2
GAMES_DEV = 64
POOL = 64
POOL_ALL = 2048
GAMES = 2048
N_DP = 32


def plan_counts(key):
    base = jax.random.fold_in(key, 11)
    first, second = jax.random.split(base)
    counts = jax.random.randint(first, (N_DP, N_DP), 0, CAP + 1)
    busiest = jax.random.randint(second, (), 0, N_DP)
    places = jnp.arange(N_DP)
    counts = jnp.where(places[None, :] == busiest, CAP, counts)
    counts = jnp.where(places[:, None] == places[None, :], 0, counts)
    return counts.astype(jnp.int32)


def draw_move_count(key, part):
    return plan_counts(key)


def draw_send_slots(key, part):
    return jax.random.randint(jax.random.fold_in(key, 12), (N_DP * N_DP, CAP), 0, POOL).astype(jnp.int32)


def draw_page_table(key, part):
    counts = plan_counts(key)
    first, second = jax.random.split(jax.random.fold_in(key, 13))
    picks = jax.random.randint(first, (GAMES, MAXP), 0, POOL + N_DP * CAP)
    resident = jax.random.randint(second, (GAMES, MAXP), 0, POOL)
    owner = (jnp.arange(GAMES) // GAMES_DEV)[:, None]
    source = jnp.clip((picks - POOL) // CAP, 0, N_DP - 1)
    column = (picks - POOL) % CAP
    usable = (picks >= POOL) & (column < counts[source, owner])
    table = jnp.where(picks < POOL, picks, jnp.where(usable, picks, resident))
    return table.astype(jnp.int32)


def draw_history_len(key, part):
    first, second, third = jax.random.split(jax.random.fold_in(key, 14), 3)
    longest = MAXP * PAGE
    levels = longest.bit_length() - 1
    powers = jax.random.randint(first, (GAMES,), 0, levels + 1)
    ceiling = jnp.minimum(jnp.left_shift(jnp.ones((GAMES,), jnp.int32), powers.astype(jnp.int32)), longest)
    lengths = jax.random.randint(second, (GAMES,), 1, ceiling + 1)
    chosen = jax.random.randint(third, (), 0, GAMES)
    lengths = jnp.where(jnp.arange(GAMES) == chosen, longest, lengths)
    return lengths.astype(jnp.int32)


def draw_page_pool(key, part):
    noise = jax.random.fold_in(key, 31)
    shape = (POOL_ALL, PAGE, 2 * HD)
    values = jax.random.truncated_normal(noise, -6.0, 6.0, shape, jnp.float32)
    return values.astype(jnp.bfloat16)


def draw_queries(key, part):
    first = jax.random.fold_in(jax.random.fold_in(key, 41), 0)
    shape = (GAMES, HEADS, HD)
    values = jax.random.truncated_normal(first, -6.0, 6.0, shape, jnp.float32)
    return values.astype(jnp.bfloat16)


def draw_residual(key, part):
    first = jax.random.fold_in(jax.random.fold_in(key, 51), 0)
    values = jax.random.truncated_normal(first, -6.0, 6.0, (GAMES, D), jnp.float32)
    return values.astype(jnp.bfloat16)


def steps_of(own_key, extent, pieces, low, top_value):
    gain = 1.0
    for axis_at, parts in pieces:
        steps = jax.random.uniform(jax.random.fold_in(jax.random.fold_in(own_key, 6), axis_at), (parts,), jnp.float32, low / len(pieces), top_value / len(pieces))
        gain = gain * jnp.repeat(jnp.exp(steps), extent[axis_at] // parts).reshape((-1,) + (1,) * (len(extent) - 1 - axis_at))
    return gain


def centred(stream_key, extent, scale, bound, cuts=(), kind=jnp.bfloat16):
    entries = jax.random.normal(stream_key, extent, jnp.float32) * scale
    if len(cuts) > 0:
        entries = steps_of(stream_key, extent, cuts, -0.22, 0.18) * entries
    return jnp.clip(entries, min=-bound, max=bound).astype(kind)


def setup_inputs(seed: int = 0) -> dict:
    key_list = jax.random.split(jax.random.key(seed), 14)
    page_pool = draw_page_pool(jax.random.fold_in(key_list[13], 71), 0)
    move_count = draw_move_count(jax.random.fold_in(key_list[13], 71), 0)
    send_slots = draw_send_slots(jax.random.fold_in(key_list[13], 71), 0)
    page_table = draw_page_table(jax.random.fold_in(key_list[13], 71), 0)
    history_len = draw_history_len(jax.random.fold_in(key_list[13], 71), 0)
    queries = draw_queries(jax.random.fold_in(key_list[13], 71), 0)
    new_entry = centred(key_list[6], (GAMES, 2 * HD), 1.0, 6.0, ((0, 32),))
    residual = draw_residual(jax.random.fold_in(key_list[13], 71), 0)
    out_proj = centred(key_list[8], (HEADS * HD, D), (HEADS * HD) ** -0.5, 0.125, ((0, 4),))
    ffn_gain = jnp.clip(jax.random.uniform(key_list[9], (D,), jnp.float32, -0.5, 0.5), -0.5, 0.5)
    gate_proj = centred(key_list[10], (D, FF), D ** -0.5, 0.125, ((1, 128),))
    up_proj = centred(key_list[11], (D, FF), D ** -0.5, 0.125, ((1, 128),))
    down_proj = centred(key_list[12], (FF, D), FF ** -0.5, 0.046875, ((0, 128),))
    return dict(page_pool=page_pool, move_count=move_count, send_slots=send_slots, page_table=page_table, history_len=history_len, queries=queries, new_entry=new_entry, residual=residual, out_proj=out_proj, ffn_gain=ffn_gain, gate_proj=gate_proj, up_proj=up_proj, down_proj=down_proj)


def attend_block(query_blk, page_rows, length_blk, entry_blk):
    keys = page_rows[:, :, :HD].astype(jnp.float32)
    values = page_rows[:, :, HD:].astype(jnp.float32)
    query_f = query_blk.astype(jnp.float32)
    entry_f = entry_blk.astype(jnp.float32)
    factor = 1.0 / math.sqrt(HD)
    scores = jnp.einsum('bhd,btd->bht', query_f, keys) * factor
    own = jnp.einsum('bhd,bd->bh', query_f, entry_f[:, :HD]) * factor
    places = jnp.arange(page_rows.shape[1], dtype=jnp.int32)
    valid = places[None, None, :] < length_blk[:, None, None]
    scores = jnp.where(valid, scores, jnp.float32(-1e+30))
    biggest = jnp.maximum(lax.optimization_barrier(jnp.max(scores, axis=-1)), own)
    probs = jnp.where(valid, jnp.exp(scores - biggest[..., None]), jnp.float32(0.0))
    prob_own = jnp.exp(own - biggest)
    denom = lax.optimization_barrier(jnp.sum(probs, axis=-1)) + prob_own
    weights = (probs / denom[..., None]).astype(jnp.bfloat16)
    weight_own = (prob_own / denom).astype(jnp.bfloat16)
    weights = lax.optimization_barrier(weights).astype(jnp.float32)
    weight_own = lax.optimization_barrier(weight_own).astype(jnp.float32)
    result = jnp.einsum('bht,btd->bhd', weights, values)
    result = result + weight_own[..., None] * entry_f[:, None, HD:]
    return result.astype(jnp.bfloat16)

def reference(page_pool, move_count, send_slots, page_table, history_len, queries, new_entry, residual, out_proj, ffn_gain, gate_proj, up_proj, down_proj):
    slots = send_slots.reshape(N_DP, N_DP, CAP)
    owners = jnp.arange(N_DP, dtype=jnp.int32)[:, None, None] * POOL + slots.astype(jnp.int32)
    live = jnp.arange(CAP, dtype=jnp.int32)[None, None, :] < move_count[:, :, None]
    owners = jnp.transpose(owners, (1, 0, 2)).reshape(-1)
    live = jnp.transpose(live, (1, 0, 2)).reshape(-1)
    arrived = jnp.where(live[:, None, None], page_pool[owners], jnp.zeros((), jnp.bfloat16))
    block = math.gcd(GAMES_DEV, 8)

    def one_device(index):
        own_pages = lax.dynamic_slice_in_dim(page_pool, (index * POOL).astype(jnp.int32), POOL, 0)
        got_pages = lax.dynamic_slice_in_dim(arrived, (index * N_DP * CAP).astype(jnp.int32), N_DP * CAP, 0)
        every_page = jnp.concatenate([own_pages, got_pages], axis=0)
        first = (index * GAMES_DEV).astype(jnp.int32)
        table = lax.dynamic_slice_in_dim(page_table, first, GAMES_DEV, 0).reshape(-1, block, MAXP)
        lengths = lax.dynamic_slice_in_dim(history_len, first, GAMES_DEV, 0).reshape(-1, block)
        query_dev = lax.dynamic_slice_in_dim(queries, first, GAMES_DEV, 0).reshape(-1, block, HEADS, HD)
        entry_dev = lax.dynamic_slice_in_dim(new_entry, first, GAMES_DEV, 0).reshape(-1, block, 2 * HD)

        def one_block(items):
            table_blk, length_blk, query_blk, entry_blk = items
            page_rows = every_page[table_blk].reshape(block, MAXP * PAGE, 2 * HD)
            return attend_block(query_blk, page_rows, length_blk, entry_blk)
        result = lax.map(one_block, (table, lengths, query_dev, entry_dev))
        return result.reshape(GAMES_DEV, HEADS * HD)
    attended = lax.map(one_device, jnp.arange(N_DP, dtype=jnp.int32)).reshape(GAMES, HEADS * HD)
    stream_in = residual.astype(jnp.float32) + jnp.dot(attended, out_proj, preferred_element_type=jnp.float32)
    scale_row = lax.rsqrt(lax.optimization_barrier(jnp.mean(stream_in * stream_in, axis=-1, keepdims=True)) + 1e-06)
    normed = (stream_in * scale_row * (1.0 + ffn_gain)).astype(jnp.bfloat16)
    gate = jnp.dot(normed, gate_proj, preferred_element_type=jnp.float32)
    up_val = jnp.dot(normed, up_proj, preferred_element_type=jnp.float32)
    hidden = (jax.nn.gelu(gate, approximate=True) * up_val).astype(jnp.bfloat16)
    mixed = jnp.dot(hidden, down_proj, preferred_element_type=jnp.float32)
    layer_out = (stream_in + mixed).astype(jnp.bfloat16)
    return (arrived, layer_out)
```

```python
import jax
import jax.numpy as jnp
from jax import lax
from jax.experimental import pallas as pl
from jax.experimental.pallas import tpu as pltpu
from jax.sharding import PartitionSpec as P

NEG = -1e30
BF = jnp.bfloat16
F32 = jnp.float32
VLIM = 60 * 1024 * 1024


def params(**kw):
    return pltpu.CompilerParams(vmem_limit_bytes=VLIM, **kw)


def cost(us):
    return pl.CostEstimate(flops=int(us * 4e8), bytes_accessed=int(us * 2e6), transcendentals=0)


def outgoing_kernel(half_ref, slot_ref, count_ref, pool_ref, out_ref, sems):
    pages, rows, _ = out_ref.shape
    caps = pages // count_ref.shape[0]
    first = pl.multiple_of(half_ref[0] * rows, rows)

    def copy(i):
        src = pool_ref.at[slot_ref[i], pl.ds(first, rows), :]
        return pltpu.make_async_copy(src, out_ref.at[i], sems.at[i])

    for i in range(pages):
        copy(i).start()
    for i in range(pages):
        copy(i).wait()

        @pl.when(i % caps >= count_ref[i // caps])
        def _():
            out_ref[i] = jnp.zeros(out_ref.shape[1:], out_ref.dtype)


def outgoing_pages(half, slots, counts, pool):
    pages = slots.shape[0]
    rows = pool.shape[1] // 2
    return pl.pallas_call(
        outgoing_kernel,
        grid_spec=pltpu.PrefetchScalarGridSpec(
            num_scalar_prefetch=3,
            grid=(1,),
            in_specs=[pl.BlockSpec(memory_space=pl.ANY)],
            out_specs=pl.BlockSpec((pages, rows, pool.shape[2]), lambda i, *_: (0, 0, 0)),
            scratch_shapes=[pltpu.SemaphoreType.DMA((pages,))],
        ),
        out_shape=jax.ShapeDtypeStruct((pages, rows, pool.shape[2]), pool.dtype),
        compiler_params=params(),
        cost_estimate=cost(3),
        name="outgoing",
    )(half, slots, counts, pool)


def attend_kernel(
    half_ref, qa_ref, qb_ref, entry_ref, tab_ref, len_ref, pool_ref, got_ref,
    keep_ref, send_ref, acc, stat, full, part,
):
    i = pl.program_id(0)
    steps = pl.num_programs(0)
    pages, rows, width = pool_ref.shape
    hd = width // 2
    mine = qa_ref.shape[0]
    lanes = 2 * mine
    games = entry_ref.shape[0]
    q = jnp.concatenate([qa_ref[...], qb_ref[...]], axis=0)

    @pl.when(i == 0)
    def _():
        entries = full.shape[0]
        page_id = lax.broadcasted_iota(jnp.int32, (entries, lanes), 0)
        whole = jnp.zeros((entries, lanes), F32)
        rest = jnp.zeros((entries, lanes), jnp.int32)
        for j in range(tab_ref.shape[0]):
            hit = page_id == tab_ref[j : j + 1, :]
            kept = len_ref[...] - j * 2 * rows
            whole += jnp.where(hit & (kept >= 2 * rows), 1.0, 0.0)
            rest += jnp.where(hit & (kept > 0) & (kept < 2 * rows), kept, 0)
        full[...] = whole
        part[...] = rest - half_ref[0] * rows
        s = lax.dot_general(
            entry_ref[:, :hd], q, (((1,), (1,)), ((), ())), preferred_element_type=F32
        )
        game = lax.broadcasted_iota(jnp.int32, (games, lanes), 0)
        lane = lax.broadcasted_iota(jnp.int32, (games, lanes), 1)
        own = (lane < mine) & (lax.rem(lane, games) == game)
        top = jnp.max(jnp.where(own, s, NEG), axis=0, keepdims=True)
        p = jnp.where(own, 1.0, 0.0)
        stat[0:1, :] = top
        stat[1:2, :] = jnp.sum(p, axis=0, keepdims=True)
        acc[...] = lax.dot_general(
            entry_ref[:, hd:], p.astype(BF), (((0,), (0,)), ((), ())), preferred_element_type=F32
        )

    def chunk(block):
        keys = block[:, :, :hd].reshape(pages * rows, hd)
        values = block[:, :, hd:].reshape(pages * rows, hd)
        s = lax.dot_general(keys, q, (((1,), (1,)), ((), ())), preferred_element_type=F32)
        spot = lax.broadcasted_iota(jnp.int32, (rows, lanes), 0)
        old = stat[0:1, :]
        top = old
        counts = []
        masked = []
        base = i * pages
        for j in range(pages):
            c = full[pl.ds(base + j, 1), :] + jnp.where(
                spot < part[pl.ds(base + j, 1), :], 1.0, 0.0
            )
            sj = jnp.where(c > 0.0, s[j * rows : (j + 1) * rows, :], NEG)
            top = jnp.maximum(top, jnp.max(sj, axis=0, keepdims=True))
            counts.append(c)
            masked.append(sj)
        shrink = jnp.exp(old - top)
        total = stat[1:2, :] * shrink
        probs = []
        for j in range(pages):
            p = jnp.exp(masked[j] - top) * counts[j]
            total += jnp.sum(p, axis=0, keepdims=True)
            probs.append(p.astype(BF))
        p = jnp.concatenate(probs, axis=0)
        stat[0:1, :] = top
        stat[1:2, :] = total
        acc[...] = acc[...] * shrink + lax.dot_general(
            values, p, (((0,), (0,)), ((), ())), preferred_element_type=F32
        )

    @pl.when(i < steps // 2)
    def _():
        chunk(pool_ref)

    @pl.when(i >= steps // 2)
    def _():
        chunk(got_ref)

    @pl.when(i == steps - 1)
    def _():
        for k, out in enumerate((keep_ref, send_ref)):
            out[:hd, :] = acc[:, k * mine : (k + 1) * mine]
            out[hd : hd + 8, :] = stat[:, k * mine : (k + 1) * mine]


def attend(half, q_mine, q_peer, entry, table, lengths, pool, got):
    slots, rows, width = got.shape
    mine, hd = q_mine.shape
    block = 8
    half_steps = slots // block
    whole = lambda shape: pl.BlockSpec(shape, lambda i, *_: (0,) * len(shape))
    out = jax.ShapeDtypeStruct((hd + 8, mine), F32)
    return pl.pallas_call(
        attend_kernel,
        grid_spec=pltpu.PrefetchScalarGridSpec(
            num_scalar_prefetch=1,
            grid=(2 * half_steps,),
            in_specs=[
                whole(q_mine.shape),
                whole(q_peer.shape),
                whole(entry.shape),
                whole(table.shape),
                whole(lengths.shape),
                pl.BlockSpec(
                    (block, rows, width), lambda i, h: (jnp.minimum(i, half_steps - 1), h[0], 0)
                ),
                pl.BlockSpec(
                    (block, rows, width), lambda i, h: (jnp.maximum(i - half_steps, 0), 0, 0)
                ),
            ],
            out_specs=[whole(out.shape), whole(out.shape)],
            scratch_shapes=[
                pltpu.VMEM((hd, 2 * mine), F32),
                pltpu.VMEM((8, 2 * mine), F32),
                pltpu.VMEM((2 * slots, 2 * mine), F32),
                pltpu.VMEM((2 * slots, 2 * mine), jnp.int32),
            ],
        ),
        out_shape=[out, out],
        compiler_params=params(),
        cost_estimate=cost(8),
        name="attend",
    )(half, q_mine, q_peer, entry, table, lengths, pool, got)


def project_kernel(mine_ref, a_ref, b_ref, w_ref, keep_ref, send_ref, scratch):
    hd = a_ref.shape[0] - 8
    ma, mb = a_ref[hd : hd + 1, :], b_ref[hd : hd + 1, :]
    top = jnp.maximum(ma, mb)
    wa, wb = jnp.exp(ma - top), jnp.exp(mb - top)
    den = a_ref[hd + 1 : hd + 2, :] * wa + b_ref[hd + 1 : hd + 2, :] * wb
    att = (a_ref[:hd, :] * wa + b_ref[:hd, :] * wb) / den
    att = att.T.astype(BF)
    games = scratch.shape[0]
    out = jnp.zeros(scratch.shape, F32)
    for h in range(att.shape[0] // games):
        out += jnp.dot(
            att[h * games : (h + 1) * games, :],
            w_ref[h * hd : (h + 1) * hd, :],
            preferred_element_type=F32,
        )
    scratch[...] = out
    rows = keep_ref.shape[1]
    m = mine_ref[0]
    core = lax.rem(m, 2)
    side = m // 2
    for ref, c in ((keep_ref, core), (send_ref, 1 - core)):
        for k, z in enumerate((side, 1 - side)):
            first = pl.multiple_of((z * 2 + c) * rows, rows)
            ref[k] = scratch[pl.ds(first, rows), :]


def project(mine, a, b, w, games):
    rows = games // 4
    whole = lambda shape: pl.BlockSpec(shape, lambda i, *_: (0,) * len(shape))
    out = jax.ShapeDtypeStruct((2, rows, w.shape[1]), F32)
    return pl.pallas_call(
        project_kernel,
        grid_spec=pltpu.PrefetchScalarGridSpec(
            num_scalar_prefetch=1,
            grid=(1,),
            in_specs=[whole(a.shape), whole(b.shape), whole(w.shape)],
            out_specs=[whole(out.shape), whole(out.shape)],
            scratch_shapes=[pltpu.VMEM((games, w.shape[1]), F32)],
        ),
        out_shape=[out, out],
        compiler_params=params(),
        cost_estimate=cost(3),
        name="project",
    )(mine, a, b, w)


def norm_kernel(mine_ref, keep_ref, got_ref, side_ref, res_ref, gain_ref, copies_ref, stream_ref):
    stream = res_ref[...].astype(F32) + ((keep_ref[0] + got_ref[0]) + side_ref[...])
    scale = lax.rsqrt(jnp.mean(stream * stream, axis=-1, keepdims=True) + 1e-06)
    normed = (stream * scale * (1.0 + gain_ref[...])).astype(BF)
    stream_ref[...] = stream
    for k in range(copies_ref.shape[0]):
        copies_ref[k] = normed


def norm(mine, keep, got, side, residual, gain, peers):
    _, rows, d = keep.shape
    whole = lambda shape: pl.BlockSpec(shape, lambda i, *_: (0,) * len(shape))
    outs = [
        jax.ShapeDtypeStruct((peers, rows, d), BF),
        jax.ShapeDtypeStruct((rows, d), F32),
    ]
    return pl.pallas_call(
        norm_kernel,
        grid_spec=pltpu.PrefetchScalarGridSpec(
            num_scalar_prefetch=1,
            grid=(1,),
            in_specs=[
                pl.BlockSpec((1, rows, d), lambda i, *_: (0, 0, 0)),
                pl.BlockSpec((1, rows, d), lambda i, *_: (0, 0, 0)),
                whole(side.shape),
                pl.BlockSpec((rows, d), lambda i, m: (m[0], 0)),
                whole(gain.shape),
            ],
            out_specs=[whole(o.shape) for o in outs],
        ),
        out_shape=outs,
        compiler_params=params(),
        cost_estimate=cost(2),
        name="norm",
    )(mine, keep, got, side, residual, gain)


def ffn_kernel(*refs):
    n = (len(refs) - 7) // 3
    x_ref = refs[0]
    w = [refs[1 + 3 * b : 4 + 3 * b] for b in range(n)]
    out_ref, x, gu, down, hid, sem_x, sem_w = refs[1 + 3 * n :]
    unit = gu.shape[2] // 2

    def copies(b):
        g, u, d = w[b]
        return (
            pltpu.make_async_copy(g, gu.at[b, :, pl.ds(0, unit)], sem_w.at[3 * b]),
            pltpu.make_async_copy(u, gu.at[b, :, pl.ds(unit, unit)], sem_w.at[3 * b + 1]),
            pltpu.make_async_copy(d, down.at[pl.ds(b * unit, unit), :], sem_w.at[3 * b + 2]),
        )

    load_x = pltpu.make_async_copy(x_ref, x, sem_x)
    load_x.start()
    for b in range(n):
        for c in copies(b):
            c.start()
    load_x.wait()
    for b in range(n):
        for c in copies(b)[:2]:
            c.wait()
        both = jnp.dot(x[...], gu[b], preferred_element_type=F32)
        gate = both[:, :unit]
        hid[:, b * unit : (b + 1) * unit] = (
            jax.nn.gelu(gate, approximate=True) * both[:, unit:]
        ).astype(BF)
    for b in range(n):
        copies(b)[2].wait()
    cols = 256

    @pl.loop(0, out_ref.shape[1] // cols)
    def _(k):
        at = pl.ds(pl.multiple_of(k * cols, cols), cols)
        out_ref[:, at] = jnp.dot(hid[...], down[:, at], preferred_element_type=F32).astype(BF)


def ffn(x, weights):
    n = len(weights)
    rows, d = x.shape
    unit = weights[0][0].shape[1]
    any_spec = pl.BlockSpec(memory_space=pl.ANY)
    return pl.pallas_call(
        ffn_kernel,
        in_specs=[any_spec] * (1 + 3 * n),
        out_specs=pl.BlockSpec(memory_space=pltpu.VMEM),
        out_shape=jax.ShapeDtypeStruct((rows, d), BF),
        scratch_shapes=[
            pltpu.VMEM((rows, d), BF),
            pltpu.VMEM((n, d, 2 * unit), BF),
            pltpu.VMEM((n * unit, d), BF),
            pltpu.VMEM((rows, n * unit), BF),
            pltpu.SemaphoreType.DMA,
            pltpu.SemaphoreType.DMA((3 * n,)),
        ],
        compiler_params=params(),
        cost_estimate=cost(8),
        name="ffn",
    )(x, *[a for block in weights for a in block])


def finish_kernel(parts_ref, stream_ref, out_ref):
    total = parts_ref[0].astype(F32)
    for k in range(1, parts_ref.shape[0]):
        total += parts_ref[k].astype(F32)
    out_ref[...] = (stream_ref[...] + total).astype(BF)


def finish(parts, stream):
    return pl.pallas_call(
        finish_kernel,
        out_shape=jax.ShapeDtypeStruct(stream.shape, BF),
        compiler_params=params(),
        cost_estimate=cost(2),
        name="finish",
    )(parts, stream)


def assemble_kernel(half_ref, mine_ref, peer_ref, out_ref):
    rows = mine_ref.shape[1]
    for ref, h in ((mine_ref, half_ref[0]), (peer_ref, 1 - half_ref[0])):
        out_ref[:, pl.ds(pl.multiple_of(h * rows, rows), rows), :] = ref[...]


def assemble(half, mine, peer):
    pages, rows, width = mine.shape
    block = 8
    spec = pl.BlockSpec((block, rows, width), lambda i, *_: (i, 0, 0))
    return pl.pallas_call(
        assemble_kernel,
        grid_spec=pltpu.PrefetchScalarGridSpec(
            num_scalar_prefetch=1,
            grid=(pages // block,),
            in_specs=[spec, spec],
            out_specs=pl.BlockSpec((block, 2 * rows, width), lambda i, *_: (i, 0, 0)),
        ),
        out_shape=jax.ShapeDtypeStruct((pages, 2 * rows, width), mine.dtype),
        compiler_params=params(),
        cost_estimate=cost(6),
        name="assemble",
    )(half, mine, peer)


def local(
    page_pool, move_count, send_slots, page_table, history_len, queries, new_entry, residual,
    out_proj, ffn_gain, gate_proj, up_proj, down_proj,
):
    axes = ("dp", "mp")
    n_dp, n_mp = lax.axis_size("dp"), lax.axis_size("mp")
    devices = n_dp * n_mp
    games, heads, hd = queries.shape
    page_len, width = page_pool.shape[1:]
    mine = lax.axis_index("mp").reshape(1)
    half = mine % 2
    swap = lambda bit: [(k, k ^ bit) for k in range(devices)]
    core, side, across = swap(1), swap(2), swap(8)
    send = lambda a, pairs: lax.ppermute(a, axes, pairs)

    out_pages = outgoing_pages(half, send_slots.reshape(-1), move_count.reshape(-1), page_pool)
    got = lax.all_to_all(
        out_pages.reshape(n_dp, -1, page_len // 2, width), "dp", 0, 0, tiled=True
    ).reshape(out_pages.shape)

    q_mine = (queries.transpose(1, 0, 2) * jnp.asarray(hd**-0.5, BF)).reshape(heads * games, hd)
    q_peer = send(q_mine, core)
    copies = 2 * heads
    table = jnp.tile(page_table.T, (1, copies))
    lengths = jnp.tile(history_len[None, :], (1, copies))

    weights = (gate_proj, up_proj, down_proj)
    w_core = tuple(send(a, core) for a in weights)
    late, got = lax.optimization_barrier((weights, got))
    w_far = tuple(send(a, across) for a in late)
    w_far_core = tuple(send(a, core) for a in w_far)

    keep, give = attend(half, q_mine, q_peer, new_entry, table, lengths, page_pool, got)
    other = send(give, core)
    got_peer = send(got, core)
    hold, pass_on = project(mine, keep, other, out_proj, games)
    hold_got = send(pass_on, core)
    side_got = send(hold[1] + hold_got[1], side)
    arrived = assemble(half, got, got_peer)

    groups = [
        [k for k in range(devices) if k % 2 == c and (k >> 3) % 2 == x]
        for x in range(2)
        for c in range(2)
    ]
    peers = len(groups[0])
    spread, stream = norm(
        mine, hold, hold_got, side_got, residual, ffn_gain.reshape(1, -1), peers
    )
    rows, d = stream.shape
    x = lax.all_to_all(spread, axes, 0, 0, tiled=True, axis_index_groups=groups)
    parts = ffn(x.reshape(peers * rows, d), [weights, w_core, w_far, w_far_core])
    back = lax.all_to_all(
        parts.reshape(peers, rows, d), axes, 0, 0, tiled=True, axis_index_groups=groups
    )
    quarter = finish(back, stream)
    layer_out = lax.all_gather(quarter, "mp", axis=0, tiled=True)
    return arrived, layer_out


def solution(mesh):
    in_specs = (
        P("dp", None, None),
        P("dp", None),
        P("dp", None),
        P("dp", None),
        P("dp"),
        P("dp", "mp", None),
        P("dp", None),
        P("dp", None),
        P("mp", None),
        P(),
        P(None, ("dp", "mp")),
        P(None, ("dp", "mp")),
        P(("dp", "mp"), None),
    )
    out_specs = (P("dp", None, None), P("dp", None))
    return jax.shard_map(local, mesh=mesh, in_specs=in_specs, out_specs=out_specs, check_vma=False)
```

```python
import jax
import jax.numpy as jnp
from jax import lax
from jax.experimental import pallas as pl
from jax.experimental.pallas import tpu as pltpu
from jax.sharding import PartitionSpec as P


NEG = -1e30
BF = jnp.bfloat16
F32 = jnp.float32
VLIM = 60 * 1024 * 1024


def params(**kw):
    return pltpu.CompilerParams(vmem_limit_bytes=VLIM, **kw)


def cost(us):
    return pl.CostEstimate(flops=int(us * 4e8), bytes_accessed=int(us * 2e6), transcendentals=0)


def outgoing_kernel(half_ref, slot_ref, count_ref, pool_ref, out_ref, sems):
    pages, rows, _ = out_ref.shape
    caps = pages // count_ref.shape[0]
    first = pl.multiple_of(half_ref[0] * rows, rows)

    def copy(i):
        src = pool_ref.at[slot_ref[i], pl.ds(first, rows), :]
        return pltpu.make_async_copy(src, out_ref.at[i], sems.at[i])

    copies = [copy(i) for i in range(pages)]
    for c in copies:
        c.start()
    for i, c in enumerate(copies):
        c.wait()

        @pl.when(i % caps >= count_ref[i // caps])
        def _():
            out_ref[i] = jnp.zeros(out_ref.shape[1:], out_ref.dtype)


def outgoing_pages(half, slots, counts, pool):
    pages = slots.shape[0]
    rows = pool.shape[1] // 2
    return pl.pallas_call(
        outgoing_kernel,
        grid_spec=pltpu.PrefetchScalarGridSpec(
            num_scalar_prefetch=3,
            grid=(1,),
            in_specs=[pl.BlockSpec(memory_space=pl.ANY)],
            out_specs=pl.BlockSpec((pages, rows, pool.shape[2]), lambda i, *_: (0, 0, 0)),
            scratch_shapes=[pltpu.SemaphoreType.DMA((pages,))],
        ),
        out_shape=jax.ShapeDtypeStruct((pages, rows, pool.shape[2]), pool.dtype),
        compiler_params=params(),
        cost_estimate=cost(3),
        name="outgoing",
    )(half, slots, counts, pool)


def chunk_step(block, base, qt, full, part, acc, stat):
    pages, rows, width = block.shape
    hd = width // 2
    lanes = qt.shape[1]
    keys = block[:, :, :hd].reshape(pages * rows, hd)
    values = block[:, :, hd:].reshape(pages * rows, hd)
    s = jnp.dot(keys, qt[...], preferred_element_type=F32)
    spot = lax.broadcasted_iota(jnp.int32, (rows, lanes), 0)
    old = stat[0:1, :]
    tops = jnp.full((8, lanes), NEG, F32)
    counts = []
    masked = []
    for j in range(pages):
        c = full[pl.ds(base + j, 1), :] + jnp.where(
            spot < part[pl.ds(base + j, 1), :], 1.0, 0.0
        )
        sj = jnp.where(c > 0.0, s[j * rows : (j + 1) * rows, :], NEG)
        tops = jnp.maximum(tops, jnp.max(sj.reshape(rows // 8, 8, lanes), axis=0))
        counts.append(c)
        masked.append(sj)
    top = jnp.maximum(old, jnp.max(tops, axis=0, keepdims=True))
    shrink = jnp.exp(old - top)
    sums = jnp.zeros((8, lanes), F32)
    probs = []
    for j in range(pages):
        p = jnp.exp(masked[j] - top) * counts[j]
        sums += jnp.sum(p.reshape(rows // 8, 8, lanes), axis=0)
        probs.append(p.astype(BF))
    p = jnp.concatenate(probs, axis=0)
    stat[0:1, :] = top
    stat[1:2, :] = stat[1:2, :] * shrink + jnp.sum(sums, axis=0, keepdims=True)
    acc[...] = acc[...] * shrink + lax.dot_general(
        values, p, (((0,), (0,)), ((), ())), preferred_element_type=F32
    )


def tables(first, half, rows, tab_ref, len_ref, full, part):
    entries, lanes = full.shape
    page_id = lax.broadcasted_iota(jnp.int32, (entries, lanes), 0) + first
    whole = jnp.zeros((entries, lanes), F32)
    rest = jnp.zeros((entries, lanes), jnp.int32)
    for j in range(tab_ref.shape[0]):
        hit = page_id == tab_ref[j : j + 1, :]
        kept = len_ref[...] - j * 2 * rows
        whole += jnp.where(hit & (kept >= 2 * rows), 1.0, 0.0)
        rest += jnp.where(hit & (kept > 0) & (kept < 2 * rows), kept, 0)
    full[...] = whole
    part[...] = rest - half * rows


def resident_kernel(
    half_ref, qa_ref, qb_ref, entry_ref, tab_ref, len_ref, pool_ref,
    acc_ref, stat_ref, qt_ref, full, part,
):
    i = pl.program_id(0)
    pages, rows, width = pool_ref.shape
    hd = width // 2
    mine = qa_ref.shape[0]
    games = entry_ref.shape[0]

    @pl.when(i == 0)
    def _():
        q = jnp.concatenate([qa_ref[...], qb_ref[...]], axis=0)
        qt_ref[...] = q.T
        tables(0, half_ref[0], rows, tab_ref, len_ref, full, part)
        s = jnp.dot(entry_ref[:, :hd], qt_ref[...], preferred_element_type=F32)
        game = lax.broadcasted_iota(jnp.int32, s.shape, 0)
        lane = lax.broadcasted_iota(jnp.int32, s.shape, 1)
        own = (lane < mine) & (lax.rem(lane, games) == game)
        p = jnp.where(own, 1.0, 0.0)
        stat_ref[...] = jnp.zeros(stat_ref.shape, F32)
        stat_ref[0:1, :] = jnp.max(jnp.where(own, s, NEG), axis=0, keepdims=True)
        stat_ref[1:2, :] = jnp.sum(p, axis=0, keepdims=True)
        acc_ref[...] = lax.dot_general(
            entry_ref[:, hd:], p.astype(BF), (((0,), (0,)), ((), ())), preferred_element_type=F32
        )

    chunk_step(pool_ref, i * pages, qt_ref, full, part, acc_ref, stat_ref)


def resident(half, q_mine, q_peer, entry, table, lengths, pool):
    slots, page_len, width = pool.shape
    rows = page_len // 2
    mine, hd = q_mine.shape
    lanes = 2 * mine
    block = 16
    whole = lambda shape: pl.BlockSpec(shape, lambda i, *_: (0,) * len(shape))
    outs = [
        jax.ShapeDtypeStruct((hd, lanes), F32),
        jax.ShapeDtypeStruct((8, lanes), F32),
        jax.ShapeDtypeStruct((hd, lanes), BF),
    ]
    return pl.pallas_call(
        resident_kernel,
        grid_spec=pltpu.PrefetchScalarGridSpec(
            num_scalar_prefetch=1,
            grid=(slots // block,),
            in_specs=[
                whole(q_mine.shape),
                whole(q_peer.shape),
                whole(entry.shape),
                whole(table.shape),
                whole(lengths.shape),
                pl.BlockSpec((block, rows, width), lambda i, h: (i, h[0], 0)),
            ],
            out_specs=[whole(o.shape) for o in outs],
            scratch_shapes=[
                pltpu.VMEM((slots, lanes), F32),
                pltpu.VMEM((slots, lanes), jnp.int32),
            ],
        ),
        out_shape=outs,
        compiler_params=params(),
        cost_estimate=cost(8),
        name="resident",
    )(half, q_mine, q_peer, entry, table, lengths, pool)


def moved_kernel(
    half_ref, qt_ref, tab_ref, len_ref, acc_in, stat_in, got_ref,
    keep_ref, send_ref, acc, stat, full, part,
):
    i = pl.program_id(0)
    pages, rows, width = got_ref.shape
    hd = width // 2
    mine = qt_ref.shape[1] // 2

    @pl.when(i == 0)
    def _():
        tables(full.shape[0], half_ref[0], rows, tab_ref, len_ref, full, part)
        acc[...] = acc_in[...]
        stat[...] = stat_in[...]

    chunk_step(got_ref, i * pages, qt_ref, full, part, acc, stat)

    @pl.when(i == pl.num_programs(0) - 1)
    def _():
        for k, out in enumerate((keep_ref, send_ref)):
            out[:hd, :] = acc[:, k * mine : (k + 1) * mine]
            out[hd : hd + 8, :] = stat[:, k * mine : (k + 1) * mine]


def moved(half, qt, table, lengths, acc, stat, got):
    slots, rows, width = got.shape
    hd, lanes = qt.shape
    block = 16
    whole = lambda shape: pl.BlockSpec(shape, lambda i, *_: (0,) * len(shape))
    out = jax.ShapeDtypeStruct((hd + 8, lanes // 2), F32)
    return pl.pallas_call(
        moved_kernel,
        grid_spec=pltpu.PrefetchScalarGridSpec(
            num_scalar_prefetch=1,
            grid=(slots // block,),
            in_specs=[
                whole(qt.shape),
                whole(table.shape),
                whole(lengths.shape),
                whole(acc.shape),
                whole(stat.shape),
                pl.BlockSpec((block, rows, width), lambda i, *_: (i, 0, 0)),
            ],
            out_specs=[whole(out.shape), whole(out.shape)],
            scratch_shapes=[
                pltpu.VMEM((hd, lanes), F32),
                pltpu.VMEM((8, lanes), F32),
                pltpu.VMEM((slots, lanes), F32),
                pltpu.VMEM((slots, lanes), jnp.int32),
            ],
        ),
        out_shape=[out, out],
        compiler_params=params(),
        cost_estimate=cost(8),
        name="moved",
    )(half, qt, table, lengths, acc, stat, got)


def project_kernel(mine_ref, a_ref, b_ref, w_ref, keep_ref, send_ref, scratch):
    hd = a_ref.shape[0] - 8
    ma, mb = a_ref[hd : hd + 1, :], b_ref[hd : hd + 1, :]
    top = jnp.maximum(ma, mb)
    wa, wb = jnp.exp(ma - top), jnp.exp(mb - top)
    den = a_ref[hd + 1 : hd + 2, :] * wa + b_ref[hd + 1 : hd + 2, :] * wb
    att = (a_ref[:hd, :] * wa + b_ref[:hd, :] * wb) / den
    att = att.T.astype(BF)
    games = scratch.shape[0]
    out = jnp.zeros(scratch.shape, F32)
    for h in range(att.shape[0] // games):
        out += jnp.dot(
            att[h * games : (h + 1) * games, :],
            w_ref[h * hd : (h + 1) * hd, :],
            preferred_element_type=F32,
        )
    scratch[...] = out
    rows = keep_ref.shape[1]
    m = mine_ref[0]
    core = lax.rem(m, 2)
    side = m // 2
    for ref, c in ((keep_ref, core), (send_ref, 1 - core)):
        for k, z in enumerate((side, 1 - side)):
            first = pl.multiple_of((z * 2 + c) * rows, rows)
            ref[k] = scratch[pl.ds(first, rows), :]


def project(mine, a, b, w, games):
    rows = games // 4
    whole = lambda shape: pl.BlockSpec(shape, lambda i, *_: (0,) * len(shape))
    out = jax.ShapeDtypeStruct((2, rows, w.shape[1]), F32)
    return pl.pallas_call(
        project_kernel,
        grid_spec=pltpu.PrefetchScalarGridSpec(
            num_scalar_prefetch=1,
            grid=(1,),
            in_specs=[whole(a.shape), whole(b.shape), whole(w.shape)],
            out_specs=[whole(out.shape), whole(out.shape)],
            scratch_shapes=[pltpu.VMEM((games, w.shape[1]), F32)],
        ),
        out_shape=[out, out],
        compiler_params=params(),
        cost_estimate=cost(3),
        name="project",
    )(mine, a, b, w)


def norm_kernel(mine_ref, keep_ref, got_ref, side_ref, res_ref, gain_ref, copies_ref, stream_ref):
    stream = res_ref[...].astype(F32) + ((keep_ref[0] + got_ref[0]) + side_ref[...])
    scale = lax.rsqrt(jnp.mean(stream * stream, axis=-1, keepdims=True) + 1e-06)
    normed = (stream * scale * (1.0 + gain_ref[...])).astype(BF)
    stream_ref[...] = stream
    for k in range(copies_ref.shape[0]):
        copies_ref[k] = normed


def norm(mine, keep, got, side, residual, gain, peers):
    _, rows, d = keep.shape
    whole = lambda shape: pl.BlockSpec(shape, lambda i, *_: (0,) * len(shape))
    outs = [
        jax.ShapeDtypeStruct((peers, rows, d), BF),
        jax.ShapeDtypeStruct((rows, d), F32),
    ]
    return pl.pallas_call(
        norm_kernel,
        grid_spec=pltpu.PrefetchScalarGridSpec(
            num_scalar_prefetch=1,
            grid=(1,),
            in_specs=[
                pl.BlockSpec((1, rows, d), lambda i, *_: (0, 0, 0)),
                pl.BlockSpec((1, rows, d), lambda i, *_: (0, 0, 0)),
                whole(side.shape),
                pl.BlockSpec((rows, d), lambda i, m: (m[0], 0)),
                whole(gain.shape),
            ],
            out_specs=[whole(o.shape) for o in outs],
        ),
        out_shape=outs,
        compiler_params=params(),
        cost_estimate=cost(2),
        name="norm",
    )(mine, keep, got, side, residual, gain)


def ffn_kernel(*refs):
    n = (len(refs) - 5) // 3
    x_ref = refs[0]
    w = [refs[1 + 3 * b : 4 + 3 * b] for b in range(n)]
    out_ref, x, hid, sem = refs[1 + 3 * n :]
    rows = x.shape[0]
    unit = w[0][0].shape[1]
    parts = sem.shape[0]
    step = rows // parts

    def load(k):
        at = pl.ds(k * step, step)
        return pltpu.make_async_copy(x_ref.at[at, :], x.at[at, :], sem.at[k])

    for k in range(parts):
        load(k).start()
    for k in range(parts):
        load(k).wait()
        at = slice(k * step, (k + 1) * step)
        for b, (g, u, _) in enumerate(w):
            both = jnp.dot(
                x[at, :], jnp.concatenate([g[...], u[...]], axis=1), preferred_element_type=F32
            )
            hid[at, b * unit : (b + 1) * unit] = (
                jax.nn.gelu(both[:, :unit], approximate=True) * both[:, unit:]
            ).astype(BF)
    cols = 512

    @pl.loop(0, out_ref.shape[1] // cols)
    def _(k):
        at = pl.ds(pl.multiple_of(k * cols, cols), cols)
        down = jnp.concatenate([d[:, at] for _, _, d in w], axis=0)
        out_ref[:, at] = jnp.dot(hid[...], down, preferred_element_type=F32).astype(BF)


def ffn(x, weights):
    n = len(weights)
    rows, d = x.shape
    unit = weights[0][0].shape[1]
    vmem = pl.BlockSpec(memory_space=pltpu.VMEM)
    return pl.pallas_call(
        ffn_kernel,
        in_specs=[pl.BlockSpec(memory_space=pltpu.HBM)] + [vmem] * (3 * n),
        out_specs=vmem,
        out_shape=jax.ShapeDtypeStruct((rows, d), BF),
        scratch_shapes=[
            pltpu.VMEM((rows, d), BF),
            pltpu.VMEM((rows, n * unit), BF),
            pltpu.SemaphoreType.DMA((2,)),
        ],
        compiler_params=params(),
        cost_estimate=cost(8),
        name="ffn",
    )(x, *[a for block in weights for a in block])


def finish_kernel(parts_ref, stream_ref, out_ref, held, sems):
    n = sems.shape[0]
    step = held.shape[0] // n

    def load(k):
        at = pl.ds(k * step, step)
        return pltpu.make_async_copy(parts_ref.at[at], held.at[at], sems.at[k])

    for k in range(n):
        load(k).start()
    total = jnp.zeros(out_ref.shape, F32)
    for k in range(n):
        load(k).wait()
        for j in range(k * step, (k + 1) * step):
            total += held[j].astype(F32)
    out_ref[...] = (stream_ref[...] + total).astype(BF)


def finish(parts, stream):
    vmem = pl.BlockSpec(memory_space=pltpu.VMEM)
    return pl.pallas_call(
        finish_kernel,
        in_specs=[pl.BlockSpec(memory_space=pltpu.HBM), vmem],
        out_specs=vmem,
        out_shape=jax.ShapeDtypeStruct(stream.shape, BF),
        scratch_shapes=[pltpu.VMEM(parts.shape, BF), pltpu.SemaphoreType.DMA((4,))],
        compiler_params=params(),
        cost_estimate=cost(2),
        name="finish",
    )(parts, stream)


def assemble_kernel(half_ref, mine_ref, peer_ref, out_ref):
    rows = mine_ref.shape[1]
    for ref, h in ((mine_ref, half_ref[0]), (peer_ref, 1 - half_ref[0])):
        out_ref[:, pl.ds(pl.multiple_of(h * rows, rows), rows), :] = ref[...]


def assemble(half, mine, peer):
    pages, rows, width = mine.shape
    block = 8
    spec = pl.BlockSpec((block, rows, width), lambda i, *_: (i, 0, 0))
    return pl.pallas_call(
        assemble_kernel,
        grid_spec=pltpu.PrefetchScalarGridSpec(
            num_scalar_prefetch=1,
            grid=(pages // block,),
            in_specs=[spec, spec],
            out_specs=pl.BlockSpec((block, 2 * rows, width), lambda i, *_: (i, 0, 0)),
        ),
        out_shape=jax.ShapeDtypeStruct((pages, 2 * rows, width), mine.dtype),
        compiler_params=params(),
        cost_estimate=cost(6),
        name="assemble",
    )(half, mine, peer)


def step(
    page_pool, move_count, send_slots, page_table, history_len, queries, new_entry, residual,
    out_proj, ffn_gain, gate_proj, up_proj, down_proj,
):
    axes = ("dp", "mp")
    n_dp, n_mp = lax.axis_size("dp"), lax.axis_size("mp")
    devices = n_dp * n_mp
    games, heads, hd = queries.shape
    page_len, width = page_pool.shape[1:]
    mine = lax.axis_index("mp").reshape(1)
    half = mine % 2
    swap = lambda bit: [(k, k ^ bit) for k in range(devices)]
    core, side = swap(1), swap(2)
    send = lambda a, pairs: lax.ppermute(a, axes, pairs)
    groups = [
        [k for k in range(devices) if k % 2 == c and ((k >> 1) ^ (k >> 2)) % 2 == w]
        for w in range(2)
        for c in range(2)
    ]
    peers = len(groups[0])
    exchange = lambda a: lax.all_to_all(a, axes, 0, 0, tiled=True, axis_index_groups=groups)

    out_pages = outgoing_pages(half, send_slots.reshape(-1), move_count.reshape(-1), page_pool)
    got = exchange(out_pages.reshape(n_dp, -1, page_len // 2, width)).reshape(out_pages.shape)

    q_mine = (queries.transpose(1, 0, 2) * jnp.asarray(hd**-0.5, BF)).reshape(
        heads * games, hd
    )
    q_peer = send(q_mine, core)
    copies = 2 * heads
    table = jnp.tile(page_table.T, (1, copies))
    lengths = jnp.tile(history_len[None, :], (1, copies))

    weights = (gate_proj, up_proj, down_proj)
    w_side = tuple(send(a, side) for a in weights)
    w_core = tuple(send(a, core) for a in weights)
    w_last = tuple(send(a, core) for a in w_side)

    acc, stat, qt = resident(half, q_mine, q_peer, new_entry, table, lengths, page_pool)
    keep, give = moved(half, qt, table, lengths, acc, stat, got)
    other = send(give, core)
    got_peer = send(got, core)
    hold, pass_on = project(mine, keep, other, out_proj, games)
    hold_got = send(pass_on, core)
    side_got = send(hold[1] + hold_got[1], side)
    arrived = assemble(half, got, got_peer)

    spread, stream = norm(
        mine, hold, hold_got, side_got, residual, ffn_gain.reshape(1, -1), peers
    )
    rows, d = stream.shape
    x = exchange(spread)
    parts = ffn(x.reshape(peers * rows, d), [weights, w_core, w_side, w_last])
    back = exchange(parts.reshape(peers, rows, d))
    quarter = finish(back, stream)
    layer_out = lax.all_gather(quarter, "mp", axis=0, tiled=True)
    return arrived, layer_out


def solution(mesh):
    in_specs = (
        P("dp", None, None),
        P("dp", None),
        P("dp", None),
        P("dp", None),
        P("dp"),
        P("dp", "mp", None),
        P("dp", None),
        P("dp", None),
        P("mp", None),
        P(),
        P(None, ("dp", "mp")),
        P(None, ("dp", "mp")),
        P(("dp", "mp"), None),
    )
    out_specs = (P("dp", None, None), P("dp", None))
    return jax.shard_map(step, mesh=mesh, in_specs=in_specs, out_specs=out_specs, check_vma=False)
```

```python
import jax
import jax.numpy as jnp
from jax import lax
from jax.experimental import pallas as pl
from jax.experimental.pallas import tpu as pltpu
from jax.sharding import PartitionSpec as P


NEG = -1e30
BF = jnp.bfloat16
F32 = jnp.float32


def params(mib):
    return pltpu.CompilerParams(vmem_limit_bytes=mib * 1024 * 1024)


def cost(us):
    return pl.CostEstimate(flops=int(us * 4e8), bytes_accessed=int(us * 2e6), transcendentals=0)


def outgoing_kernel(half_ref, slot_ref, count_ref, pool_ref, out_ref, sems):
    pages, rows, _ = out_ref.shape
    caps = pages // count_ref.shape[0]
    first = pl.multiple_of(half_ref[0] * rows, rows)

    def copy(i):
        src = pool_ref.at[slot_ref[i], pl.ds(first, rows), :]
        return pltpu.make_async_copy(src, out_ref.at[i], sems.at[i])

    copies = [copy(i) for i in range(pages)]
    for c in copies:
        c.start()
    for i, c in enumerate(copies):
        c.wait()

        @pl.when(i % caps >= count_ref[i // caps])
        def _():
            out_ref[i] = jnp.zeros(out_ref.shape[1:], out_ref.dtype)


def outgoing_pages(half, slots, counts, pool):
    pages = slots.shape[0]
    rows = pool.shape[1] // 2
    return pl.pallas_call(
        outgoing_kernel,
        grid_spec=pltpu.PrefetchScalarGridSpec(
            num_scalar_prefetch=3,
            grid=(1,),
            in_specs=[pl.BlockSpec(memory_space=pl.ANY)],
            out_specs=pl.BlockSpec((pages, rows, pool.shape[2]), lambda i, *_: (0, 0, 0)),
            scratch_shapes=[pltpu.SemaphoreType.DMA((pages,))],
        ),
        out_shape=jax.ShapeDtypeStruct((pages, rows, pool.shape[2]), pool.dtype),
        compiler_params=params(60),
        cost_estimate=cost(3),
        name="outgoing",
    )(half, slots, counts, pool)


def chunk_step(block, base, qt, full, part, acc, stat):
    pages, rows, width = block.shape
    hd = width // 2
    lanes = qt.shape[1]
    keys = block[:, :, :hd].reshape(pages * rows, hd)
    values = block[:, :, hd:].reshape(pages * rows, hd)
    s = jnp.dot(keys, qt[...], preferred_element_type=F32)
    spot = lax.broadcasted_iota(jnp.int32, (rows, lanes), 0)
    old = stat[0:1, :]
    tops = jnp.full((8, lanes), NEG, F32)
    counts = []
    masked = []
    for j in range(pages):
        c = full[pl.ds(base + j, 1), :] + jnp.where(
            spot < part[pl.ds(base + j, 1), :], 1.0, 0.0
        )
        sj = jnp.where(c > 0.0, s[j * rows : (j + 1) * rows, :], NEG)
        tops = jnp.maximum(tops, jnp.max(sj.reshape(rows // 8, 8, lanes), axis=0))
        counts.append(c)
        masked.append(sj)
    top = jnp.maximum(old, jnp.max(tops, axis=0, keepdims=True))
    shrink = jnp.exp(old - top)
    sums = jnp.zeros((8, lanes), F32)
    probs = []
    for j in range(pages):
        p = jnp.exp(masked[j] - top) * counts[j]
        sums += jnp.sum(p.reshape(rows // 8, 8, lanes), axis=0)
        probs.append(p.astype(BF))
    p = jnp.concatenate(probs, axis=0)
    stat[0:1, :] = top
    stat[1:2, :] = stat[1:2, :] * shrink + jnp.sum(sums, axis=0, keepdims=True)
    acc[...] = acc[...] * shrink + lax.dot_general(
        values, p, (((0,), (0,)), ((), ())), preferred_element_type=F32
    )


def tables(first, half, rows, tab_ref, len_ref, full, part):
    entries, lanes = full.shape
    page_id = lax.broadcasted_iota(jnp.int32, (entries, lanes), 0) + first
    whole = jnp.zeros((entries, lanes), F32)
    rest = jnp.zeros((entries, lanes), jnp.int32)
    for j in range(tab_ref.shape[0]):
        hit = page_id == tab_ref[j : j + 1, :]
        kept = len_ref[...] - j * 2 * rows
        whole += jnp.where(hit & (kept >= 2 * rows), 1.0, 0.0)
        rest += jnp.where(hit & (kept > 0) & (kept < 2 * rows), kept, 0)
    full[...] = whole
    part[...] = rest - half * rows


def resident_kernel(
    half_ref, qa_ref, qb_ref, entry_ref, tab_ref, len_ref, pool_ref,
    acc_ref, stat_ref, qt_ref, full, part,
):
    i = pl.program_id(0)
    pages, rows, width = pool_ref.shape
    hd = width // 2
    mine = qa_ref.shape[0]
    games = entry_ref.shape[0]

    @pl.when(i == 0)
    def _():
        q = jnp.concatenate([qa_ref[...], qb_ref[...]], axis=0)
        qt_ref[...] = q.T
        tables(0, half_ref[0], rows, tab_ref, len_ref, full, part)
        s = jnp.dot(entry_ref[:, :hd], qt_ref[...], preferred_element_type=F32)
        game = lax.broadcasted_iota(jnp.int32, s.shape, 0)
        lane = lax.broadcasted_iota(jnp.int32, s.shape, 1)
        own = (lane < mine) & (lax.rem(lane, games) == game)
        p = jnp.where(own, 1.0, 0.0)
        stat_ref[...] = jnp.zeros(stat_ref.shape, F32)
        stat_ref[0:1, :] = jnp.max(jnp.where(own, s, NEG), axis=0, keepdims=True)
        stat_ref[1:2, :] = jnp.sum(p, axis=0, keepdims=True)
        acc_ref[...] = lax.dot_general(
            entry_ref[:, hd:], p.astype(BF), (((0,), (0,)), ((), ())), preferred_element_type=F32
        )

    chunk_step(pool_ref, i * pages, qt_ref, full, part, acc_ref, stat_ref)


def resident(half, q_mine, q_peer, entry, table, lengths, pool):
    slots, page_len, width = pool.shape
    rows = page_len // 2
    mine, hd = q_mine.shape
    lanes = 2 * mine
    block = 16
    whole = lambda shape: pl.BlockSpec(shape, lambda i, *_: (0,) * len(shape))
    outs = [
        jax.ShapeDtypeStruct((hd, lanes), F32),
        jax.ShapeDtypeStruct((8, lanes), F32),
        jax.ShapeDtypeStruct((hd, lanes), BF),
    ]
    return pl.pallas_call(
        resident_kernel,
        grid_spec=pltpu.PrefetchScalarGridSpec(
            num_scalar_prefetch=1,
            grid=(slots // block,),
            in_specs=[
                whole(q_mine.shape),
                whole(q_peer.shape),
                whole(entry.shape),
                whole(table.shape),
                whole(lengths.shape),
                pl.BlockSpec((block, rows, width), lambda i, h: (i, h[0], 0)),
            ],
            out_specs=[whole(o.shape) for o in outs],
            scratch_shapes=[
                pltpu.VMEM((slots, lanes), F32),
                pltpu.VMEM((slots, lanes), jnp.int32),
            ],
        ),
        out_shape=outs,
        compiler_params=params(60),
        cost_estimate=cost(8),
        name="resident",
    )(half, q_mine, q_peer, entry, table, lengths, pool)


def moved_kernel(
    half_ref, qt_ref, tab_ref, len_ref, acc_in, stat_in, got_ref,
    keep_ref, send_ref, acc, stat, full, part,
):
    i = pl.program_id(0)
    pages, rows, width = got_ref.shape
    hd = width // 2
    mine = qt_ref.shape[1] // 2

    @pl.when(i == 0)
    def _():
        tables(full.shape[0], half_ref[0], rows, tab_ref, len_ref, full, part)
        acc[...] = acc_in[...]
        stat[...] = stat_in[...]

    chunk_step(got_ref, i * pages, qt_ref, full, part, acc, stat)

    @pl.when(i == pl.num_programs(0) - 1)
    def _():
        for k, out in enumerate((keep_ref, send_ref)):
            out[:hd, :] = acc[:, k * mine : (k + 1) * mine]
            out[hd : hd + 8, :] = stat[:, k * mine : (k + 1) * mine]


def moved(half, qt, table, lengths, acc, stat, got):
    slots, rows, width = got.shape
    hd, lanes = qt.shape
    block = 16
    whole = lambda shape: pl.BlockSpec(shape, lambda i, *_: (0,) * len(shape))
    out = jax.ShapeDtypeStruct((hd + 8, lanes // 2), F32)
    return pl.pallas_call(
        moved_kernel,
        grid_spec=pltpu.PrefetchScalarGridSpec(
            num_scalar_prefetch=1,
            grid=(slots // block,),
            in_specs=[
                whole(qt.shape),
                whole(table.shape),
                whole(lengths.shape),
                whole(acc.shape),
                whole(stat.shape),
                pl.BlockSpec((block, rows, width), lambda i, *_: (i, 0, 0)),
            ],
            out_specs=[whole(out.shape), whole(out.shape)],
            scratch_shapes=[
                pltpu.VMEM((hd, lanes), F32),
                pltpu.VMEM((8, lanes), F32),
                pltpu.VMEM((slots, lanes), F32),
                pltpu.VMEM((slots, lanes), jnp.int32),
            ],
        ),
        out_shape=[out, out],
        compiler_params=params(20),
        cost_estimate=cost(8),
        name="moved",
    )(half, qt, table, lengths, acc, stat, got)


def project_kernel(mine_ref, a_ref, b_ref, w_ref, keep_ref, send_ref, scratch):
    hd = a_ref.shape[0] - 8
    ma, mb = a_ref[hd : hd + 1, :], b_ref[hd : hd + 1, :]
    top = jnp.maximum(ma, mb)
    wa, wb = jnp.exp(ma - top), jnp.exp(mb - top)
    den = a_ref[hd + 1 : hd + 2, :] * wa + b_ref[hd + 1 : hd + 2, :] * wb
    att = (a_ref[:hd, :] * wa + b_ref[:hd, :] * wb) / den
    att = att.T.astype(BF)
    games = scratch.shape[0]
    out = jnp.zeros(scratch.shape, F32)
    for h in range(att.shape[0] // games):
        out += jnp.dot(
            att[h * games : (h + 1) * games, :],
            w_ref[h * hd : (h + 1) * hd, :],
            preferred_element_type=F32,
        )
    scratch[...] = out
    rows = keep_ref.shape[1]
    m = mine_ref[0]
    core = lax.rem(m, 2)
    side = m // 2
    for ref, c in ((keep_ref, core), (send_ref, 1 - core)):
        for k, z in enumerate((side, 1 - side)):
            first = pl.multiple_of((z * 2 + c) * rows, rows)
            ref[k] = scratch[pl.ds(first, rows), :]


def project(mine, a, b, w, games):
    rows = games // 4
    whole = lambda shape: pl.BlockSpec(shape, lambda i, *_: (0,) * len(shape))
    out = jax.ShapeDtypeStruct((2, rows, w.shape[1]), F32)
    return pl.pallas_call(
        project_kernel,
        grid_spec=pltpu.PrefetchScalarGridSpec(
            num_scalar_prefetch=1,
            grid=(1,),
            in_specs=[whole(a.shape), whole(b.shape), whole(w.shape)],
            out_specs=[whole(out.shape), whole(out.shape)],
            scratch_shapes=[pltpu.VMEM((games, w.shape[1]), F32)],
        ),
        out_shape=[out, out],
        compiler_params=params(10),
        cost_estimate=cost(3),
        name="project",
    )(mine, a, b, w)


def norm_kernel(mine_ref, keep_ref, got_ref, side_ref, res_ref, gain_ref, copies_ref, stream_ref):
    stream = res_ref[...].astype(F32) + ((keep_ref[0] + got_ref[0]) + side_ref[...])
    scale = lax.rsqrt(jnp.mean(stream * stream, axis=-1, keepdims=True) + 1e-06)
    normed = (stream * scale * (1.0 + gain_ref[...])).astype(BF)
    stream_ref[...] = stream
    for k in range(copies_ref.shape[0]):
        copies_ref[k] = normed


def norm(mine, keep, got, side, residual, gain, peers):
    _, rows, d = keep.shape
    whole = lambda shape: pl.BlockSpec(shape, lambda i, *_: (0,) * len(shape))
    outs = [
        jax.ShapeDtypeStruct((peers, rows, d), BF),
        jax.ShapeDtypeStruct((rows, d), F32),
    ]
    return pl.pallas_call(
        norm_kernel,
        grid_spec=pltpu.PrefetchScalarGridSpec(
            num_scalar_prefetch=1,
            grid=(1,),
            in_specs=[
                pl.BlockSpec((1, rows, d), lambda i, *_: (0, 0, 0)),
                pl.BlockSpec((1, rows, d), lambda i, *_: (0, 0, 0)),
                whole(side.shape),
                pl.BlockSpec((rows, d), lambda i, m: (m[0], 0)),
                whole(gain.shape),
            ],
            out_specs=[whole(o.shape) for o in outs],
        ),
        out_shape=outs,
        compiler_params=params(6),
        cost_estimate=cost(2),
        name="norm",
    )(mine, keep, got, side, residual, gain)


def ffn_kernel(*refs):
    n = (len(refs) - 3) // 3
    x_ref = refs[0]
    w = [refs[1 + 3 * b : 4 + 3 * b] for b in range(n)]
    out_ref, hid = refs[1 + 3 * n :]
    unit = w[0][0].shape[1]
    for b, (g, u, _) in enumerate(w):
        both = jnp.dot(
            x_ref[...], jnp.concatenate([g[...], u[...]], axis=1), preferred_element_type=F32
        )
        hid[:, b * unit : (b + 1) * unit] = (
            jax.nn.gelu(both[:, :unit], approximate=True) * both[:, unit:]
        ).astype(BF)
    cols = 512

    @pl.loop(0, out_ref.shape[1] // cols)
    def _(k):
        at = pl.ds(pl.multiple_of(k * cols, cols), cols)
        down = jnp.concatenate([d[:, at] for _, _, d in w], axis=0)
        out_ref[:, at] = jnp.dot(hid[...], down, preferred_element_type=F32).astype(BF)


def ffn(x, weights):
    n = len(weights)
    rows, d = x.shape
    unit = weights[0][0].shape[1]
    vmem = pl.BlockSpec(memory_space=pltpu.VMEM)
    return pl.pallas_call(
        ffn_kernel,
        in_specs=[vmem] * (1 + 3 * n),
        out_specs=vmem,
        out_shape=jax.ShapeDtypeStruct((rows, d), BF),
        scratch_shapes=[pltpu.VMEM((rows, n * unit), BF)],
        compiler_params=params(24),
        cost_estimate=cost(8),
        name="ffn",
    )(x, *[a for block in weights for a in block])


def finish_kernel(parts_ref, stream_ref, out_ref):
    total = parts_ref[0].astype(F32)
    for k in range(1, parts_ref.shape[0]):
        total += parts_ref[k].astype(F32)
    out_ref[...] = (stream_ref[...] + total).astype(BF)


def finish(parts, stream):
    vmem = pl.BlockSpec(memory_space=pltpu.VMEM)
    return pl.pallas_call(
        finish_kernel,
        in_specs=[vmem, vmem],
        out_specs=vmem,
        out_shape=jax.ShapeDtypeStruct(stream.shape, BF),
        compiler_params=params(4),
        cost_estimate=cost(2),
        name="finish",
    )(parts, stream)


def assemble_kernel(half_ref, mine_ref, peer_ref, out_ref):
    rows = mine_ref.shape[1]
    for ref, h in ((mine_ref, half_ref[0]), (peer_ref, 1 - half_ref[0])):
        out_ref[:, pl.ds(pl.multiple_of(h * rows, rows), rows), :] = ref[...]


def assemble(half, mine, peer):
    pages, rows, width = mine.shape
    block = 8
    spec = pl.BlockSpec((block, rows, width), lambda i, *_: (i, 0, 0))
    return pl.pallas_call(
        assemble_kernel,
        grid_spec=pltpu.PrefetchScalarGridSpec(
            num_scalar_prefetch=1,
            grid=(pages // block,),
            in_specs=[spec, spec],
            out_specs=pl.BlockSpec((block, 2 * rows, width), lambda i, *_: (i, 0, 0)),
        ),
        out_shape=jax.ShapeDtypeStruct((pages, 2 * rows, width), mine.dtype),
        compiler_params=params(8),
        cost_estimate=cost(6),
        name="assemble",
    )(half, mine, peer)


def step(
    page_pool, move_count, send_slots, page_table, history_len, queries, new_entry, residual,
    out_proj, ffn_gain, gate_proj, up_proj, down_proj,
):
    axes = ("dp", "mp")
    n_dp, n_mp = lax.axis_size("dp"), lax.axis_size("mp")
    devices = n_dp * n_mp
    games, heads, hd = queries.shape
    page_len, width = page_pool.shape[1:]
    mine = lax.axis_index("mp").reshape(1)
    half = mine % 2
    swap = lambda bit: [(k, k ^ bit) for k in range(devices)]
    send = lambda a, pairs: lax.ppermute(a, axes, pairs)
    core, side, far = swap(1), swap(2), swap(6)
    every = range(devices)
    groups = [
        [k for k in every if k % 2 == c and ((k >> 1) ^ (k >> 2)) % 2 == w]
        for w in range(2)
        for c in range(2)
    ]
    planes = [[k for k in every if k % 8 == z] for z in range(8)]
    peers = len(planes[0])
    exchange = lambda a, who: lax.all_to_all(
        a, axes, 0, 0, tiled=True, axis_index_groups=who
    )

    out_pages = outgoing_pages(half, send_slots.reshape(-1), move_count.reshape(-1), page_pool)
    got = exchange(
        out_pages.reshape(n_dp, -1, page_len // 2, width), groups
    ).reshape(out_pages.shape)

    q_mine = (queries.transpose(1, 0, 2) * jnp.asarray(hd**-0.5, BF)).reshape(
        heads * games, hd
    )
    q_peer = send(q_mine, core)
    copies = 2 * heads
    table = jnp.tile(page_table.T, (1, copies))
    lengths = jnp.tile(history_len[None, :], (1, copies))

    weights = (gate_proj, up_proj, down_proj)
    each = lambda ws, pairs: tuple(send(a, pairs) for a in ws)
    w_side = each(weights, side)
    w_core = each(weights, core)
    w_side_core = each(w_side, core)
    w_far = each(weights, far)
    w_diag = each(w_far, side)
    w_far_core = each(w_far, core)
    w_diag_core = each(w_diag, core)
    blocks = [
        weights, w_core, w_side, w_side_core, w_far, w_far_core, w_diag, w_diag_core
    ]

    acc, stat, qt = resident(half, q_mine, q_peer, new_entry, table, lengths, page_pool)
    keep, give = moved(half, qt, table, lengths, acc, stat, got)
    other = send(give, core)
    got_peer = send(got, core)
    hold, pass_on = project(mine, keep, other, out_proj, games)
    hold_got = send(pass_on, core)
    side_got = send(hold[1] + hold_got[1], side)
    arrived = assemble(half, got, got_peer)

    spread, stream = norm(
        mine, hold, hold_got, side_got, residual, ffn_gain.reshape(1, -1), peers
    )
    rows, d = stream.shape
    x = exchange(spread, planes)
    parts = ffn(x.reshape(peers * rows, d), blocks)
    back = exchange(parts.reshape(peers, rows, d), planes)
    quarter = finish(back, stream)
    layer_out = lax.all_gather(quarter, "mp", axis=0, tiled=True)
    return arrived, layer_out


def solution(mesh):
    in_specs = (
        P("dp", None, None),
        P("dp", None),
        P("dp", None),
        P("dp", None),
        P("dp"),
        P("dp", "mp", None),
        P("dp", None),
        P("dp", None),
        P("mp", None),
        P(),
        P(None, ("dp", "mp")),
        P(None, ("dp", "mp")),
        P(("dp", "mp"), None),
    )
    out_specs = (P("dp", None, None), P("dp", None))
    return jax.shard_map(
        step, mesh=mesh, in_specs=in_specs, out_specs=out_specs, check_vma=False
    )
```

```python
import jax
import jax.numpy as jnp
from jax import lax
from jax.experimental import pallas as pl
from jax.experimental.pallas import tpu as pltpu
from jax.sharding import PartitionSpec as P


NEG = -1e30
BF = jnp.bfloat16
F32 = jnp.float32


def params(mib):
    return pltpu.CompilerParams(vmem_limit_bytes=mib * 1024 * 1024)


def cost(us):
    return pl.CostEstimate(flops=int(us * 4e8), bytes_accessed=int(us * 2e6), transcendentals=0)


def outgoing_kernel(half_ref, slot_ref, count_ref, pool_ref, out_ref, sems):
    pages, rows, _ = out_ref.shape
    caps = pages // count_ref.shape[0]
    first = pl.multiple_of(half_ref[0] * rows, rows)

    def copy(i):
        src = pool_ref.at[slot_ref[i // caps, i % caps], pl.ds(first, rows), :]
        return pltpu.make_async_copy(src, out_ref.at[i], sems.at[i])

    copies = [copy(i) for i in range(pages)]
    for c in copies:
        c.start()
    for i, c in enumerate(copies):
        c.wait()

        @pl.when(i % caps >= count_ref[i // caps])
        def _():
            out_ref[i] = jnp.zeros(out_ref.shape[1:], out_ref.dtype)


def outgoing_pages(half, slots, counts, pool):
    pages = slots.size
    rows = pool.shape[1] // 2
    return pl.pallas_call(
        outgoing_kernel,
        grid_spec=pltpu.PrefetchScalarGridSpec(
            num_scalar_prefetch=3,
            grid=(1,),
            in_specs=[pl.BlockSpec(memory_space=pltpu.HBM)],
            out_specs=pl.BlockSpec((pages, rows, pool.shape[2]), lambda i, *_: (0, 0, 0)),
            scratch_shapes=[pltpu.SemaphoreType.DMA((pages,))],
        ),
        out_shape=jax.ShapeDtypeStruct((pages, rows, pool.shape[2]), pool.dtype),
        compiler_params=params(60),
        cost_estimate=cost(3),
        name="outgoing",
    )(half, slots, counts, pool)


def chunk_step(block, base, qt, full, part, acc, stat):
    pages, rows, width = block.shape
    hd = width // 2
    lanes = qt.shape[1]
    keys = block[:, :, :hd].reshape(pages * rows, hd)
    values = block[:, :, hd:].reshape(pages * rows, hd)
    s = jnp.dot(keys, qt[...], preferred_element_type=F32)
    spot = lax.broadcasted_iota(jnp.int32, (rows, lanes), 0)
    old = stat[0:1, :]
    tops = jnp.full((8, lanes), NEG, F32)
    counts = []
    masked = []
    for j in range(pages):
        c = full[pl.ds(base + j, 1), :] + jnp.where(
            spot < part[pl.ds(base + j, 1), :], 1.0, 0.0
        )
        sj = jnp.where(c > 0.0, s[j * rows : (j + 1) * rows, :], NEG)
        tops = jnp.maximum(tops, jnp.max(sj.reshape(rows // 8, 8, lanes), axis=0))
        counts.append(c)
        masked.append(sj)
    top = jnp.maximum(old, jnp.max(tops, axis=0, keepdims=True))
    shrink = jnp.exp(old - top)
    sums = jnp.zeros((8, lanes), F32)
    probs = []
    for j in range(pages):
        p = jnp.exp(masked[j] - top) * counts[j]
        sums += jnp.sum(p.reshape(rows // 8, 8, lanes), axis=0)
        probs.append(p.astype(BF))
    p = jnp.concatenate(probs, axis=0)
    stat[0:1, :] = top
    stat[1:2, :] = stat[1:2, :] * shrink + jnp.sum(sums, axis=0, keepdims=True)
    acc[...] = acc[...] * shrink + lax.dot_general(
        values, p, (((0,), (0,)), ((), ())), preferred_element_type=F32
    )


def tables(first, half, rows, tab_ref, len_ref, full, part):
    entries, lanes = full.shape
    page_id = lax.broadcasted_iota(jnp.int32, (entries, lanes), 0) + first
    whole = jnp.zeros((entries, lanes), F32)
    rest = jnp.zeros((entries, lanes), jnp.int32)
    for j in range(tab_ref.shape[0]):
        hit = page_id == tab_ref[j : j + 1, :]
        kept = len_ref[...] - j * 2 * rows
        whole += jnp.where(hit & (kept >= 2 * rows), 1.0, 0.0)
        rest += jnp.where(hit & (kept > 0) & (kept < 2 * rows), kept, 0)
    full[...] = whole
    part[...] = rest - half * rows


def resident_kernel(
    half_ref, qa_ref, qb_ref, entry_ref, tab_ref, len_ref, pool_ref,
    acc_ref, stat_ref, qt_ref, full, part, held, sems,
):
    i = pl.program_id(0)
    steps = sems.shape[0]
    slots, rows, width = held.shape
    pages = slots // steps
    hd = width // 2
    first = pl.multiple_of(half_ref[0] * rows, rows)

    def load(k):
        at = pl.ds(k * pages, pages)
        return pltpu.make_async_copy(
            pool_ref.at[at, pl.ds(first, rows), :], held.at[at], sems.at[k]
        )

    mine = qa_ref.shape[0]
    games = entry_ref.shape[0]

    @pl.when(i == 0)
    def _():
        for k in range(steps):
            load(k).start()
        q = jnp.concatenate([qa_ref[...], qb_ref[...]], axis=0)
        qt_ref[...] = q.T
        tables(0, half_ref[0], rows, tab_ref, len_ref, full, part)
        s = jnp.dot(entry_ref[:, :hd], qt_ref[...], preferred_element_type=F32)
        game = lax.broadcasted_iota(jnp.int32, s.shape, 0)
        lane = lax.broadcasted_iota(jnp.int32, s.shape, 1)
        own = (lane < mine) & (lax.rem(lane, games) == game)
        p = jnp.where(own, 1.0, 0.0)
        stat_ref[...] = jnp.zeros(stat_ref.shape, F32)
        stat_ref[0:1, :] = jnp.max(jnp.where(own, s, NEG), axis=0, keepdims=True)
        stat_ref[1:2, :] = jnp.sum(p, axis=0, keepdims=True)
        acc_ref[...] = lax.dot_general(
            entry_ref[:, hd:], p.astype(BF), (((0,), (0,)), ((), ())), preferred_element_type=F32
        )

    load(i).wait()
    at = pl.ds(pl.multiple_of(i * pages, pages), pages)
    chunk_step(held.at[at], i * pages, qt_ref, full, part, acc_ref, stat_ref)


def resident(half, q_mine, q_peer, entry, table, lengths, pool):
    slots, page_len, width = pool.shape
    rows = page_len // 2
    mine, hd = q_mine.shape
    lanes = 2 * mine
    block = 16
    whole = lambda shape: pl.BlockSpec(shape, lambda i, *_: (0,) * len(shape))
    outs = [
        jax.ShapeDtypeStruct((hd, lanes), F32),
        jax.ShapeDtypeStruct((8, lanes), F32),
        jax.ShapeDtypeStruct((hd, lanes), BF),
    ]
    return pl.pallas_call(
        resident_kernel,
        grid_spec=pltpu.PrefetchScalarGridSpec(
            num_scalar_prefetch=1,
            grid=(slots // block,),
            in_specs=[
                whole(q_mine.shape),
                whole(q_peer.shape),
                whole(entry.shape),
                whole(table.shape),
                whole(lengths.shape),
                pl.BlockSpec(memory_space=pltpu.HBM),
            ],
            out_specs=[whole(o.shape) for o in outs],
            scratch_shapes=[
                pltpu.VMEM((slots, lanes), F32),
                pltpu.VMEM((slots, lanes), jnp.int32),
                pltpu.VMEM((slots, rows, width), BF),
                pltpu.SemaphoreType.DMA((slots // block,)),
            ],
        ),
        out_shape=outs,
        compiler_params=params(57),
        cost_estimate=cost(8),
        name="resident",
    )(half, q_mine, q_peer, entry, table, lengths, pool)


def moved_kernel(
    half_ref, qt_ref, tab_ref, len_ref, acc_in, stat_in, got_ref,
    keep_ref, send_ref, acc, stat, full, part,
):
    i = pl.program_id(0)
    pages, rows, width = got_ref.shape
    hd = width // 2
    mine = qt_ref.shape[1] // 2

    @pl.when(i == 0)
    def _():
        tables(full.shape[0], half_ref[0], rows, tab_ref, len_ref, full, part)
        acc[...] = acc_in[...]
        stat[...] = stat_in[...]

    chunk_step(got_ref, i * pages, qt_ref, full, part, acc, stat)

    @pl.when(i == pl.num_programs(0) - 1)
    def _():
        for k, out in enumerate((keep_ref, send_ref)):
            out[:hd, :] = acc[:, k * mine : (k + 1) * mine]
            out[hd : hd + 8, :] = stat[:, k * mine : (k + 1) * mine]


def moved(half, qt, table, lengths, acc, stat, got):
    slots, rows, width = got.shape
    hd, lanes = qt.shape
    block = 16
    whole = lambda shape: pl.BlockSpec(shape, lambda i, *_: (0,) * len(shape))
    out = jax.ShapeDtypeStruct((hd + 8, lanes // 2), F32)
    return pl.pallas_call(
        moved_kernel,
        grid_spec=pltpu.PrefetchScalarGridSpec(
            num_scalar_prefetch=1,
            grid=(slots // block,),
            in_specs=[
                whole(qt.shape),
                whole(table.shape),
                whole(lengths.shape),
                whole(acc.shape),
                whole(stat.shape),
                pl.BlockSpec((block, rows, width), lambda i, *_: (i, 0, 0)),
            ],
            out_specs=[whole(out.shape), whole(out.shape)],
            scratch_shapes=[
                pltpu.VMEM((hd, lanes), F32),
                pltpu.VMEM((8, lanes), F32),
                pltpu.VMEM((slots, lanes), F32),
                pltpu.VMEM((slots, lanes), jnp.int32),
            ],
        ),
        out_shape=[out, out],
        compiler_params=params(60),
        cost_estimate=cost(8),
        name="moved",
    )(half, qt, table, lengths, acc, stat, got)


def project_kernel(mine_ref, a_ref, b_ref, w_ref, keep_ref, send_ref, scratch):
    hd = a_ref.shape[0] - 8
    ma, mb = a_ref[hd : hd + 1, :], b_ref[hd : hd + 1, :]
    top = jnp.maximum(ma, mb)
    wa, wb = jnp.exp(ma - top), jnp.exp(mb - top)
    den = a_ref[hd + 1 : hd + 2, :] * wa + b_ref[hd + 1 : hd + 2, :] * wb
    att = (a_ref[:hd, :] * wa + b_ref[:hd, :] * wb) / den
    att = att.T.astype(BF)
    games = scratch.shape[0]
    out = jnp.zeros(scratch.shape, F32)
    for h in range(att.shape[0] // games):
        out += jnp.dot(
            att[h * games : (h + 1) * games, :],
            w_ref[h * hd : (h + 1) * hd, :],
            preferred_element_type=F32,
        )
    scratch[...] = out
    rows = keep_ref.shape[1]
    m = mine_ref[0]
    core = lax.rem(m, 2)
    side = m // 2
    for ref, c in ((keep_ref, core), (send_ref, 1 - core)):
        for k, z in enumerate((side, 1 - side)):
            first = pl.multiple_of((z * 2 + c) * rows, rows)
            ref[k] = scratch[pl.ds(first, rows), :]


def project(mine, a, b, w, games):
    rows = games // 4
    whole = lambda shape: pl.BlockSpec(shape, lambda i, *_: (0,) * len(shape))
    out = jax.ShapeDtypeStruct((2, rows, w.shape[1]), F32)
    return pl.pallas_call(
        project_kernel,
        grid_spec=pltpu.PrefetchScalarGridSpec(
            num_scalar_prefetch=1,
            grid=(1,),
            in_specs=[whole(a.shape), whole(b.shape), whole(w.shape)],
            out_specs=[whole(out.shape), whole(out.shape)],
            scratch_shapes=[pltpu.VMEM((games, w.shape[1]), F32)],
        ),
        out_shape=[out, out],
        compiler_params=params(10),
        cost_estimate=cost(3),
        name="project",
    )(mine, a, b, w)


def norm_kernel(mine_ref, keep_ref, got_ref, side_ref, res_ref, gain_ref, copies_ref, stream_ref):
    stream = res_ref[...].astype(F32) + ((keep_ref[0] + got_ref[0]) + side_ref[...])
    scale = lax.rsqrt(jnp.mean(stream * stream, axis=-1, keepdims=True) + 1e-06)
    normed = (stream * scale * (1.0 + gain_ref[...])).astype(BF)
    stream_ref[...] = stream
    for k in range(copies_ref.shape[0]):
        copies_ref[k] = normed


def norm(mine, keep, got, side, residual, gain, peers):
    _, rows, d = keep.shape
    whole = lambda shape: pl.BlockSpec(shape, lambda i, *_: (0,) * len(shape))
    outs = [
        jax.ShapeDtypeStruct((peers, rows, d), BF),
        jax.ShapeDtypeStruct((rows, d), F32),
    ]
    return pl.pallas_call(
        norm_kernel,
        grid_spec=pltpu.PrefetchScalarGridSpec(
            num_scalar_prefetch=1,
            grid=(1,),
            in_specs=[
                pl.BlockSpec((1, rows, d), lambda i, *_: (0, 0, 0)),
                pl.BlockSpec((1, rows, d), lambda i, *_: (0, 0, 0)),
                whole(side.shape),
                pl.BlockSpec((rows, d), lambda i, m: (m[0], 0)),
                whole(gain.shape),
            ],
            out_specs=[whole(o.shape) for o in outs],
        ),
        out_shape=outs,
        compiler_params=params(6),
        cost_estimate=cost(2),
        name="norm",
    )(mine, keep, got, side, residual, gain)


def ffn_kernel(*refs):
    n = (len(refs) - 6) // 3
    x_ref = refs[0]
    w = [refs[1 + 3 * b : 4 + 3 * b] for b in range(n)]
    out_ref, gu, down, hid, sems = refs[1 + 3 * n :]
    unit = gu.shape[2] // 2

    def loads(b):
        g, u, d = w[b]
        return (
            pltpu.make_async_copy(g, gu.at[b, :, pl.ds(0, unit)], sems.at[3 * b]),
            pltpu.make_async_copy(u, gu.at[b, :, pl.ds(unit, unit)], sems.at[3 * b + 1]),
            pltpu.make_async_copy(d, down.at[pl.ds(b * unit, unit), :], sems.at[3 * b + 2]),
        )

    copies = [loads(b) for b in range(n)]
    gates = [c for block in copies for c in block[:2]]
    downs = [block[2] for block in copies]
    queue = gates + downs
    ahead = 4
    for c in queue[:ahead]:
        c.start()
    for b in range(n):
        for k in (2 * b, 2 * b + 1):
            queue[k].wait()
            queue[k + ahead].start()
        both = jnp.dot(x_ref[...], gu[b], preferred_element_type=F32)
        hid[:, b * unit : (b + 1) * unit] = (
            jax.nn.gelu(both[:, :unit], approximate=True) * both[:, unit:]
        ).astype(BF)
    for c in queue[2 * n + ahead :]:
        c.start()
    for c in downs:
        c.wait()
    cols = 512

    @pl.loop(0, out_ref.shape[1] // cols)
    def _(k):
        at = pl.ds(pl.multiple_of(k * cols, cols), cols)
        out_ref[:, at] = jnp.dot(
            hid[...], down[:, at], preferred_element_type=F32
        ).astype(BF)


def ffn(x, weights):
    n = len(weights)
    rows, d = x.shape
    unit = weights[0][0].shape[1]
    vmem = pl.BlockSpec(memory_space=pltpu.VMEM)
    return pl.pallas_call(
        ffn_kernel,
        in_specs=[vmem] + [pl.BlockSpec(memory_space=pl.ANY)] * (3 * n),
        out_specs=vmem,
        out_shape=jax.ShapeDtypeStruct((rows, d), BF),
        scratch_shapes=[
            pltpu.VMEM((n, d, 2 * unit), BF),
            pltpu.VMEM((n * unit, d), BF),
            pltpu.VMEM((rows, n * unit), BF),
            pltpu.SemaphoreType.DMA((3 * n,)),
        ],
        compiler_params=params(60),
        cost_estimate=cost(8),
        name="ffn",
    )(x, *[a for block in weights for a in block])


def finish_kernel(parts_ref, stream_ref, out_ref):
    total = parts_ref[0].astype(F32)
    for k in range(1, parts_ref.shape[0]):
        total += parts_ref[k].astype(F32)
    out_ref[...] = (stream_ref[...] + total).astype(BF)


def finish(parts, stream):
    vmem = pl.BlockSpec(memory_space=pltpu.VMEM)
    return pl.pallas_call(
        finish_kernel,
        in_specs=[vmem, vmem],
        out_specs=vmem,
        out_shape=jax.ShapeDtypeStruct(stream.shape, BF),
        compiler_params=params(4),
        cost_estimate=cost(2),
        name="finish",
    )(parts, stream)


def assemble_kernel(half_ref, mine_ref, peer_ref, out_ref):
    rows = mine_ref.shape[1]
    for ref, h in ((mine_ref, half_ref[0]), (peer_ref, 1 - half_ref[0])):
        out_ref[:, pl.ds(pl.multiple_of(h * rows, rows), rows), :] = ref[...]


def assemble(half, mine, peer):
    pages, rows, width = mine.shape
    block = 8
    spec = pl.BlockSpec((block, rows, width), lambda i, *_: (i, 0, 0))
    return pl.pallas_call(
        assemble_kernel,
        grid_spec=pltpu.PrefetchScalarGridSpec(
            num_scalar_prefetch=1,
            grid=(pages // block,),
            in_specs=[spec, spec],
            out_specs=pl.BlockSpec((block, 2 * rows, width), lambda i, *_: (i, 0, 0)),
        ),
        out_shape=jax.ShapeDtypeStruct((pages, 2 * rows, width), mine.dtype),
        compiler_params=params(8),
        cost_estimate=cost(6),
        name="assemble",
    )(half, mine, peer)


def step(
    page_pool, move_count, send_slots, page_table, history_len, queries, new_entry, residual,
    out_proj, ffn_gain, gate_proj, up_proj, down_proj,
):
    axes = ("dp", "mp")
    n_dp, n_mp = lax.axis_size("dp"), lax.axis_size("mp")
    devices = n_dp * n_mp
    games, heads, hd = queries.shape
    page_len, width = page_pool.shape[1:]
    mine = lax.axis_index("mp").reshape(1)
    half = mine % 2
    swap = lambda bit: [(k, k ^ bit) for k in range(devices)]
    send = lambda a, pairs: lax.ppermute(a, axes, pairs)
    core, side, far = swap(1), swap(2), swap(6)
    every = range(devices)
    groups = [
        [k for k in every if k % 2 == c and ((k >> 1) ^ (k >> 2)) % 2 == w]
        for w in range(2)
        for c in range(2)
    ]
    planes = [[k for k in every if k % 8 == z] for z in range(8)]
    peers = len(planes[0])
    exchange = lambda a, who: lax.all_to_all(
        a, axes, 0, 0, tiled=True, axis_index_groups=who
    )

    out_pages = outgoing_pages(half, send_slots, move_count.reshape(-1), page_pool)
    got = exchange(
        out_pages.reshape(n_dp, -1, page_len // 2, width), groups
    ).reshape(out_pages.shape)

    q_mine = (queries.transpose(1, 0, 2) * jnp.asarray(hd**-0.5, BF)).reshape(
        heads * games, hd
    )
    q_peer = send(q_mine, core)
    copies = 2 * heads
    table = jnp.tile(page_table.T, (1, copies))
    lengths = jnp.tile(history_len[None, :], (1, copies))

    weights = (gate_proj, up_proj, down_proj)
    each = lambda ws, pairs: tuple(send(a, pairs) for a in ws)
    w_side = each(weights, side)
    w_core = each(weights, core)
    w_side_core = each(w_side, core)
    far_up, far_down, far_gate = (send(weights[k], far) for k in (1, 2, 0))
    w_far = (far_gate, far_up, far_down)
    diag_gate = send(w_side[0], far)
    diag_up = send(far_up, side)
    diag_down = send(far_down, side)
    w_diag = (diag_gate, diag_up, diag_down)
    w_far_core = each(w_far, core)
    w_diag_core = each(w_diag, core)
    blocks = [
        weights, w_core, w_side, w_side_core, w_far, w_far_core, w_diag, w_diag_core
    ]

    acc, stat, qt = resident(half, q_mine, q_peer, new_entry, table, lengths, page_pool)
    keep, give = moved(half, qt, table, lengths, acc, stat, got)
    other = send(give, core)
    got_peer = send(got, core)
    hold, pass_on = project(mine, keep, other, out_proj, games)
    hold_got = send(pass_on, core)
    side_got = send(hold[1] + hold_got[1], side)
    arrived = assemble(half, got, got_peer)

    spread, stream = norm(
        mine, hold, hold_got, side_got, residual, ffn_gain.reshape(1, -1), peers
    )
    rows, d = stream.shape
    x = exchange(spread, planes)
    parts = ffn(x.reshape(peers * rows, d), blocks)
    back = exchange(parts.reshape(peers, rows, d), planes)
    quarter = finish(back, stream)
    layer_out = lax.all_gather(quarter, "mp", axis=0, tiled=True)
    return arrived, layer_out


def solution(mesh):
    in_specs = (
        P("dp", None, None),
        P("dp", None),
        P("dp", None),
        P("dp", None),
        P("dp"),
        P("dp", "mp", None),
        P("dp", None),
        P("dp", None),
        P("mp", None),
        P(),
        P(None, ("dp", "mp")),
        P(None, ("dp", "mp")),
        P(("dp", "mp"), None),
    )
    out_specs = (P("dp", None, None), P("dp", None))
    return jax.shard_map(
        step, mesh=mesh, in_specs=in_specs, out_specs=out_specs, check_vma=False
    )
```

```python
import jax
import jax.numpy as jnp
from jax import lax
from jax.experimental import pallas as pl
from jax.experimental.pallas import tpu as pltpu
from jax.sharding import PartitionSpec as P


NEG = -1e30
BF = jnp.bfloat16
F32 = jnp.float32


def params(mib):
    return pltpu.CompilerParams(vmem_limit_bytes=mib * 1024 * 1024)


def cost(us):
    return pl.CostEstimate(flops=int(us * 4e8), bytes_accessed=int(us * 2e6), transcendentals=0)


def outgoing_kernel(half_ref, slot_ref, count_ref, pool_ref, out_ref, sems):
    pages, rows, _ = out_ref.shape
    caps = pages // count_ref.shape[0]
    first = pl.multiple_of(half_ref[0] * rows, rows)

    def copy(i):
        src = pool_ref.at[slot_ref[i // caps, i % caps], pl.ds(first, rows), :]
        return pltpu.make_async_copy(src, out_ref.at[i], sems.at[i])

    copies = [copy(i) for i in range(pages)]
    for c in copies:
        c.start()
    for i, c in enumerate(copies):
        c.wait()

        @pl.when(i % caps >= count_ref[i // caps])
        def _():
            out_ref[i] = jnp.zeros(out_ref.shape[1:], out_ref.dtype)


def outgoing_pages(half, slots, counts, pool):
    pages = slots.size
    rows = pool.shape[1] // 2
    return pl.pallas_call(
        outgoing_kernel,
        grid_spec=pltpu.PrefetchScalarGridSpec(
            num_scalar_prefetch=3,
            grid=(1,),
            in_specs=[pl.BlockSpec(memory_space=pltpu.HBM)],
            out_specs=pl.BlockSpec((pages, rows, pool.shape[2]), lambda i, *_: (0, 0, 0)),
            scratch_shapes=[pltpu.SemaphoreType.DMA((pages,))],
        ),
        out_shape=jax.ShapeDtypeStruct((pages, rows, pool.shape[2]), pool.dtype),
        compiler_params=params(60),
        cost_estimate=cost(3),
        name="outgoing",
    )(half, slots, counts, pool)


def chunk_step(block, base, qt, full, part, acc, stat):
    pages, rows, width = block.shape
    hd = width // 2
    lanes = qt.shape[1]
    keys = block[:, :, :hd].reshape(pages * rows, hd)
    values = block[:, :, hd:].reshape(pages * rows, hd)
    s = jnp.dot(keys, qt[...], preferred_element_type=F32)
    spot = lax.broadcasted_iota(jnp.int32, (rows, lanes), 0)
    old = stat[0:1, :]
    tops = jnp.full((8, lanes), NEG, F32)
    counts = []
    masked = []
    for j in range(pages):
        c = full[pl.ds(base + j, 1), :] + jnp.where(
            spot < part[pl.ds(base + j, 1), :], 1.0, 0.0
        )
        sj = jnp.where(c > 0.0, s[j * rows : (j + 1) * rows, :], NEG)
        tops = jnp.maximum(tops, jnp.max(sj.reshape(rows // 8, 8, lanes), axis=0))
        counts.append(c)
        masked.append(sj)
    top = jnp.maximum(old, jnp.max(tops, axis=0, keepdims=True))
    shrink = jnp.exp(old - top)
    sums = jnp.zeros((8, lanes), F32)
    probs = []
    for j in range(pages):
        p = jnp.exp(masked[j] - top) * counts[j]
        sums += jnp.sum(p.reshape(rows // 8, 8, lanes), axis=0)
        probs.append(p.astype(BF))
    p = jnp.concatenate(probs, axis=0)
    stat[0:1, :] = top
    stat[1:2, :] = stat[1:2, :] * shrink + jnp.sum(sums, axis=0, keepdims=True)
    acc[...] = acc[...] * shrink + lax.dot_general(
        values, p, (((0,), (0,)), ((), ())), preferred_element_type=F32
    )


def tables(first, half, rows, tab_ref, len_ref, full, part):
    entries, lanes = full.shape
    page_id = lax.broadcasted_iota(jnp.int32, (entries, lanes), 0) + first
    whole = jnp.zeros((entries, lanes), F32)
    rest = jnp.zeros((entries, lanes), jnp.int32)
    for j in range(tab_ref.shape[0]):
        hit = page_id == tab_ref[j : j + 1, :]
        kept = len_ref[...] - j * 2 * rows
        whole += jnp.where(hit & (kept >= 2 * rows), 1.0, 0.0)
        rest += jnp.where(hit & (kept > 0) & (kept < 2 * rows), kept, 0)
    full[...] = whole
    part[...] = rest - half * rows


def resident_kernel(
    half_ref, qa_ref, qb_ref, entry_ref, tab_ref, len_ref, pool_ref,
    acc_ref, stat_ref, qt_ref, full, part, held, sems,
):
    i = pl.program_id(0)
    steps = sems.shape[0]
    slots, rows, width = held.shape
    pages = slots // steps
    hd = width // 2
    first = pl.multiple_of(half_ref[0] * rows, rows)

    def load(k):
        at = pl.ds(k * pages, pages)
        return pltpu.make_async_copy(
            pool_ref.at[at, pl.ds(first, rows), :], held.at[at], sems.at[k]
        )

    mine = qa_ref.shape[0]
    games = entry_ref.shape[0]

    @pl.when(i == 0)
    def _():
        for k in range(steps):
            load(k).start()
        q = jnp.concatenate([qa_ref[...], qb_ref[...]], axis=0)
        qt_ref[...] = q.T
        tables(0, half_ref[0], rows, tab_ref, len_ref, full, part)
        s = jnp.dot(entry_ref[:, :hd], qt_ref[...], preferred_element_type=F32)
        game = lax.broadcasted_iota(jnp.int32, s.shape, 0)
        lane = lax.broadcasted_iota(jnp.int32, s.shape, 1)
        own = (lane < mine) & (lax.rem(lane, games) == game)
        p = jnp.where(own, 1.0, 0.0)
        stat_ref[...] = jnp.zeros(stat_ref.shape, F32)
        stat_ref[0:1, :] = jnp.max(jnp.where(own, s, NEG), axis=0, keepdims=True)
        stat_ref[1:2, :] = jnp.sum(p, axis=0, keepdims=True)
        acc_ref[...] = lax.dot_general(
            entry_ref[:, hd:], p.astype(BF), (((0,), (0,)), ((), ())), preferred_element_type=F32
        )

    load(i).wait()
    at = pl.ds(pl.multiple_of(i * pages, pages), pages)
    chunk_step(held.at[at], i * pages, qt_ref, full, part, acc_ref, stat_ref)


def resident(half, q_mine, q_peer, entry, table, lengths, pool):
    slots, page_len, width = pool.shape
    rows = page_len // 2
    mine, hd = q_mine.shape
    lanes = 2 * mine
    block = 16
    whole = lambda shape: pl.BlockSpec(shape, lambda i, *_: (0,) * len(shape))
    outs = [
        jax.ShapeDtypeStruct((hd, lanes), F32),
        jax.ShapeDtypeStruct((8, lanes), F32),
        jax.ShapeDtypeStruct((hd, lanes), BF),
    ]
    return pl.pallas_call(
        resident_kernel,
        grid_spec=pltpu.PrefetchScalarGridSpec(
            num_scalar_prefetch=1,
            grid=(slots // block,),
            in_specs=[
                whole(q_mine.shape),
                whole(q_peer.shape),
                whole(entry.shape),
                whole(table.shape),
                whole(lengths.shape),
                pl.BlockSpec(memory_space=pltpu.HBM),
            ],
            out_specs=[whole(o.shape) for o in outs],
            scratch_shapes=[
                pltpu.VMEM((slots, lanes), F32),
                pltpu.VMEM((slots, lanes), jnp.int32),
                pltpu.VMEM((slots, rows, width), BF),
                pltpu.SemaphoreType.DMA((slots // block,)),
            ],
        ),
        out_shape=outs,
        compiler_params=params(48),
        cost_estimate=cost(8),
        name="resident",
    )(half, q_mine, q_peer, entry, table, lengths, pool)


def moved_kernel(
    half_ref, qt_ref, tab_ref, len_ref, acc_in, stat_in, got_ref,
    keep_ref, send_ref, acc, stat, full, part,
):
    i = pl.program_id(0)
    pages, rows, width = got_ref.shape
    hd = width // 2
    mine = qt_ref.shape[1] // 2

    @pl.when(i == 0)
    def _():
        tables(full.shape[0], half_ref[0], rows, tab_ref, len_ref, full, part)
        acc[...] = acc_in[...]
        stat[...] = stat_in[...]

    chunk_step(got_ref, i * pages, qt_ref, full, part, acc, stat)

    @pl.when(i == pl.num_programs(0) - 1)
    def _():
        for k, out in enumerate((keep_ref, send_ref)):
            out[:hd, :] = acc[:, k * mine : (k + 1) * mine]
            out[hd : hd + 8, :] = stat[:, k * mine : (k + 1) * mine]


def moved(half, qt, table, lengths, acc, stat, got):
    slots, rows, width = got.shape
    hd, lanes = qt.shape
    block = 16
    whole = lambda shape: pl.BlockSpec(shape, lambda i, *_: (0,) * len(shape))
    out = jax.ShapeDtypeStruct((hd + 8, lanes // 2), F32)
    return pl.pallas_call(
        moved_kernel,
        grid_spec=pltpu.PrefetchScalarGridSpec(
            num_scalar_prefetch=1,
            grid=(slots // block,),
            in_specs=[
                whole(qt.shape),
                whole(table.shape),
                whole(lengths.shape),
                whole(acc.shape),
                whole(stat.shape),
                pl.BlockSpec((block, rows, width), lambda i, *_: (i, 0, 0)),
            ],
            out_specs=[whole(out.shape), whole(out.shape)],
            scratch_shapes=[
                pltpu.VMEM((hd, lanes), F32),
                pltpu.VMEM((8, lanes), F32),
                pltpu.VMEM((slots, lanes), F32),
                pltpu.VMEM((slots, lanes), jnp.int32),
            ],
        ),
        out_shape=[out, out],
        compiler_params=params(40),
        cost_estimate=cost(8),
        name="moved",
    )(half, qt, table, lengths, acc, stat, got)


def project_kernel(mine_ref, a_ref, b_ref, w_ref, keep_ref, send_ref, scratch):
    hd = a_ref.shape[0] - 8
    ma, mb = a_ref[hd : hd + 1, :], b_ref[hd : hd + 1, :]
    top = jnp.maximum(ma, mb)
    wa, wb = jnp.exp(ma - top), jnp.exp(mb - top)
    den = a_ref[hd + 1 : hd + 2, :] * wa + b_ref[hd + 1 : hd + 2, :] * wb
    att = (a_ref[:hd, :] * wa + b_ref[:hd, :] * wb) / den
    att = att.T.astype(BF)
    games = scratch.shape[0]
    out = jnp.zeros(scratch.shape, F32)
    for h in range(att.shape[0] // games):
        out += jnp.dot(
            att[h * games : (h + 1) * games, :],
            w_ref[h * hd : (h + 1) * hd, :],
            preferred_element_type=F32,
        )
    scratch[...] = out
    rows = keep_ref.shape[1]
    m = mine_ref[0]
    core = lax.rem(m, 2)
    side = m // 2
    for ref, c in ((keep_ref, core), (send_ref, 1 - core)):
        for k, z in enumerate((side, 1 - side)):
            first = pl.multiple_of((z * 2 + c) * rows, rows)
            ref[k] = scratch[pl.ds(first, rows), :]


def project(mine, a, b, w, games):
    rows = games // 4
    whole = lambda shape: pl.BlockSpec(shape, lambda i, *_: (0,) * len(shape))
    out = jax.ShapeDtypeStruct((2, rows, w.shape[1]), F32)
    return pl.pallas_call(
        project_kernel,
        grid_spec=pltpu.PrefetchScalarGridSpec(
            num_scalar_prefetch=1,
            grid=(1,),
            in_specs=[whole(a.shape), whole(b.shape), whole(w.shape)],
            out_specs=[whole(out.shape), whole(out.shape)],
            scratch_shapes=[pltpu.VMEM((games, w.shape[1]), F32)],
        ),
        out_shape=[out, out],
        compiler_params=params(10),
        cost_estimate=cost(3),
        name="project",
    )(mine, a, b, w)


def norm_kernel(mine_ref, keep_ref, got_ref, side_ref, res_ref, gain_ref, copies_ref, stream_ref):
    stream = res_ref[...].astype(F32) + ((keep_ref[0] + got_ref[0]) + side_ref[...])
    scale = lax.rsqrt(jnp.mean(stream * stream, axis=-1, keepdims=True) + 1e-06)
    normed = (stream * scale * (1.0 + gain_ref[...])).astype(BF)
    stream_ref[...] = stream
    for k in range(copies_ref.shape[0]):
        copies_ref[k] = normed


def norm(mine, keep, got, side, residual, gain, peers):
    _, rows, d = keep.shape
    whole = lambda shape: pl.BlockSpec(shape, lambda i, *_: (0,) * len(shape))
    outs = [
        jax.ShapeDtypeStruct((peers, rows, d), BF),
        jax.ShapeDtypeStruct((rows, d), F32),
    ]
    return pl.pallas_call(
        norm_kernel,
        grid_spec=pltpu.PrefetchScalarGridSpec(
            num_scalar_prefetch=1,
            grid=(1,),
            in_specs=[
                pl.BlockSpec((1, rows, d), lambda i, *_: (0, 0, 0)),
                pl.BlockSpec((1, rows, d), lambda i, *_: (0, 0, 0)),
                whole(side.shape),
                pl.BlockSpec((rows, d), lambda i, m: (m[0], 0)),
                whole(gain.shape),
            ],
            out_specs=[whole(o.shape) for o in outs],
        ),
        out_shape=outs,
        compiler_params=params(6),
        cost_estimate=cost(2),
        name="norm",
    )(mine, keep, got, side, residual, gain)


def ffn_kernel(*refs):
    n = (len(refs) - 3) // 3
    x_ref = refs[0]
    w = [refs[1 + 3 * b : 4 + 3 * b] for b in range(n)]
    out_ref, hid = refs[1 + 3 * n :]
    unit = w[0][0].shape[1]
    for b, (g, u, _) in enumerate(w):
        both = jnp.dot(
            x_ref[...], jnp.concatenate([g[...], u[...]], axis=1), preferred_element_type=F32
        )
        hid[:, b * unit : (b + 1) * unit] = (
            jax.nn.gelu(both[:, :unit], approximate=True) * both[:, unit:]
        ).astype(BF)
    cols = 512

    @pl.loop(0, out_ref.shape[1] // cols)
    def _(k):
        at = pl.ds(pl.multiple_of(k * cols, cols), cols)
        down = jnp.concatenate([d[:, at] for _, _, d in w], axis=0)
        out_ref[:, at] = jnp.dot(hid[...], down, preferred_element_type=F32).astype(BF)


def ffn(x, weights):
    n = len(weights)
    rows, d = x.shape
    unit = weights[0][0].shape[1]
    vmem = pl.BlockSpec(memory_space=pltpu.VMEM)
    return pl.pallas_call(
        ffn_kernel,
        in_specs=[vmem] * (1 + 3 * n),
        out_specs=vmem,
        out_shape=jax.ShapeDtypeStruct((rows, d), BF),
        scratch_shapes=[pltpu.VMEM((rows, n * unit), BF)],
        compiler_params=params(24),
        cost_estimate=cost(8),
        name="ffn",
    )(x, *[a for block in weights for a in block])


def finish_kernel(parts_ref, stream_ref, out_ref):
    total = parts_ref[0].astype(F32)
    for k in range(1, parts_ref.shape[0]):
        total += parts_ref[k].astype(F32)
    out_ref[...] = (stream_ref[...] + total).astype(BF)


def finish(parts, stream):
    vmem = pl.BlockSpec(memory_space=pltpu.VMEM)
    return pl.pallas_call(
        finish_kernel,
        in_specs=[vmem, vmem],
        out_specs=vmem,
        out_shape=jax.ShapeDtypeStruct(stream.shape, BF),
        compiler_params=params(4),
        cost_estimate=cost(2),
        name="finish",
    )(parts, stream)


def assemble_kernel(half_ref, mine_ref, peer_ref, out_ref):
    rows = mine_ref.shape[1]
    for ref, h in ((mine_ref, half_ref[0]), (peer_ref, 1 - half_ref[0])):
        out_ref[:, pl.ds(pl.multiple_of(h * rows, rows), rows), :] = ref[...]


def assemble(half, mine, peer):
    pages, rows, width = mine.shape
    block = 8
    spec = pl.BlockSpec((block, rows, width), lambda i, *_: (i, 0, 0))
    return pl.pallas_call(
        assemble_kernel,
        grid_spec=pltpu.PrefetchScalarGridSpec(
            num_scalar_prefetch=1,
            grid=(pages // block,),
            in_specs=[spec, spec],
            out_specs=pl.BlockSpec((block, 2 * rows, width), lambda i, *_: (i, 0, 0)),
        ),
        out_shape=jax.ShapeDtypeStruct((pages, 2 * rows, width), mine.dtype),
        compiler_params=params(8),
        cost_estimate=cost(6),
        name="assemble",
    )(half, mine, peer)


def step(
    page_pool, move_count, send_slots, page_table, history_len, queries, new_entry, residual,
    out_proj, ffn_gain, gate_proj, up_proj, down_proj,
):
    axes = ("dp", "mp")
    n_dp, n_mp = lax.axis_size("dp"), lax.axis_size("mp")
    devices = n_dp * n_mp
    games, heads, hd = queries.shape
    page_len, width = page_pool.shape[1:]
    mine = lax.axis_index("mp").reshape(1)
    half = mine % 2
    swap = lambda bit: [(k, k ^ bit) for k in range(devices)]
    send = lambda a, pairs: lax.ppermute(a, axes, pairs)
    core, side, far = swap(1), swap(2), swap(6)
    every = range(devices)
    groups = [
        [k for k in every if k % 2 == c and ((k >> 1) ^ (k >> 2)) % 2 == w]
        for w in range(2)
        for c in range(2)
    ]
    planes = [[k for k in every if k % 8 == z] for z in range(8)]
    peers = len(planes[0])
    exchange = lambda a, who: lax.all_to_all(
        a, axes, 0, 0, tiled=True, axis_index_groups=who
    )

    out_pages = outgoing_pages(half, send_slots, move_count.reshape(-1), page_pool)
    got = exchange(
        out_pages.reshape(n_dp, -1, page_len // 2, width), groups
    ).reshape(out_pages.shape)

    q_mine = (queries.transpose(1, 0, 2) * jnp.asarray(hd**-0.5, BF)).reshape(
        heads * games, hd
    )
    q_peer = send(q_mine, core)
    copies = 2 * heads
    table = jnp.tile(page_table.T, (1, copies))
    lengths = jnp.tile(history_len[None, :], (1, copies))

    weights = (gate_proj, up_proj, down_proj)
    each = lambda ws, pairs: tuple(send(a, pairs) for a in ws)
    w_side = each(weights, side)
    w_core = each(weights, core)
    w_side_core = each(w_side, core)
    far_up, far_down, far_gate = (send(weights[k], far) for k in (1, 2, 0))
    w_far = (far_gate, far_up, far_down)
    diag_gate = send(w_side[0], far)
    diag_up = send(far_up, side)
    diag_down = send(far_down, side)
    w_diag = (diag_gate, diag_up, diag_down)
    w_far_core = each(w_far, core)
    w_diag_core = each(w_diag, core)
    blocks = [
        weights, w_core, w_side, w_side_core, w_far, w_far_core, w_diag, w_diag_core
    ]

    acc, stat, qt = resident(half, q_mine, q_peer, new_entry, table, lengths, page_pool)
    keep, give = moved(half, qt, table, lengths, acc, stat, got)
    other = send(give, core)
    got_peer = send(got, core)
    hold, pass_on = project(mine, keep, other, out_proj, games)
    hold_got = send(pass_on, core)
    side_got = send(hold[1] + hold_got[1], side)
    arrived = assemble(half, got, got_peer)

    spread, stream = norm(
        mine, hold, hold_got, side_got, residual, ffn_gain.reshape(1, -1), peers
    )
    rows, d = stream.shape
    x = exchange(spread, planes)
    parts = ffn(x.reshape(peers * rows, d), blocks)
    back = exchange(parts.reshape(peers, rows, d), planes)
    quarter = finish(back, stream)
    layer_out = lax.all_gather(quarter, "mp", axis=0, tiled=True)
    return arrived, layer_out


def solution(mesh):
    in_specs = (
        P("dp", None, None),
        P("dp", None),
        P("dp", None),
        P("dp", None),
        P("dp"),
        P("dp", "mp", None),
        P("dp", None),
        P("dp", None),
        P("mp", None),
        P(),
        P(None, ("dp", "mp")),
        P(None, ("dp", "mp")),
        P(("dp", "mp"), None),
    )
    out_specs = (P("dp", None, None), P("dp", None))
    return jax.shard_map(
        step, mesh=mesh, in_specs=in_specs, out_specs=out_specs, check_vma=False
    )
```

```python
import jax
import jax.numpy as jnp
from jax import lax
from jax.experimental import pallas as pl
from jax.experimental.pallas import tpu as pltpu
from jax.sharding import PartitionSpec as P


NEG = -1e30
BF = jnp.bfloat16
F32 = jnp.float32


def params(mib):
    return pltpu.CompilerParams(vmem_limit_bytes=mib * 1024 * 1024)


def cost(us):
    return pl.CostEstimate(flops=int(us * 4e8), bytes_accessed=int(us * 2e6), transcendentals=0)


def outgoing_kernel(half_ref, slot_ref, count_ref, pool_ref, out_ref, sems):
    pages, rows, _ = out_ref.shape
    caps = pages // count_ref.shape[0]
    first = pl.multiple_of(half_ref[0] * rows, rows)

    def copy(i):
        src = pool_ref.at[slot_ref[i // caps, i % caps], pl.ds(first, rows), :]
        return pltpu.make_async_copy(src, out_ref.at[i], sems.at[i])

    copies = [copy(i) for i in range(pages)]
    for c in copies:
        c.start()
    for i, c in enumerate(copies):
        c.wait()

        @pl.when(i % caps >= count_ref[i // caps])
        def _():
            out_ref[i] = jnp.zeros(out_ref.shape[1:], out_ref.dtype)


def outgoing_pages(half, slots, counts, pool):
    pages = slots.size
    rows = pool.shape[1] // 2
    return pl.pallas_call(
        outgoing_kernel,
        grid_spec=pltpu.PrefetchScalarGridSpec(
            num_scalar_prefetch=3,
            grid=(1,),
            in_specs=[pl.BlockSpec(memory_space=pltpu.HBM)],
            out_specs=pl.BlockSpec((pages, rows, pool.shape[2]), lambda i, *_: (0, 0, 0)),
            scratch_shapes=[pltpu.SemaphoreType.DMA((pages,))],
        ),
        out_shape=jax.ShapeDtypeStruct((pages, rows, pool.shape[2]), pool.dtype),
        compiler_params=params(60),
        cost_estimate=cost(3),
        name="outgoing",
    )(half, slots, counts, pool)


def chunk_step(block, base, qt, full, part, acc, stat):
    pages, rows, width = block.shape
    hd = width // 2
    lanes = qt.shape[1]
    keys = block[:, :, :hd].reshape(pages * rows, hd)
    values = block[:, :, hd:].reshape(pages * rows, hd)
    s = jnp.dot(keys, qt[...], preferred_element_type=F32)
    spot = lax.broadcasted_iota(jnp.int32, (rows, lanes), 0)
    old = stat[0:1, :]
    tops = jnp.full((8, lanes), NEG, F32)
    counts = []
    masked = []
    for j in range(pages):
        c = full[pl.ds(base + j, 1), :] + jnp.where(
            spot < part[pl.ds(base + j, 1), :], 1.0, 0.0
        )
        sj = jnp.where(c > 0.0, s[j * rows : (j + 1) * rows, :], NEG)
        tops = jnp.maximum(tops, jnp.max(sj.reshape(rows // 8, 8, lanes), axis=0))
        counts.append(c)
        masked.append(sj)
    top = jnp.maximum(old, jnp.max(tops, axis=0, keepdims=True))
    shrink = jnp.exp(old - top)
    sums = jnp.zeros((8, lanes), F32)
    probs = []
    for j in range(pages):
        p = jnp.exp(masked[j] - top) * counts[j]
        sums += jnp.sum(p.reshape(rows // 8, 8, lanes), axis=0)
        probs.append(p.astype(BF))
    p = jnp.concatenate(probs, axis=0)
    stat[0:1, :] = top
    stat[1:2, :] = stat[1:2, :] * shrink + jnp.sum(sums, axis=0, keepdims=True)
    acc[...] = acc[...] * shrink + lax.dot_general(
        values, p, (((0,), (0,)), ((), ())), preferred_element_type=F32
    )


def tables(first, half, rows, tab_ref, len_ref, full, part):
    entries, lanes = full.shape
    page_id = lax.broadcasted_iota(jnp.int32, (entries, lanes), 0) + first
    whole = jnp.zeros((entries, lanes), F32)
    rest = jnp.zeros((entries, lanes), jnp.int32)
    for j in range(tab_ref.shape[0]):
        hit = page_id == tab_ref[j : j + 1, :]
        kept = len_ref[...] - j * 2 * rows
        whole += jnp.where(hit & (kept >= 2 * rows), 1.0, 0.0)
        rest += jnp.where(hit & (kept > 0) & (kept < 2 * rows), kept, 0)
    full[...] = whole
    part[...] = rest - half * rows


def resident_kernel(
    half_ref, qa_ref, qb_ref, entry_ref, tab_ref, len_ref, pool_ref,
    acc_ref, stat_ref, qt_ref, full, part, held, sems,
):
    i = pl.program_id(0)
    steps = sems.shape[0]
    slots, rows, width = held.shape
    pages = slots // steps
    hd = width // 2
    first = pl.multiple_of(half_ref[0] * rows, rows)

    def load(k):
        at = pl.ds(k * pages, pages)
        return pltpu.make_async_copy(
            pool_ref.at[at, pl.ds(first, rows), :], held.at[at], sems.at[k]
        )

    mine = qa_ref.shape[0]
    games = entry_ref.shape[0]

    @pl.when(i == 0)
    def _():
        for k in range(steps):
            load(k).start()
        q = jnp.concatenate([qa_ref[...], qb_ref[...]], axis=0)
        qt_ref[...] = q.T
        tables(0, half_ref[0], rows, tab_ref, len_ref, full, part)
        s = jnp.dot(entry_ref[:, :hd], qt_ref[...], preferred_element_type=F32)
        game = lax.broadcasted_iota(jnp.int32, s.shape, 0)
        lane = lax.broadcasted_iota(jnp.int32, s.shape, 1)
        own = (lane < mine) & (lax.rem(lane, games) == game)
        p = jnp.where(own, 1.0, 0.0)
        stat_ref[...] = jnp.zeros(stat_ref.shape, F32)
        stat_ref[0:1, :] = jnp.max(jnp.where(own, s, NEG), axis=0, keepdims=True)
        stat_ref[1:2, :] = jnp.sum(p, axis=0, keepdims=True)
        acc_ref[...] = lax.dot_general(
            entry_ref[:, hd:], p.astype(BF), (((0,), (0,)), ((), ())), preferred_element_type=F32
        )

    load(i).wait()
    at = pl.ds(pl.multiple_of(i * pages, pages), pages)
    chunk_step(held.at[at], i * pages, qt_ref, full, part, acc_ref, stat_ref)


def resident(half, q_mine, q_peer, entry, table, lengths, pool):
    slots, page_len, width = pool.shape
    rows = page_len // 2
    mine, hd = q_mine.shape
    lanes = 2 * mine
    block = 16
    whole = lambda shape: pl.BlockSpec(shape, lambda i, *_: (0,) * len(shape))
    outs = [
        jax.ShapeDtypeStruct((hd, lanes), F32),
        jax.ShapeDtypeStruct((8, lanes), F32),
        jax.ShapeDtypeStruct((hd, lanes), BF),
    ]
    return pl.pallas_call(
        resident_kernel,
        grid_spec=pltpu.PrefetchScalarGridSpec(
            num_scalar_prefetch=1,
            grid=(slots // block,),
            in_specs=[
                whole(q_mine.shape),
                whole(q_peer.shape),
                whole(entry.shape),
                whole(table.shape),
                whole(lengths.shape),
                pl.BlockSpec(memory_space=pltpu.HBM),
            ],
            out_specs=[whole(o.shape) for o in outs],
            scratch_shapes=[
                pltpu.VMEM((slots, lanes), F32),
                pltpu.VMEM((slots, lanes), jnp.int32),
                pltpu.VMEM((slots, rows, width), BF),
                pltpu.SemaphoreType.DMA((slots // block,)),
            ],
        ),
        out_shape=outs,
        compiler_params=params(48),
        cost_estimate=cost(8),
        name="resident",
    )(half, q_mine, q_peer, entry, table, lengths, pool)


def moved_kernel(
    half_ref, qt_ref, tab_ref, len_ref, acc_in, stat_in, got_ref,
    keep_ref, send_ref, acc, stat, full, part,
):
    i = pl.program_id(0)
    pages, rows, width = got_ref.shape
    hd = width // 2
    mine = qt_ref.shape[1] // 2

    @pl.when(i == 0)
    def _():
        tables(full.shape[0], half_ref[0], rows, tab_ref, len_ref, full, part)
        acc[...] = acc_in[...]
        stat[...] = stat_in[...]

    chunk_step(got_ref, i * pages, qt_ref, full, part, acc, stat)

    @pl.when(i == pl.num_programs(0) - 1)
    def _():
        for k, out in enumerate((keep_ref, send_ref)):
            out[:hd, :] = acc[:, k * mine : (k + 1) * mine]
            out[hd : hd + 8, :] = stat[:, k * mine : (k + 1) * mine]


def moved(half, qt, table, lengths, acc, stat, got):
    slots, rows, width = got.shape
    hd, lanes = qt.shape
    block = 16
    whole = lambda shape: pl.BlockSpec(shape, lambda i, *_: (0,) * len(shape))
    out = jax.ShapeDtypeStruct((hd + 8, lanes // 2), F32)
    return pl.pallas_call(
        moved_kernel,
        grid_spec=pltpu.PrefetchScalarGridSpec(
            num_scalar_prefetch=1,
            grid=(slots // block,),
            in_specs=[
                whole(qt.shape),
                whole(table.shape),
                whole(lengths.shape),
                whole(acc.shape),
                whole(stat.shape),
                pl.BlockSpec((block, rows, width), lambda i, *_: (i, 0, 0)),
            ],
            out_specs=[whole(out.shape), whole(out.shape)],
            scratch_shapes=[
                pltpu.VMEM((hd, lanes), F32),
                pltpu.VMEM((8, lanes), F32),
                pltpu.VMEM((slots, lanes), F32),
                pltpu.VMEM((slots, lanes), jnp.int32),
            ],
        ),
        out_shape=[out, out],
        compiler_params=params(40),
        cost_estimate=cost(8),
        name="moved",
    )(half, qt, table, lengths, acc, stat, got)


def project_kernel(mine_ref, a_ref, b_ref, w_ref, keep_ref, send_ref, scratch):
    hd = a_ref.shape[0] - 8
    ma, mb = a_ref[hd : hd + 1, :], b_ref[hd : hd + 1, :]
    top = jnp.maximum(ma, mb)
    wa, wb = jnp.exp(ma - top), jnp.exp(mb - top)
    den = a_ref[hd + 1 : hd + 2, :] * wa + b_ref[hd + 1 : hd + 2, :] * wb
    att = (a_ref[:hd, :] * wa + b_ref[:hd, :] * wb) / den
    att = att.T.astype(BF)
    games = scratch.shape[0]
    out = jnp.zeros(scratch.shape, F32)
    for h in range(att.shape[0] // games):
        out += jnp.dot(
            att[h * games : (h + 1) * games, :],
            w_ref[h * hd : (h + 1) * hd, :],
            preferred_element_type=F32,
        )
    scratch[...] = out
    rows = keep_ref.shape[1]
    m = mine_ref[0]
    core = lax.rem(m, 2)
    side = m // 2
    for ref, c in ((keep_ref, core), (send_ref, 1 - core)):
        for k, z in enumerate((side, 1 - side)):
            first = pl.multiple_of((z * 2 + c) * rows, rows)
            ref[k] = scratch[pl.ds(first, rows), :]


def project(mine, a, b, w, games):
    rows = games // 4
    whole = lambda shape: pl.BlockSpec(shape, lambda i, *_: (0,) * len(shape))
    out = jax.ShapeDtypeStruct((2, rows, w.shape[1]), F32)
    return pl.pallas_call(
        project_kernel,
        grid_spec=pltpu.PrefetchScalarGridSpec(
            num_scalar_prefetch=1,
            grid=(1,),
            in_specs=[whole(a.shape), whole(b.shape), whole(w.shape)],
            out_specs=[whole(out.shape), whole(out.shape)],
            scratch_shapes=[pltpu.VMEM((games, w.shape[1]), F32)],
        ),
        out_shape=[out, out],
        compiler_params=params(10),
        cost_estimate=cost(3),
        name="project",
    )(mine, a, b, w)


def norm_kernel(mine_ref, keep_ref, got_ref, side_ref, res_ref, gain_ref, copies_ref, stream_ref):
    stream = res_ref[...].astype(F32) + ((keep_ref[0] + got_ref[0]) + side_ref[...])
    scale = lax.rsqrt(jnp.mean(stream * stream, axis=-1, keepdims=True) + 1e-06)
    normed = (stream * scale * (1.0 + gain_ref[...])).astype(BF)
    stream_ref[...] = stream
    for k in range(copies_ref.shape[0]):
        copies_ref[k] = normed


def norm(mine, keep, got, side, residual, gain, peers):
    _, rows, d = keep.shape
    whole = lambda shape: pl.BlockSpec(shape, lambda i, *_: (0,) * len(shape))
    outs = [
        jax.ShapeDtypeStruct((peers, rows, d), BF),
        jax.ShapeDtypeStruct((rows, d), F32),
    ]
    return pl.pallas_call(
        norm_kernel,
        grid_spec=pltpu.PrefetchScalarGridSpec(
            num_scalar_prefetch=1,
            grid=(1,),
            in_specs=[
                pl.BlockSpec((1, rows, d), lambda i, *_: (0, 0, 0)),
                pl.BlockSpec((1, rows, d), lambda i, *_: (0, 0, 0)),
                whole(side.shape),
                pl.BlockSpec((rows, d), lambda i, m: (m[0], 0)),
                whole(gain.shape),
            ],
            out_specs=[whole(o.shape) for o in outs],
        ),
        out_shape=outs,
        compiler_params=params(6),
        cost_estimate=cost(2),
        name="norm",
    )(mine, keep, got, side, residual, gain)


def ffn_kernel(*refs):
    n = (len(refs) - 3) // 3
    x_ref = refs[0]
    w = [refs[1 + 3 * b : 4 + 3 * b] for b in range(n)]
    out_ref, hid = refs[1 + 3 * n :]
    unit = w[0][0].shape[1]
    for b, (g, u, _) in enumerate(w):
        both = jnp.dot(
            x_ref[...], jnp.concatenate([g[...], u[...]], axis=1), preferred_element_type=F32
        )
        hid[:, b * unit : (b + 1) * unit] = (
            jax.nn.gelu(both[:, :unit], approximate=True) * both[:, unit:]
        ).astype(BF)
    cols = 512

    @pl.loop(0, out_ref.shape[1] // cols)
    def _(k):
        at = pl.ds(pl.multiple_of(k * cols, cols), cols)
        down = jnp.concatenate([d[:, at] for _, _, d in w], axis=0)
        out_ref[:, at] = jnp.dot(hid[...], down, preferred_element_type=F32).astype(BF)


def ffn(x, weights):
    n = len(weights)
    rows, d = x.shape
    unit = weights[0][0].shape[1]
    vmem = pl.BlockSpec(memory_space=pltpu.VMEM)
    return pl.pallas_call(
        ffn_kernel,
        in_specs=[vmem] * (1 + 3 * n),
        out_specs=vmem,
        out_shape=jax.ShapeDtypeStruct((rows, d), BF),
        scratch_shapes=[pltpu.VMEM((rows, n * unit), BF)],
        compiler_params=params(24),
        cost_estimate=cost(8),
        name="ffn",
    )(x, *[a for block in weights for a in block])


def finish_kernel(parts_ref, stream_ref, out_ref):
    total = parts_ref[0].astype(F32)
    for k in range(1, parts_ref.shape[0]):
        total += parts_ref[k].astype(F32)
    out_ref[...] = (stream_ref[...] + total).astype(BF)


def finish(parts, stream):
    vmem = pl.BlockSpec(memory_space=pltpu.VMEM)
    return pl.pallas_call(
        finish_kernel,
        in_specs=[vmem, vmem],
        out_specs=vmem,
        out_shape=jax.ShapeDtypeStruct(stream.shape, BF),
        compiler_params=params(4),
        cost_estimate=cost(2),
        name="finish",
    )(parts, stream)


def assemble_kernel(half_ref, mine_ref, peer_ref, out_ref):
    rows = mine_ref.shape[1]
    for ref, h in ((mine_ref, half_ref[0]), (peer_ref, 1 - half_ref[0])):
        out_ref[:, pl.ds(pl.multiple_of(h * rows, rows), rows), :] = ref[...]


def assemble(half, mine, peer):
    pages, rows, width = mine.shape
    block = 8
    spec = pl.BlockSpec((block, rows, width), lambda i, *_: (i, 0, 0))
    return pl.pallas_call(
        assemble_kernel,
        grid_spec=pltpu.PrefetchScalarGridSpec(
            num_scalar_prefetch=1,
            grid=(pages // block,),
            in_specs=[spec, spec],
            out_specs=pl.BlockSpec((block, 2 * rows, width), lambda i, *_: (i, 0, 0)),
        ),
        out_shape=jax.ShapeDtypeStruct((pages, 2 * rows, width), mine.dtype),
        compiler_params=params(8),
        cost_estimate=cost(6),
        name="assemble",
    )(half, mine, peer)


def step(
    page_pool, move_count, send_slots, page_table, history_len, queries, new_entry, residual,
    out_proj, ffn_gain, gate_proj, up_proj, down_proj,
):
    axes = ("dp", "mp")
    n_dp, n_mp = lax.axis_size("dp"), lax.axis_size("mp")
    devices = n_dp * n_mp
    games, heads, hd = queries.shape
    page_len, width = page_pool.shape[1:]
    mine = lax.axis_index("mp").reshape(1)
    half = mine % 2
    swap = lambda bit: [(k, k ^ bit) for k in range(devices)]
    send = lambda a, pairs: lax.ppermute(a, axes, pairs)
    core, side, far = swap(1), swap(2), swap(6)
    every = range(devices)
    groups = [
        [k for k in every if k % 2 == c and ((k >> 1) ^ (k >> 2)) % 2 == w]
        for w in range(2)
        for c in range(2)
    ]
    planes = [[k for k in every if k % 8 == z] for z in range(8)]
    peers = len(planes[0])
    exchange = lambda a, who: lax.all_to_all(
        a, axes, 0, 0, tiled=True, axis_index_groups=who
    )

    out_pages = outgoing_pages(half, send_slots, move_count.reshape(-1), page_pool)
    got = exchange(
        out_pages.reshape(n_dp, -1, page_len // 2, width), groups
    ).reshape(out_pages.shape)

    q_mine = (queries.transpose(1, 0, 2) * jnp.asarray(hd**-0.5, BF)).reshape(
        heads * games, hd
    )
    q_peer = send(q_mine, core)
    copies = 2 * heads
    table = jnp.tile(page_table.T, (1, copies))
    lengths = jnp.tile(history_len[None, :], (1, copies))

    weights = (gate_proj, up_proj, down_proj)
    each = lambda ws, pairs: tuple(send(a, pairs) for a in ws)
    w_side = each(weights, side)
    w_core = each(weights, core)
    w_side_core = each(w_side, core)
    far_up, far_down, far_gate = (send(weights[k], far) for k in (1, 2, 0))
    w_far = (far_gate, far_up, far_down)
    diag_gate = send(w_side[0], far)
    diag_up = send(far_up, side)
    diag_down = send(far_down, side)
    w_diag = (diag_gate, diag_up, diag_down)
    w_far_core = each(w_far, core)
    diag_core_gate = send(diag_gate, core)
    diag_core_up = send(diag_up, core)
    diag_core_down = send(diag_down, core)
    w_diag_core = (diag_core_gate, diag_core_up, diag_core_down)
    blocks = [
        weights, w_core, w_side, w_side_core, w_far, w_far_core, w_diag, w_diag_core
    ]

    acc, stat, qt = resident(half, q_mine, q_peer, new_entry, table, lengths, page_pool)
    keep, give = moved(half, qt, table, lengths, acc, stat, got)
    other = send(give, core)
    got_peer = send(got, core)
    hold, pass_on = project(mine, keep, other, out_proj, games)
    hold_got = send(pass_on, core)
    side_got = send(hold[1] + hold_got[1], side)
    arrived = assemble(half, got, got_peer)

    spread, stream = norm(
        mine, hold, hold_got, side_got, residual, ffn_gain.reshape(1, -1), peers
    )
    rows, d = stream.shape
    x = exchange(spread, planes)
    parts = ffn(x.reshape(peers * rows, d), blocks)
    back = exchange(parts.reshape(peers, rows, d), planes)
    quarter = finish(back, stream)
    layer_out = lax.all_gather(quarter, "mp", axis=0, tiled=True)
    return arrived, layer_out


def solution(mesh):
    in_specs = (
        P("dp", None, None),
        P("dp", None),
        P("dp", None),
        P("dp", None),
        P("dp"),
        P("dp", "mp", None),
        P("dp", None),
        P("dp", None),
        P("mp", None),
        P(),
        P(None, ("dp", "mp")),
        P(None, ("dp", "mp")),
        P(("dp", "mp"), None),
    )
    out_specs = (P("dp", None, None), P("dp", None))
    return jax.shard_map(
        step, mesh=mesh, in_specs=in_specs, out_specs=out_specs, check_vma=False
    )
```

```python
import jax
import jax.numpy as jnp
from jax import lax
from jax.experimental import pallas as pl
from jax.experimental.pallas import tpu as pltpu
from jax.sharding import PartitionSpec as P


NEG = -1e30
BF = jnp.bfloat16
F32 = jnp.float32


def params(mib):
    return pltpu.CompilerParams(vmem_limit_bytes=mib * 1024 * 1024)


def cost(us):
    return pl.CostEstimate(flops=int(us * 4e8), bytes_accessed=int(us * 2e6), transcendentals=0)


def outgoing_kernel(
    mine_ref, twist_ref, slot_ref, count_ref, pool_ref, a_ref, b_ref, sems
):
    pages, quarter, _ = a_ref.shape
    rest = b_ref.shape[1]
    caps = pages // count_ref.shape[0]
    core = lax.rem(mine_ref[0], 2)
    low = pl.multiple_of(4 * quarter + core * rest, rest)

    def copies(i):
        page = slot_ref[i // caps, i % caps]
        side = lax.rem(twist_ref[0] + (i // caps) % 2, 2)
        first = pl.multiple_of((2 * side + core) * quarter, quarter)
        return (
            pltpu.make_async_copy(
                pool_ref.at[page, pl.ds(first, quarter), :], a_ref.at[i], sems.at[2 * i]
            ),
            pltpu.make_async_copy(
                pool_ref.at[page, pl.ds(low, rest), :], b_ref.at[i], sems.at[2 * i + 1]
            ),
        )

    pending = [copies(i) for i in range(pages)]
    for pair in pending:
        for c in pair:
            c.start()
    for i, pair in enumerate(pending):
        for c in pair:
            c.wait()

        @pl.when(i % caps >= count_ref[i // caps])
        def _():
            a_ref[i] = jnp.zeros(a_ref.shape[1:], a_ref.dtype)
            b_ref[i] = jnp.zeros(b_ref.shape[1:], b_ref.dtype)


def outgoing_pages(mine, twist, slots, counts, pool):
    pages = slots.size
    page_len, width = pool.shape[1:]
    shapes = [(pages, page_len // 8, width), (pages, page_len // 4, width)]
    return pl.pallas_call(
        outgoing_kernel,
        grid_spec=pltpu.PrefetchScalarGridSpec(
            num_scalar_prefetch=4,
            grid=(1,),
            in_specs=[pl.BlockSpec(memory_space=pltpu.HBM)],
            out_specs=[pl.BlockSpec(x, lambda i, *_: (0, 0, 0)) for x in shapes],
            scratch_shapes=[pltpu.SemaphoreType.DMA((2 * pages,))],
        ),
        out_shape=[jax.ShapeDtypeStruct(x, pool.dtype) for x in shapes],
        compiler_params=params(60),
        cost_estimate=cost(3),
        name="outgoing",
    )(mine, twist, slots, counts, pool)


def chunk_step(block, base, first, qt, full, part, acc, stat):
    pages, rows, width = block.shape
    hd = width // 2
    lanes = qt.shape[1]
    keys = block[:, :, :hd].reshape(pages * rows, hd)
    values = block[:, :, hd:].reshape(pages * rows, hd)
    s = jnp.dot(keys, qt[...], preferred_element_type=F32)
    spot = lax.broadcasted_iota(jnp.int32, (rows, lanes), 0) + first
    old = stat[0:1, :]
    tops = jnp.full((8, lanes), NEG, F32)
    counts = []
    masked = []
    for j in range(pages):
        c = full[pl.ds(base + j, 1), :] + jnp.where(
            spot < part[pl.ds(base + j, 1), :], 1.0, 0.0
        )
        sj = jnp.where(c > 0.0, s[j * rows : (j + 1) * rows, :], NEG)
        tops = jnp.maximum(tops, jnp.max(sj.reshape(rows // 8, 8, lanes), axis=0))
        counts.append(c)
        masked.append(sj)
    top = jnp.maximum(old, jnp.max(tops, axis=0, keepdims=True))
    shrink = jnp.exp(old - top)
    sums = jnp.zeros((8, lanes), F32)
    probs = []
    for j in range(pages):
        p = jnp.exp(masked[j] - top) * counts[j]
        sums += jnp.sum(p.reshape(rows // 8, 8, lanes), axis=0)
        probs.append(p.astype(BF))
    p = jnp.concatenate(probs, axis=0)
    stat[0:1, :] = top
    stat[1:2, :] = stat[1:2, :] * shrink + jnp.sum(sums, axis=0, keepdims=True)
    acc[...] = acc[...] * shrink + lax.dot_general(
        values, p, (((0,), (0,)), ((), ())), preferred_element_type=F32
    )


def tables(first, page_len, tab_ref, len_ref, full, part):
    entries, lanes = full.shape
    page_id = lax.broadcasted_iota(jnp.int32, (entries, lanes), 0) + first
    whole = jnp.zeros((entries, lanes), F32)
    rest = jnp.zeros((entries, lanes), jnp.int32)
    for j in range(tab_ref.shape[0]):
        hit = page_id == tab_ref[j : j + 1, :]
        kept = len_ref[...] - j * page_len
        whole += jnp.where(hit & (kept >= page_len), 1.0, 0.0)
        rest += jnp.where(hit & (kept > 0) & (kept < page_len), kept, 0)
    full[...] = whole
    part[...] = rest


def resident_kernel(
    half_ref, qa_ref, qb_ref, entry_ref, tab_ref, len_ref, pool_ref,
    acc_ref, stat_ref, qt_ref, full, part, held, sems,
):
    i = pl.program_id(0)
    steps = sems.shape[0]
    slots, rows, width = held.shape
    pages = slots // steps
    hd = width // 2
    first = pl.multiple_of(half_ref[0] * rows, rows)

    def load(k):
        at = pl.ds(k * pages, pages)
        return pltpu.make_async_copy(
            pool_ref.at[at, pl.ds(first, rows), :], held.at[at], sems.at[k]
        )

    mine = qa_ref.shape[0]
    games = entry_ref.shape[0]

    @pl.when(i == 0)
    def _():
        for k in range(steps):
            load(k).start()
        q = jnp.concatenate([qa_ref[...], qb_ref[...]], axis=0)
        qt_ref[...] = q.T
        tables(0, 2 * rows, tab_ref, len_ref, full, part)
        s = jnp.dot(entry_ref[:, :hd], qt_ref[...], preferred_element_type=F32)
        game = lax.broadcasted_iota(jnp.int32, s.shape, 0)
        lane = lax.broadcasted_iota(jnp.int32, s.shape, 1)
        own = (lane < mine) & (lax.rem(lane, games) == game)
        p = jnp.where(own, 1.0, 0.0)
        stat_ref[...] = jnp.zeros(stat_ref.shape, F32)
        stat_ref[0:1, :] = jnp.max(jnp.where(own, s, NEG), axis=0, keepdims=True)
        stat_ref[1:2, :] = jnp.sum(p, axis=0, keepdims=True)
        acc_ref[...] = lax.dot_general(
            entry_ref[:, hd:], p.astype(BF), (((0,), (0,)), ((), ())), preferred_element_type=F32
        )

    load(i).wait()
    at = pl.ds(pl.multiple_of(i * pages, pages), pages)
    chunk_step(held.at[at], i * pages, first, qt_ref, full, part, acc_ref, stat_ref)


def resident(half, q_mine, q_peer, entry, table, lengths, pool):
    slots, page_len, width = pool.shape
    rows = page_len // 2
    mine, hd = q_mine.shape
    lanes = 2 * mine
    block = 16
    whole = lambda shape: pl.BlockSpec(shape, lambda i, *_: (0,) * len(shape))
    outs = [
        jax.ShapeDtypeStruct((hd, lanes), F32),
        jax.ShapeDtypeStruct((8, lanes), F32),
        jax.ShapeDtypeStruct((hd, lanes), BF),
    ]
    return pl.pallas_call(
        resident_kernel,
        grid_spec=pltpu.PrefetchScalarGridSpec(
            num_scalar_prefetch=1,
            grid=(slots // block,),
            in_specs=[
                whole(q_mine.shape),
                whole(q_peer.shape),
                whole(entry.shape),
                whole(table.shape),
                whole(lengths.shape),
                pl.BlockSpec(memory_space=pltpu.HBM),
            ],
            out_specs=[whole(o.shape) for o in outs],
            scratch_shapes=[
                pltpu.VMEM((slots, lanes), F32),
                pltpu.VMEM((slots, lanes), jnp.int32),
                pltpu.VMEM((slots, rows, width), BF),
                pltpu.SemaphoreType.DMA((slots // block,)),
            ],
        ),
        out_shape=outs,
        compiler_params=params(48),
        cost_estimate=cost(8),
        name="resident",
    )(half, q_mine, q_peer, entry, table, lengths, pool)


def moved_kernel(
    mine_ref, qt_ref, tab_ref, len_ref, acc_in, stat_in, a_ref, z_ref, b_ref,
    keep_ref, send_ref, acc, stat, full, part,
):
    i = pl.program_id(0)
    quarter = a_ref.shape[1]
    pages, rest, width = b_ref.shape
    hd = width // 2
    half = qt_ref.shape[1] // 2
    m = mine_ref[0]
    core = lax.rem(m, 2)
    state = (qt_ref, full, part, acc, stat)

    @pl.when(i == 0)
    def _():
        tables(full.shape[0], 8 * quarter, tab_ref, len_ref, full, part)
        acc[...] = acc_in[...]
        stat[...] = stat_in[...]
        chunk_step(a_ref, 0, m * quarter, *state)

    @pl.when(i == 1)
    def _():
        chunk_step(z_ref, 0, lax.rem(m + 2, 4) * quarter, *state)

    @pl.when(i >= 2)
    def _():
        chunk_step(b_ref, (i - 2) * pages, 4 * quarter + core * rest, *state)

    @pl.when(i == pl.num_programs(0) - 1)
    def _():
        for k, out in enumerate((keep_ref, send_ref)):
            out[:hd, :] = acc[:, k * half : (k + 1) * half]
            out[hd : hd + 8, :] = stat[:, k * half : (k + 1) * half]


def moved(mine, qt, table, lengths, acc, stat, got_a, got_z, got_b):
    slots, rest, width = got_b.shape
    hd, lanes = qt.shape
    block = slots // 2
    whole = lambda shape: pl.BlockSpec(shape, lambda i, *_: (0,) * len(shape))
    out = jax.ShapeDtypeStruct((hd + 8, lanes // 2), F32)
    return pl.pallas_call(
        moved_kernel,
        grid_spec=pltpu.PrefetchScalarGridSpec(
            num_scalar_prefetch=1,
            grid=(4,),
            in_specs=[
                whole(qt.shape),
                whole(table.shape),
                whole(lengths.shape),
                whole(acc.shape),
                whole(stat.shape),
                whole(got_a.shape),
                whole(got_z.shape),
                pl.BlockSpec((block, rest, width), lambda i, *_: (jnp.maximum(i - 2, 0), 0, 0)),
            ],
            out_specs=[whole(out.shape), whole(out.shape)],
            scratch_shapes=[
                pltpu.VMEM((hd, lanes), F32),
                pltpu.VMEM((8, lanes), F32),
                pltpu.VMEM((slots, lanes), F32),
                pltpu.VMEM((slots, lanes), jnp.int32),
            ],
        ),
        out_shape=[out, out],
        compiler_params=params(40),
        cost_estimate=cost(8),
        name="moved",
    )(mine, qt, table, lengths, acc, stat, got_a, got_z, got_b)


def project_kernel(mine_ref, a_ref, b_ref, w_ref, keep_ref, send_ref, scratch):
    hd = a_ref.shape[0] - 8
    ma, mb = a_ref[hd : hd + 1, :], b_ref[hd : hd + 1, :]
    top = jnp.maximum(ma, mb)
    wa, wb = jnp.exp(ma - top), jnp.exp(mb - top)
    den = a_ref[hd + 1 : hd + 2, :] * wa + b_ref[hd + 1 : hd + 2, :] * wb
    att = (a_ref[:hd, :] * wa + b_ref[:hd, :] * wb) / den
    att = att.T.astype(BF)
    games = scratch.shape[0]
    out = jnp.zeros(scratch.shape, F32)
    for h in range(att.shape[0] // games):
        out += jnp.dot(
            att[h * games : (h + 1) * games, :],
            w_ref[h * hd : (h + 1) * hd, :],
            preferred_element_type=F32,
        )
    scratch[...] = out
    rows = keep_ref.shape[1]
    m = mine_ref[0]
    core = lax.rem(m, 2)
    side = m // 2
    for ref, c in ((keep_ref, core), (send_ref, 1 - core)):
        for k, z in enumerate((side, 1 - side)):
            first = pl.multiple_of((z * 2 + c) * rows, rows)
            ref[k] = scratch[pl.ds(first, rows), :]


def project(mine, a, b, w, games):
    rows = games // 4
    whole = lambda shape: pl.BlockSpec(shape, lambda i, *_: (0,) * len(shape))
    out = jax.ShapeDtypeStruct((2, rows, w.shape[1]), F32)
    return pl.pallas_call(
        project_kernel,
        grid_spec=pltpu.PrefetchScalarGridSpec(
            num_scalar_prefetch=1,
            grid=(1,),
            in_specs=[whole(a.shape), whole(b.shape), whole(w.shape)],
            out_specs=[whole(out.shape), whole(out.shape)],
            scratch_shapes=[pltpu.VMEM((games, w.shape[1]), F32)],
        ),
        out_shape=[out, out],
        compiler_params=params(10),
        cost_estimate=cost(3),
        name="project",
    )(mine, a, b, w)


def norm_kernel(mine_ref, keep_ref, got_ref, side_ref, res_ref, gain_ref, copies_ref, stream_ref):
    stream = res_ref[...].astype(F32) + ((keep_ref[0] + got_ref[0]) + side_ref[...])
    scale = lax.rsqrt(jnp.mean(stream * stream, axis=-1, keepdims=True) + 1e-06)
    normed = (stream * scale * (1.0 + gain_ref[...])).astype(BF)
    stream_ref[...] = stream
    for k in range(copies_ref.shape[0]):
        copies_ref[k] = normed


def norm(mine, keep, got, side, residual, gain, peers):
    _, rows, d = keep.shape
    whole = lambda shape: pl.BlockSpec(shape, lambda i, *_: (0,) * len(shape))
    outs = [
        jax.ShapeDtypeStruct((peers, rows, d), BF),
        jax.ShapeDtypeStruct((rows, d), F32),
    ]
    return pl.pallas_call(
        norm_kernel,
        grid_spec=pltpu.PrefetchScalarGridSpec(
            num_scalar_prefetch=1,
            grid=(1,),
            in_specs=[
                pl.BlockSpec((1, rows, d), lambda i, *_: (0, 0, 0)),
                pl.BlockSpec((1, rows, d), lambda i, *_: (0, 0, 0)),
                whole(side.shape),
                pl.BlockSpec((rows, d), lambda i, m: (m[0], 0)),
                whole(gain.shape),
            ],
            out_specs=[whole(o.shape) for o in outs],
        ),
        out_shape=outs,
        compiler_params=params(6),
        cost_estimate=cost(2),
        name="norm",
    )(mine, keep, got, side, residual, gain)


def ffn_kernel(*refs):
    n = (len(refs) - 3) // 3
    x_ref = refs[0]
    w = [refs[1 + 3 * b : 4 + 3 * b] for b in range(n)]
    out_ref, hid = refs[1 + 3 * n :]
    unit = w[0][0].shape[1]
    for b, (g, u, _) in enumerate(w):
        both = jnp.dot(
            x_ref[...], jnp.concatenate([g[...], u[...]], axis=1), preferred_element_type=F32
        )
        hid[:, b * unit : (b + 1) * unit] = (
            jax.nn.gelu(both[:, :unit], approximate=True) * both[:, unit:]
        ).astype(BF)
    cols = 512

    @pl.loop(0, out_ref.shape[1] // cols)
    def _(k):
        at = pl.ds(pl.multiple_of(k * cols, cols), cols)
        down = jnp.concatenate([d[:, at] for _, _, d in w], axis=0)
        out_ref[:, at] = jnp.dot(hid[...], down, preferred_element_type=F32).astype(BF)


def ffn(x, weights):
    n = len(weights)
    rows, d = x.shape
    unit = weights[0][0].shape[1]
    vmem = pl.BlockSpec(memory_space=pltpu.VMEM)
    return pl.pallas_call(
        ffn_kernel,
        in_specs=[vmem] * (1 + 3 * n),
        out_specs=vmem,
        out_shape=jax.ShapeDtypeStruct((rows, d), BF),
        scratch_shapes=[pltpu.VMEM((rows, n * unit), BF)],
        compiler_params=params(24),
        cost_estimate=cost(8),
        name="ffn",
    )(x, *[a for block in weights for a in block])


def finish_kernel(parts_ref, stream_ref, out_ref):
    total = parts_ref[0].astype(F32)
    for k in range(1, parts_ref.shape[0]):
        total += parts_ref[k].astype(F32)
    out_ref[...] = (stream_ref[...] + total).astype(BF)


def finish(parts, stream):
    vmem = pl.BlockSpec(memory_space=pltpu.VMEM)
    return pl.pallas_call(
        finish_kernel,
        in_specs=[vmem, vmem],
        out_specs=vmem,
        out_shape=jax.ShapeDtypeStruct(stream.shape, BF),
        compiler_params=params(4),
        cost_estimate=cost(2),
        name="finish",
    )(parts, stream)


def assemble_kernel(mine_ref, *refs):
    out_ref = refs[6]
    m = mine_ref[0]
    core, side = lax.rem(m, 2), m // 2
    for c, (a, z, b) in ((core, refs[:3]), (1 - core, refs[3:6])):
        quarter, rest = a.shape[1], b.shape[1]
        for ref, first in (
            (a, (2 * side + c) * quarter),
            (z, (2 * (1 - side) + c) * quarter),
            (b, 4 * quarter + c * rest),
        ):
            rows = ref.shape[1]
            out_ref[:, pl.ds(pl.multiple_of(first, rows), rows), :] = ref[...]


def assemble(mine, parts):
    pages, quarter, width = parts[0].shape
    block = 8
    page_len = 8 * quarter
    return pl.pallas_call(
        assemble_kernel,
        grid_spec=pltpu.PrefetchScalarGridSpec(
            num_scalar_prefetch=1,
            grid=(pages // block,),
            in_specs=[
                pl.BlockSpec((block, p.shape[1], width), lambda i, *_: (i, 0, 0)) for p in parts
            ],
            out_specs=pl.BlockSpec((block, page_len, width), lambda i, *_: (i, 0, 0)),
        ),
        out_shape=jax.ShapeDtypeStruct((pages, page_len, width), parts[0].dtype),
        compiler_params=params(8),
        cost_estimate=cost(6),
        name="assemble",
    )(mine, *parts)


def step(
    page_pool, move_count, send_slots, page_table, history_len, queries, new_entry, residual,
    out_proj, ffn_gain, gate_proj, up_proj, down_proj,
):
    axes = ("dp", "mp")
    n_dp, n_mp = lax.axis_size("dp"), lax.axis_size("mp")
    devices = n_dp * n_mp
    games, heads, hd = queries.shape
    mine = lax.axis_index("mp").reshape(1)
    half = mine % 2
    swap = lambda bit: [(k, k ^ bit) for k in range(devices)]
    send = lambda a, pairs: lax.ppermute(a, axes, pairs)
    core, side, far = swap(1), swap(2), swap(6)
    every = range(devices)
    groups = [
        [k for k in every if k % 2 == c and ((k >> 1) ^ (k >> 2)) % 2 == w]
        for w in range(2)
        for c in range(2)
    ]
    planes = [[k for k in every if k % 8 == z] for z in range(8)]
    peers = len(planes[0])
    exchange = lambda a, who: lax.all_to_all(
        a, axes, 0, 0, tiled=True, axis_index_groups=who
    )

    twist = (mine // 2 + lax.axis_index("dp")) % 2
    out_a, out_b = outgoing_pages(mine, twist, send_slots, move_count.reshape(-1), page_pool)
    spread_out = lambda a: exchange(a.reshape(n_dp, -1, *a.shape[1:]), groups).reshape(a.shape)
    got_a = spread_out(out_a)
    got_b = spread_out(out_b)
    got_z = send(got_a, side)

    q_mine = (queries.transpose(1, 0, 2) * jnp.asarray(hd**-0.5, BF)).reshape(
        heads * games, hd
    )
    q_peer = send(q_mine, core)
    copies = 2 * heads
    table = jnp.tile(page_table.T, (1, copies))
    lengths = jnp.tile(history_len[None, :], (1, copies))

    weights = (gate_proj, up_proj, down_proj)
    each = lambda ws, pairs: tuple(send(a, pairs) for a in ws)
    side_gate, side_up = send(weights[0], side), send(weights[1], side)
    side_down = send(weights[2], side)
    w_side = (side_gate, side_up, side_down)
    w_core = each(weights, core)
    side_core_gate, side_core_up = send(side_gate, core), send(side_up, core)
    side_core_down = send(side_down, core)
    w_side_core = (side_core_gate, side_core_up, side_core_down)
    far_up, far_down, far_gate = (send(weights[k], far) for k in (1, 2, 0))
    w_far = (far_gate, far_up, far_down)
    diag_gate = send(w_side[0], far)
    diag_up = send(far_up, side)
    diag_down = send(far_down, side)
    w_diag = (diag_gate, diag_up, diag_down)
    w_far_core = each(w_far, core)
    w_diag_core = each(w_diag, core)
    blocks = [
        weights, w_core, w_side, w_side_core, w_far, w_far_core, w_diag, w_diag_core
    ]

    acc, stat, qt = resident(half, q_mine, q_peer, new_entry, table, lengths, page_pool)
    keep, give = moved(mine, qt, table, lengths, acc, stat, got_a, got_z, got_b)
    other = send(give, core)
    got_peer = each((got_a, got_z, got_b), core)
    hold, pass_on = project(mine, keep, other, out_proj, games)
    hold_got = send(pass_on, core)
    side_got = send(hold[1] + hold_got[1], side)
    arrived = assemble(mine, (got_a, got_z, got_b, *got_peer))

    spread, stream = norm(
        mine, hold, hold_got, side_got, residual, ffn_gain.reshape(1, -1), peers
    )
    rows, d = stream.shape
    x = exchange(spread, planes)
    parts = ffn(x.reshape(peers * rows, d), blocks)
    back = exchange(parts.reshape(peers, rows, d), planes)
    quarter = finish(back, stream)
    layer_out = lax.all_gather(quarter, "mp", axis=0, tiled=True)
    return arrived, layer_out


def solution(mesh):
    in_specs = (
        P("dp", None, None),
        P("dp", None),
        P("dp", None),
        P("dp", None),
        P("dp"),
        P("dp", "mp", None),
        P("dp", None),
        P("dp", None),
        P("mp", None),
        P(),
        P(None, ("dp", "mp")),
        P(None, ("dp", "mp")),
        P(("dp", "mp"), None),
    )
    out_specs = (P("dp", None, None), P("dp", None))
    return jax.shard_map(
        step, mesh=mesh, in_specs=in_specs, out_specs=out_specs, check_vma=False
    )
```

```python
import jax
import jax.numpy as jnp
from jax import lax
from jax.experimental import pallas as pl
from jax.experimental.pallas import tpu as pltpu
from jax.sharding import PartitionSpec as P


NEG = -1e30
BF = jnp.bfloat16
F32 = jnp.float32


def params(mib):
    return pltpu.CompilerParams(vmem_limit_bytes=mib * 1024 * 1024)


def cost(us):
    return pl.CostEstimate(flops=int(us * 4e8), bytes_accessed=int(us * 2e6), transcendentals=0)


def outgoing_kernel(
    mine_ref, twist_ref, slot_ref, count_ref, pool_ref, a_ref, b_ref, sems
):
    pages, quarter, _ = a_ref.shape
    rest = b_ref.shape[1]
    caps = pages // count_ref.shape[0]
    core = lax.rem(mine_ref[0], 2)
    low = pl.multiple_of(4 * quarter + core * rest, rest)

    def copies(i):
        page = slot_ref[i // caps, i % caps]
        side = lax.rem(twist_ref[0] + (i // caps) % 2, 2)
        first = pl.multiple_of((2 * side + core) * quarter, quarter)
        return (
            pltpu.make_async_copy(
                pool_ref.at[page, pl.ds(first, quarter), :], a_ref.at[i], sems.at[2 * i]
            ),
            pltpu.make_async_copy(
                pool_ref.at[page, pl.ds(low, rest), :], b_ref.at[i], sems.at[2 * i + 1]
            ),
        )

    pending = [copies(i) for i in range(pages)]
    for pair in pending:
        for c in pair:
            c.start()
    for i, pair in enumerate(pending):
        for c in pair:
            c.wait()

        @pl.when(i % caps >= count_ref[i // caps])
        def _():
            a_ref[i] = jnp.zeros(a_ref.shape[1:], a_ref.dtype)
            b_ref[i] = jnp.zeros(b_ref.shape[1:], b_ref.dtype)


def outgoing_pages(mine, twist, slots, counts, pool):
    pages = slots.size
    page_len, width = pool.shape[1:]
    shapes = [(pages, page_len // 8, width), (pages, page_len // 4, width)]
    return pl.pallas_call(
        outgoing_kernel,
        grid_spec=pltpu.PrefetchScalarGridSpec(
            num_scalar_prefetch=4,
            grid=(1,),
            in_specs=[pl.BlockSpec(memory_space=pltpu.HBM)],
            out_specs=[pl.BlockSpec(x, lambda i, *_: (0, 0, 0)) for x in shapes],
            scratch_shapes=[pltpu.SemaphoreType.DMA((2 * pages,))],
        ),
        out_shape=[jax.ShapeDtypeStruct(x, pool.dtype) for x in shapes],
        compiler_params=params(60),
        cost_estimate=cost(3),
        name="outgoing",
    )(mine, twist, slots, counts, pool)


def chunk_step(block, base, first, qt, full, part, acc, stat):
    pages, rows, width = block.shape
    hd = width // 2
    lanes = qt.shape[1]
    keys = block[:, :, :hd].reshape(pages * rows, hd)
    values = block[:, :, hd:].reshape(pages * rows, hd)
    s = jnp.dot(keys, qt[...], preferred_element_type=F32)
    spot = lax.broadcasted_iota(jnp.int32, (rows, lanes), 0) + first
    old = stat[0:1, :]
    tops = jnp.full((8, lanes), NEG, F32)
    counts = []
    masked = []
    for j in range(pages):
        c = full[pl.ds(base + j, 1), :] + jnp.where(
            spot < part[pl.ds(base + j, 1), :], 1.0, 0.0
        )
        sj = jnp.where(c > 0.0, s[j * rows : (j + 1) * rows, :], NEG)
        tops = jnp.maximum(tops, jnp.max(sj.reshape(rows // 8, 8, lanes), axis=0))
        counts.append(c)
        masked.append(sj)
    top = jnp.maximum(old, jnp.max(tops, axis=0, keepdims=True))
    shrink = jnp.exp(old - top)
    sums = jnp.zeros((8, lanes), F32)
    probs = []
    for j in range(pages):
        p = jnp.exp(masked[j] - top) * counts[j]
        sums += jnp.sum(p.reshape(rows // 8, 8, lanes), axis=0)
        probs.append(p.astype(BF))
    p = jnp.concatenate(probs, axis=0)
    stat[0:1, :] = top
    stat[1:2, :] = stat[1:2, :] * shrink + jnp.sum(sums, axis=0, keepdims=True)
    acc[...] = acc[...] * shrink + lax.dot_general(
        values, p, (((0,), (0,)), ((), ())), preferred_element_type=F32
    )


def tables(first, page_len, tab_ref, len_ref, full, part):
    entries, lanes = full.shape
    page_id = lax.broadcasted_iota(jnp.int32, (entries, lanes), 0) + first
    whole = jnp.zeros((entries, lanes), F32)
    rest = jnp.zeros((entries, lanes), jnp.int32)
    for j in range(tab_ref.shape[0]):
        hit = page_id == tab_ref[j : j + 1, :]
        kept = len_ref[...] - j * page_len
        whole += jnp.where(hit & (kept >= page_len), 1.0, 0.0)
        rest += jnp.where(hit & (kept > 0) & (kept < page_len), kept, 0)
    full[...] = whole
    part[...] = rest


def resident_kernel(
    half_ref, qa_ref, qb_ref, entry_ref, tab_ref, len_ref, pool_ref,
    acc_ref, stat_ref, qt_ref, full, part, held, sems,
):
    i = pl.program_id(0)
    steps = sems.shape[0]
    slots, rows, width = held.shape
    pages = slots // steps
    hd = width // 2
    first = pl.multiple_of(half_ref[0] * rows, rows)

    def load(k):
        at = pl.ds(k * pages, pages)
        return pltpu.make_async_copy(
            pool_ref.at[at, pl.ds(first, rows), :], held.at[at], sems.at[k]
        )

    mine = qa_ref.shape[0]
    games = entry_ref.shape[0]

    @pl.when(i == 0)
    def _():
        for k in range(steps):
            load(k).start()
        q = jnp.concatenate([qa_ref[...], qb_ref[...]], axis=0)
        qt_ref[...] = q.T
        tables(0, 2 * rows, tab_ref, len_ref, full, part)
        s = jnp.dot(entry_ref[:, :hd], qt_ref[...], preferred_element_type=F32)
        game = lax.broadcasted_iota(jnp.int32, s.shape, 0)
        lane = lax.broadcasted_iota(jnp.int32, s.shape, 1)
        own = (lane < mine) & (lax.rem(lane, games) == game)
        p = jnp.where(own, 1.0, 0.0)
        stat_ref[...] = jnp.zeros(stat_ref.shape, F32)
        stat_ref[0:1, :] = jnp.max(jnp.where(own, s, NEG), axis=0, keepdims=True)
        stat_ref[1:2, :] = jnp.sum(p, axis=0, keepdims=True)
        acc_ref[...] = lax.dot_general(
            entry_ref[:, hd:], p.astype(BF), (((0,), (0,)), ((), ())), preferred_element_type=F32
        )

    load(i).wait()
    at = pl.ds(pl.multiple_of(i * pages, pages), pages)
    chunk_step(held.at[at], i * pages, first, qt_ref, full, part, acc_ref, stat_ref)


def resident(half, q_mine, q_peer, entry, table, lengths, pool):
    slots, page_len, width = pool.shape
    rows = page_len // 2
    mine, hd = q_mine.shape
    lanes = 2 * mine
    block = 16
    whole = lambda shape: pl.BlockSpec(shape, lambda i, *_: (0,) * len(shape))
    outs = [
        jax.ShapeDtypeStruct((hd, lanes), F32),
        jax.ShapeDtypeStruct((8, lanes), F32),
        jax.ShapeDtypeStruct((hd, lanes), BF),
    ]
    return pl.pallas_call(
        resident_kernel,
        grid_spec=pltpu.PrefetchScalarGridSpec(
            num_scalar_prefetch=1,
            grid=(slots // block,),
            in_specs=[
                whole(q_mine.shape),
                whole(q_peer.shape),
                whole(entry.shape),
                whole(table.shape),
                whole(lengths.shape),
                pl.BlockSpec(memory_space=pltpu.HBM),
            ],
            out_specs=[whole(o.shape) for o in outs],
            scratch_shapes=[
                pltpu.VMEM((slots, lanes), F32),
                pltpu.VMEM((slots, lanes), jnp.int32),
                pltpu.VMEM((slots, rows, width), BF),
                pltpu.SemaphoreType.DMA((slots // block,)),
            ],
        ),
        out_shape=outs,
        compiler_params=params(48),
        cost_estimate=cost(8),
        name="resident",
    )(half, q_mine, q_peer, entry, table, lengths, pool)


def moved_kernel(
    mine_ref, qt_ref, tab_ref, len_ref, acc_in, stat_in, a_ref, z_ref, b_ref,
    keep_ref, send_ref, acc, stat, full, part,
):
    i = pl.program_id(0)
    quarter = a_ref.shape[1]
    pages, rest, width = b_ref.shape
    hd = width // 2
    half = qt_ref.shape[1] // 2
    m = mine_ref[0]
    core = lax.rem(m, 2)
    state = (qt_ref, full, part, acc, stat)

    @pl.when(i == 0)
    def _():
        tables(full.shape[0], 8 * quarter, tab_ref, len_ref, full, part)
        acc[...] = acc_in[...]
        stat[...] = stat_in[...]
        chunk_step(a_ref, 0, m * quarter, *state)

    @pl.when(i == 1)
    def _():
        chunk_step(z_ref, 0, lax.rem(m + 2, 4) * quarter, *state)

    @pl.when(i >= 2)
    def _():
        chunk_step(b_ref, (i - 2) * pages, 4 * quarter + core * rest, *state)

    @pl.when(i == pl.num_programs(0) - 1)
    def _():
        for k, out in enumerate((keep_ref, send_ref)):
            out[:hd, :] = acc[:, k * half : (k + 1) * half]
            out[hd : hd + 8, :] = stat[:, k * half : (k + 1) * half]


def moved(mine, qt, table, lengths, acc, stat, got_a, got_z, got_b):
    slots, rest, width = got_b.shape
    hd, lanes = qt.shape
    block = slots // 2
    whole = lambda shape: pl.BlockSpec(shape, lambda i, *_: (0,) * len(shape))
    out = jax.ShapeDtypeStruct((hd + 8, lanes // 2), F32)
    return pl.pallas_call(
        moved_kernel,
        grid_spec=pltpu.PrefetchScalarGridSpec(
            num_scalar_prefetch=1,
            grid=(4,),
            in_specs=[
                whole(qt.shape),
                whole(table.shape),
                whole(lengths.shape),
                whole(acc.shape),
                whole(stat.shape),
                whole(got_a.shape),
                whole(got_z.shape),
                pl.BlockSpec((block, rest, width), lambda i, *_: (jnp.maximum(i - 2, 0), 0, 0)),
            ],
            out_specs=[whole(out.shape), whole(out.shape)],
            scratch_shapes=[
                pltpu.VMEM((hd, lanes), F32),
                pltpu.VMEM((8, lanes), F32),
                pltpu.VMEM((slots, lanes), F32),
                pltpu.VMEM((slots, lanes), jnp.int32),
            ],
        ),
        out_shape=[out, out],
        compiler_params=params(40),
        cost_estimate=cost(8),
        name="moved",
    )(mine, qt, table, lengths, acc, stat, got_a, got_z, got_b)


def project_kernel(mine_ref, a_ref, b_ref, w_ref, keep_ref, send_ref, scratch):
    hd = a_ref.shape[0] - 8
    ma, mb = a_ref[hd : hd + 1, :], b_ref[hd : hd + 1, :]
    top = jnp.maximum(ma, mb)
    wa, wb = jnp.exp(ma - top), jnp.exp(mb - top)
    den = a_ref[hd + 1 : hd + 2, :] * wa + b_ref[hd + 1 : hd + 2, :] * wb
    att = (a_ref[:hd, :] * wa + b_ref[:hd, :] * wb) / den
    att = att.T.astype(BF)
    games = scratch.shape[0]
    out = jnp.zeros(scratch.shape, F32)
    for h in range(att.shape[0] // games):
        out += jnp.dot(
            att[h * games : (h + 1) * games, :],
            w_ref[h * hd : (h + 1) * hd, :],
            preferred_element_type=F32,
        )
    scratch[...] = out
    rows = keep_ref.shape[1]
    m = mine_ref[0]
    core = lax.rem(m, 2)
    side = m // 2
    for ref, c in ((keep_ref, core), (send_ref, 1 - core)):
        for k, z in enumerate((side, 1 - side)):
            first = pl.multiple_of((z * 2 + c) * rows, rows)
            ref[k] = scratch[pl.ds(first, rows), :]


def project(mine, a, b, w, games):
    rows = games // 4
    whole = lambda shape: pl.BlockSpec(shape, lambda i, *_: (0,) * len(shape))
    out = jax.ShapeDtypeStruct((2, rows, w.shape[1]), F32)
    return pl.pallas_call(
        project_kernel,
        grid_spec=pltpu.PrefetchScalarGridSpec(
            num_scalar_prefetch=1,
            grid=(1,),
            in_specs=[whole(a.shape), whole(b.shape), whole(w.shape)],
            out_specs=[whole(out.shape), whole(out.shape)],
            scratch_shapes=[pltpu.VMEM((games, w.shape[1]), F32)],
        ),
        out_shape=[out, out],
        compiler_params=params(10),
        cost_estimate=cost(3),
        name="project",
    )(mine, a, b, w)


def norm_kernel(mine_ref, keep_ref, got_ref, side_ref, res_ref, gain_ref, copies_ref, stream_ref):
    stream = res_ref[...].astype(F32) + ((keep_ref[0] + got_ref[0]) + side_ref[...])
    scale = lax.rsqrt(jnp.mean(stream * stream, axis=-1, keepdims=True) + 1e-06)
    normed = (stream * scale * (1.0 + gain_ref[...])).astype(BF)
    stream_ref[...] = stream
    for k in range(copies_ref.shape[0]):
        copies_ref[k] = normed


def norm(mine, keep, got, side, residual, gain, peers):
    _, rows, d = keep.shape
    whole = lambda shape: pl.BlockSpec(shape, lambda i, *_: (0,) * len(shape))
    outs = [
        jax.ShapeDtypeStruct((peers, rows, d), BF),
        jax.ShapeDtypeStruct((rows, d), F32),
    ]
    return pl.pallas_call(
        norm_kernel,
        grid_spec=pltpu.PrefetchScalarGridSpec(
            num_scalar_prefetch=1,
            grid=(1,),
            in_specs=[
                pl.BlockSpec((1, rows, d), lambda i, *_: (0, 0, 0)),
                pl.BlockSpec((1, rows, d), lambda i, *_: (0, 0, 0)),
                whole(side.shape),
                pl.BlockSpec((rows, d), lambda i, m: (m[0], 0)),
                whole(gain.shape),
            ],
            out_specs=[whole(o.shape) for o in outs],
        ),
        out_shape=outs,
        compiler_params=params(6),
        cost_estimate=cost(2),
        name="norm",
    )(mine, keep, got, side, residual, gain)


def ffn_kernel(*refs):
    n = (len(refs) - 3) // 3
    x_ref = refs[0]
    w = [refs[1 + 3 * b : 4 + 3 * b] for b in range(n)]
    out_ref, hid = refs[1 + 3 * n :]
    unit = w[0][0].shape[1]
    for b, (g, u, _) in enumerate(w):
        both = jnp.dot(
            x_ref[...], jnp.concatenate([g[...], u[...]], axis=1), preferred_element_type=F32
        )
        hid[:, b * unit : (b + 1) * unit] = (
            jax.nn.gelu(both[:, :unit], approximate=True) * both[:, unit:]
        ).astype(BF)
    cols = 512

    @pl.loop(0, out_ref.shape[1] // cols)
    def _(k):
        at = pl.ds(pl.multiple_of(k * cols, cols), cols)
        down = jnp.concatenate([d[:, at] for _, _, d in w], axis=0)
        out_ref[:, at] = jnp.dot(hid[...], down, preferred_element_type=F32).astype(BF)


def ffn(x, weights):
    n = len(weights)
    rows, d = x.shape
    unit = weights[0][0].shape[1]
    vmem = pl.BlockSpec(memory_space=pltpu.VMEM)
    return pl.pallas_call(
        ffn_kernel,
        in_specs=[vmem] * (1 + 3 * n),
        out_specs=vmem,
        out_shape=jax.ShapeDtypeStruct((rows, d), BF),
        scratch_shapes=[pltpu.VMEM((rows, n * unit), BF)],
        compiler_params=params(24),
        cost_estimate=cost(8),
        name="ffn",
    )(x, *[a for block in weights for a in block])


def finish_kernel(parts_ref, stream_ref, out_ref):
    total = parts_ref[0].astype(F32)
    for k in range(1, parts_ref.shape[0]):
        total += parts_ref[k].astype(F32)
    out_ref[...] = (stream_ref[...] + total).astype(BF)


def finish(parts, stream):
    vmem = pl.BlockSpec(memory_space=pltpu.VMEM)
    return pl.pallas_call(
        finish_kernel,
        in_specs=[vmem, vmem],
        out_specs=vmem,
        out_shape=jax.ShapeDtypeStruct(stream.shape, BF),
        compiler_params=params(4),
        cost_estimate=cost(2),
        name="finish",
    )(parts, stream)


def join_kernel(mine_ref, *refs):
    out_ref = refs[4]
    rows = refs[0].shape[0]
    m = mine_ref[0]
    core, side = lax.rem(m, 2), m // 2
    for k, ref in enumerate(refs[:4]):
        c = 1 - core if k % 2 else core
        z = 1 - side if k >= 2 else side
        first = pl.multiple_of((2 * z + c) * rows, rows)
        out_ref[pl.ds(first, rows), :] = ref[...]


def join(mine, parts):
    rows, d = parts[0].shape
    spec = pl.BlockSpec((rows, d), lambda i, *_: (0, 0))
    return pl.pallas_call(
        join_kernel,
        grid_spec=pltpu.PrefetchScalarGridSpec(
            num_scalar_prefetch=1,
            grid=(1,),
            in_specs=[spec] * 4,
            out_specs=pl.BlockSpec((4 * rows, d), lambda i, *_: (0, 0)),
        ),
        out_shape=jax.ShapeDtypeStruct((4 * rows, d), parts[0].dtype),
        compiler_params=params(4),
        cost_estimate=cost(1),
        name="join",
    )(mine, *parts)


def assemble_kernel(mine_ref, *refs):
    out_ref = refs[6]
    m = mine_ref[0]
    core, side = lax.rem(m, 2), m // 2
    for c, (a, z, b) in ((core, refs[:3]), (1 - core, refs[3:6])):
        quarter, rest = a.shape[1], b.shape[1]
        for ref, first in (
            (a, (2 * side + c) * quarter),
            (z, (2 * (1 - side) + c) * quarter),
            (b, 4 * quarter + c * rest),
        ):
            rows = ref.shape[1]
            out_ref[:, pl.ds(pl.multiple_of(first, rows), rows), :] = ref[...]


def assemble(mine, parts):
    pages, quarter, width = parts[0].shape
    block = 8
    page_len = 8 * quarter
    return pl.pallas_call(
        assemble_kernel,
        grid_spec=pltpu.PrefetchScalarGridSpec(
            num_scalar_prefetch=1,
            grid=(pages // block,),
            in_specs=[
                pl.BlockSpec((block, p.shape[1], width), lambda i, *_: (i, 0, 0)) for p in parts
            ],
            out_specs=pl.BlockSpec((block, page_len, width), lambda i, *_: (i, 0, 0)),
        ),
        out_shape=jax.ShapeDtypeStruct((pages, page_len, width), parts[0].dtype),
        compiler_params=params(8),
        cost_estimate=cost(6),
        name="assemble",
    )(mine, *parts)


def step(
    page_pool, move_count, send_slots, page_table, history_len, queries, new_entry, residual,
    out_proj, ffn_gain, gate_proj, up_proj, down_proj,
):
    axes = ("dp", "mp")
    n_dp, n_mp = lax.axis_size("dp"), lax.axis_size("mp")
    devices = n_dp * n_mp
    games, heads, hd = queries.shape
    mine = lax.axis_index("mp").reshape(1)
    half = mine % 2
    swap = lambda bit: [(k, k ^ bit) for k in range(devices)]
    send = lambda a, pairs: lax.ppermute(a, axes, pairs)
    core, side, far = swap(1), swap(2), swap(6)
    every = range(devices)
    groups = [
        [k for k in every if k % 2 == c and ((k >> 1) ^ (k >> 2)) % 2 == w]
        for w in range(2)
        for c in range(2)
    ]
    planes = [[k for k in every if k % 8 == z] for z in range(8)]
    peers = len(planes[0])
    exchange = lambda a, who: lax.all_to_all(
        a, axes, 0, 0, tiled=True, axis_index_groups=who
    )

    twist = (mine // 2 + lax.axis_index("dp")) % 2
    out_a, out_b = outgoing_pages(mine, twist, send_slots, move_count.reshape(-1), page_pool)
    spread_out = lambda a: exchange(a.reshape(n_dp, -1, *a.shape[1:]), groups).reshape(a.shape)
    got_a = spread_out(out_a)
    got_b = spread_out(out_b)
    got_z = send(got_a, side)

    q_mine = (queries.transpose(1, 0, 2) * jnp.asarray(hd**-0.5, BF)).reshape(
        heads * games, hd
    )
    q_peer = send(q_mine, core)
    copies = 2 * heads
    table = jnp.tile(page_table.T, (1, copies))
    lengths = jnp.tile(history_len[None, :], (1, copies))

    weights = (gate_proj, up_proj, down_proj)
    each = lambda ws, pairs: tuple(send(a, pairs) for a in ws)
    side_gate, side_up = send(weights[0], side), send(weights[1], side)
    side_down = send(weights[2], side)
    w_side = (side_gate, side_up, side_down)
    w_core = each(weights, core)
    side_core_gate, side_core_up = send(side_gate, core), send(side_up, core)
    side_core_down = send(side_down, core)
    w_side_core = (side_core_gate, side_core_up, side_core_down)
    far_up, far_down, far_gate = (send(weights[k], far) for k in (1, 2, 0))
    w_far = (far_gate, far_up, far_down)
    diag_gate = send(w_side[0], far)
    diag_up = send(far_up, side)
    diag_down = send(far_down, side)
    w_diag = (diag_gate, diag_up, diag_down)
    w_far_core = each(w_far, core)
    diag_core_up, diag_core_down = send(diag_up, core), send(diag_down, core)
    diag_core_gate = send(diag_gate, core)
    w_diag_core = (diag_core_gate, diag_core_up, diag_core_down)
    blocks = [
        weights, w_core, w_side, w_side_core, w_far, w_far_core, w_diag, w_diag_core
    ]

    acc, stat, qt = resident(half, q_mine, q_peer, new_entry, table, lengths, page_pool)
    keep, give = moved(mine, qt, table, lengths, acc, stat, got_a, got_z, got_b)
    other = send(give, core)
    got_peer = each((got_a, got_z, got_b), core)
    hold, pass_on = project(mine, keep, other, out_proj, games)
    hold_got = send(pass_on, core)
    side_got = send(hold[1] + hold_got[1], side)
    arrived = assemble(mine, (got_a, got_z, got_b, *got_peer))

    spread, stream = norm(
        mine, hold, hold_got, side_got, residual, ffn_gain.reshape(1, -1), peers
    )
    rows, d = stream.shape
    x = exchange(spread, planes)
    parts = ffn(x.reshape(peers * rows, d), blocks)
    back = exchange(parts.reshape(peers, rows, d), planes)
    quarter = finish(back, stream)
    other_side = send(quarter, side)
    other_core = send(quarter, core)
    other_both = send(other_side, core)
    layer_out = join(mine, (quarter, other_core, other_side, other_both))
    return arrived, layer_out


def solution(mesh):
    in_specs = (
        P("dp", None, None),
        P("dp", None),
        P("dp", None),
        P("dp", None),
        P("dp"),
        P("dp", "mp", None),
        P("dp", None),
        P("dp", None),
        P("mp", None),
        P(),
        P(None, ("dp", "mp")),
        P(None, ("dp", "mp")),
        P(("dp", "mp"), None),
    )
    out_specs = (P("dp", None, None), P("dp", None))
    return jax.shard_map(
        step, mesh=mesh, in_specs=in_specs, out_specs=out_specs, check_vma=False
    )
```

```python
import functools

import jax
import jax.numpy as jnp
from jax import lax
from jax.experimental import pallas as pl
from jax.experimental.pallas import tpu as pltpu
from jax.sharding import PartitionSpec as P


NEG = -1e30
BF = jnp.bfloat16
F32 = jnp.float32


def params(mib):
    return pltpu.CompilerParams(vmem_limit_bytes=mib * 1024 * 1024)


def cost(us):
    return pl.CostEstimate(flops=int(us * 4e8), bytes_accessed=int(us * 2e6), transcendentals=0)


def outgoing_kernel(by_quarter, mine_ref, twist_ref, slot_ref, count_ref, pool_ref, out_ref, sems):
    pages, rows, _ = out_ref.shape
    caps = pages // count_ref.shape[0]
    core = lax.rem(mine_ref[0], 2)

    def copy(i):
        page = slot_ref[i // caps, i % caps]
        if by_quarter:
            side = lax.rem(twist_ref[0] + (i // caps) % 2, 2)
            first = (2 * side + core) * rows
        else:
            first = (2 + core) * rows
        src = pool_ref.at[page, pl.ds(pl.multiple_of(first, rows), rows), :]
        return pltpu.make_async_copy(src, out_ref.at[i], sems.at[i])

    pending = [copy(i) for i in range(pages)]
    for c in pending:
        c.start()
    for i, c in enumerate(pending):
        c.wait()

        @pl.when(i % caps >= count_ref[i // caps])
        def _():
            out_ref[i] = jnp.zeros(out_ref.shape[1:], out_ref.dtype)


def outgoing_pages(by_quarter, mine, twist, slots, counts, pool):
    pages = slots.size
    page_len, width = pool.shape[1:]
    shape = (pages, page_len // (8 if by_quarter else 4), width)
    return pl.pallas_call(
        functools.partial(outgoing_kernel, by_quarter),
        grid_spec=pltpu.PrefetchScalarGridSpec(
            num_scalar_prefetch=4,
            grid=(1,),
            in_specs=[pl.BlockSpec(memory_space=pltpu.HBM)],
            out_specs=pl.BlockSpec(shape, lambda i, *_: (0, 0, 0)),
            scratch_shapes=[pltpu.SemaphoreType.DMA((pages,))],
        ),
        out_shape=jax.ShapeDtypeStruct(shape, pool.dtype),
        compiler_params=params(60),
        cost_estimate=cost(3),
        name="outgoing",
    )(mine, twist, slots, counts, pool)


def chunk_step(block, base, first, qt, full, part, acc, stat):
    pages, rows, width = block.shape
    hd = width // 2
    lanes = qt.shape[1]
    keys = block[:, :, :hd].reshape(pages * rows, hd)
    values = block[:, :, hd:].reshape(pages * rows, hd)
    s = jnp.dot(keys, qt[...], preferred_element_type=F32)
    spot = lax.broadcasted_iota(jnp.int32, (rows, lanes), 0) + first
    old = stat[0:1, :]
    tops = jnp.full((8, lanes), NEG, F32)
    counts = []
    masked = []
    for j in range(pages):
        c = full[pl.ds(base + j, 1), :] + jnp.where(
            spot < part[pl.ds(base + j, 1), :], 1.0, 0.0
        )
        sj = jnp.where(c > 0.0, s[j * rows : (j + 1) * rows, :], NEG)
        tops = jnp.maximum(tops, jnp.max(sj.reshape(rows // 8, 8, lanes), axis=0))
        counts.append(c)
        masked.append(sj)
    top = jnp.maximum(old, jnp.max(tops, axis=0, keepdims=True))
    shrink = jnp.exp(old - top)
    sums = jnp.zeros((8, lanes), F32)
    probs = []
    for j in range(pages):
        p = jnp.exp(masked[j] - top) * counts[j]
        sums += jnp.sum(p.reshape(rows // 8, 8, lanes), axis=0)
        probs.append(p.astype(BF))
    p = jnp.concatenate(probs, axis=0)
    stat[0:1, :] = top
    stat[1:2, :] = stat[1:2, :] * shrink + jnp.sum(sums, axis=0, keepdims=True)
    acc[...] = acc[...] * shrink + lax.dot_general(
        values, p, (((0,), (0,)), ((), ())), preferred_element_type=F32
    )


def tables(first, page_len, tab_ref, len_ref, full, part):
    entries, lanes = full.shape
    page_id = lax.broadcasted_iota(jnp.int32, (entries, lanes), 0) + first
    whole = jnp.zeros((entries, lanes), F32)
    rest = jnp.zeros((entries, lanes), jnp.int32)
    for j in range(tab_ref.shape[0]):
        hit = page_id == tab_ref[j : j + 1, :]
        kept = len_ref[...] - j * page_len
        whole += jnp.where(hit & (kept >= page_len), 1.0, 0.0)
        rest += jnp.where(hit & (kept > 0) & (kept < page_len), kept, 0)
    full[...] = whole
    part[...] = rest


def resident_kernel(
    half_ref, qa_ref, qb_ref, entry_ref, tab_ref, len_ref, pool_ref,
    acc_ref, stat_ref, qt_ref, full, part, held, sems,
):
    i = pl.program_id(0)
    steps = sems.shape[0]
    slots, rows, width = held.shape
    pages = slots // steps
    hd = width // 2
    first = pl.multiple_of(half_ref[0] * rows, rows)

    def load(k):
        at = pl.ds(k * pages, pages)
        return pltpu.make_async_copy(
            pool_ref.at[at, pl.ds(first, rows), :], held.at[at], sems.at[k]
        )

    mine = qa_ref.shape[0]
    games = entry_ref.shape[0]

    @pl.when(i == 0)
    def _():
        for k in range(steps):
            load(k).start()
        q = jnp.concatenate([qa_ref[...], qb_ref[...]], axis=0)
        qt_ref[...] = q.T
        tables(0, 2 * rows, tab_ref, len_ref, full, part)
        s = jnp.dot(entry_ref[:, :hd], qt_ref[...], preferred_element_type=F32)
        game = lax.broadcasted_iota(jnp.int32, s.shape, 0)
        lane = lax.broadcasted_iota(jnp.int32, s.shape, 1)
        own = (lane < mine) & (lax.rem(lane, games) == game)
        p = jnp.where(own, 1.0, 0.0)
        stat_ref[...] = jnp.zeros(stat_ref.shape, F32)
        stat_ref[0:1, :] = jnp.max(jnp.where(own, s, NEG), axis=0, keepdims=True)
        stat_ref[1:2, :] = jnp.sum(p, axis=0, keepdims=True)
        acc_ref[...] = lax.dot_general(
            entry_ref[:, hd:], p.astype(BF), (((0,), (0,)), ((), ())), preferred_element_type=F32
        )

    load(i).wait()
    at = pl.ds(pl.multiple_of(i * pages, pages), pages)
    chunk_step(held.at[at], i * pages, first, qt_ref, full, part, acc_ref, stat_ref)


def resident(half, q_mine, q_peer, entry, table, lengths, pool):
    slots, page_len, width = pool.shape
    rows = page_len // 2
    mine, hd = q_mine.shape
    lanes = 2 * mine
    block = 16
    whole = lambda shape: pl.BlockSpec(shape, lambda i, *_: (0,) * len(shape))
    outs = [
        jax.ShapeDtypeStruct((hd, lanes), F32),
        jax.ShapeDtypeStruct((8, lanes), F32),
        jax.ShapeDtypeStruct((hd, lanes), BF),
    ]
    return pl.pallas_call(
        resident_kernel,
        grid_spec=pltpu.PrefetchScalarGridSpec(
            num_scalar_prefetch=1,
            grid=(slots // block,),
            in_specs=[
                whole(q_mine.shape),
                whole(q_peer.shape),
                whole(entry.shape),
                whole(table.shape),
                whole(lengths.shape),
                pl.BlockSpec(memory_space=pltpu.HBM),
            ],
            out_specs=[whole(o.shape) for o in outs],
            scratch_shapes=[
                pltpu.VMEM((slots, lanes), F32),
                pltpu.VMEM((slots, lanes), jnp.int32),
                pltpu.VMEM((slots, rows, width), BF),
                pltpu.SemaphoreType.DMA((slots // block,)),
            ],
        ),
        out_shape=outs,
        compiler_params=params(48),
        cost_estimate=cost(8),
        name="resident",
    )(half, q_mine, q_peer, entry, table, lengths, pool)


def moved_kernel(
    mine_ref, qt_ref, tab_ref, len_ref, acc_in, stat_in, a_ref, z_ref, b_ref,
    keep_ref, send_ref, acc, stat, full, part,
):
    i = pl.program_id(0)
    quarter = a_ref.shape[1]
    pages, rest, width = b_ref.shape
    hd = width // 2
    half = qt_ref.shape[1] // 2
    m = mine_ref[0]
    core = lax.rem(m, 2)
    state = (qt_ref, full, part, acc, stat)

    @pl.when(i == 0)
    def _():
        tables(full.shape[0], 8 * quarter, tab_ref, len_ref, full, part)
        acc[...] = acc_in[...]
        stat[...] = stat_in[...]
        chunk_step(a_ref, 0, m * quarter, *state)

    @pl.when(i == 1)
    def _():
        chunk_step(z_ref, 0, lax.rem(m + 2, 4) * quarter, *state)

    @pl.when(i >= 2)
    def _():
        chunk_step(b_ref, (i - 2) * pages, 4 * quarter + core * rest, *state)

    @pl.when(i == pl.num_programs(0) - 1)
    def _():
        for k, out in enumerate((keep_ref, send_ref)):
            out[:hd, :] = acc[:, k * half : (k + 1) * half]
            out[hd : hd + 8, :] = stat[:, k * half : (k + 1) * half]


def moved(mine, qt, table, lengths, acc, stat, got_a, got_z, got_b):
    slots, rest, width = got_b.shape
    hd, lanes = qt.shape
    block = slots // 2
    whole = lambda shape: pl.BlockSpec(shape, lambda i, *_: (0,) * len(shape))
    out = jax.ShapeDtypeStruct((hd + 8, lanes // 2), F32)
    return pl.pallas_call(
        moved_kernel,
        grid_spec=pltpu.PrefetchScalarGridSpec(
            num_scalar_prefetch=1,
            grid=(4,),
            in_specs=[
                whole(qt.shape),
                whole(table.shape),
                whole(lengths.shape),
                whole(acc.shape),
                whole(stat.shape),
                whole(got_a.shape),
                whole(got_z.shape),
                pl.BlockSpec((block, rest, width), lambda i, *_: (jnp.maximum(i - 2, 0), 0, 0)),
            ],
            out_specs=[whole(out.shape), whole(out.shape)],
            scratch_shapes=[
                pltpu.VMEM((hd, lanes), F32),
                pltpu.VMEM((8, lanes), F32),
                pltpu.VMEM((slots, lanes), F32),
                pltpu.VMEM((slots, lanes), jnp.int32),
            ],
        ),
        out_shape=[out, out],
        compiler_params=params(40),
        cost_estimate=cost(8),
        name="moved",
    )(mine, qt, table, lengths, acc, stat, got_a, got_z, got_b)


def project_kernel(mine_ref, a_ref, b_ref, w_ref, keep_ref, send_ref, scratch):
    hd = a_ref.shape[0] - 8
    ma, mb = a_ref[hd : hd + 1, :], b_ref[hd : hd + 1, :]
    top = jnp.maximum(ma, mb)
    wa, wb = jnp.exp(ma - top), jnp.exp(mb - top)
    den = a_ref[hd + 1 : hd + 2, :] * wa + b_ref[hd + 1 : hd + 2, :] * wb
    att = (a_ref[:hd, :] * wa + b_ref[:hd, :] * wb) / den
    att = att.T.astype(BF)
    games = scratch.shape[0]
    out = jnp.zeros(scratch.shape, F32)
    for h in range(att.shape[0] // games):
        out += jnp.dot(
            att[h * games : (h + 1) * games, :],
            w_ref[h * hd : (h + 1) * hd, :],
            preferred_element_type=F32,
        )
    scratch[...] = out
    rows = keep_ref.shape[1]
    m = mine_ref[0]
    core = lax.rem(m, 2)
    side = m // 2
    for ref, c in ((keep_ref, core), (send_ref, 1 - core)):
        for k, z in enumerate((side, 1 - side)):
            first = pl.multiple_of((z * 2 + c) * rows, rows)
            ref[k] = scratch[pl.ds(first, rows), :]


def project(mine, a, b, w, games):
    rows = games // 4
    whole = lambda shape: pl.BlockSpec(shape, lambda i, *_: (0,) * len(shape))
    out = jax.ShapeDtypeStruct((2, rows, w.shape[1]), F32)
    return pl.pallas_call(
        project_kernel,
        grid_spec=pltpu.PrefetchScalarGridSpec(
            num_scalar_prefetch=1,
            grid=(1,),
            in_specs=[whole(a.shape), whole(b.shape), whole(w.shape)],
            out_specs=[whole(out.shape), whole(out.shape)],
            scratch_shapes=[pltpu.VMEM((games, w.shape[1]), F32)],
        ),
        out_shape=[out, out],
        compiler_params=params(10),
        cost_estimate=cost(3),
        name="project",
    )(mine, a, b, w)


def norm_kernel(mine_ref, keep_ref, got_ref, side_ref, res_ref, gain_ref, copies_ref, stream_ref):
    stream = res_ref[...].astype(F32) + ((keep_ref[0] + got_ref[0]) + side_ref[...])
    scale = lax.rsqrt(jnp.mean(stream * stream, axis=-1, keepdims=True) + 1e-06)
    normed = (stream * scale * (1.0 + gain_ref[...])).astype(BF)
    stream_ref[...] = stream
    for k in range(copies_ref.shape[0]):
        copies_ref[k] = normed


def norm(mine, keep, got, side, residual, gain, peers):
    _, rows, d = keep.shape
    whole = lambda shape: pl.BlockSpec(shape, lambda i, *_: (0,) * len(shape))
    outs = [
        jax.ShapeDtypeStruct((peers, rows, d), BF),
        jax.ShapeDtypeStruct((rows, d), F32),
    ]
    return pl.pallas_call(
        norm_kernel,
        grid_spec=pltpu.PrefetchScalarGridSpec(
            num_scalar_prefetch=1,
            grid=(1,),
            in_specs=[
                pl.BlockSpec((1, rows, d), lambda i, *_: (0, 0, 0)),
                pl.BlockSpec((1, rows, d), lambda i, *_: (0, 0, 0)),
                whole(side.shape),
                pl.BlockSpec((rows, d), lambda i, m: (m[0], 0)),
                whole(gain.shape),
            ],
            out_specs=[whole(o.shape) for o in outs],
        ),
        out_shape=outs,
        compiler_params=params(6),
        cost_estimate=cost(2),
        name="norm",
    )(mine, keep, got, side, residual, gain)


def ffn_kernel(*refs):
    n = (len(refs) - 3) // 3
    x_ref = refs[0]
    w = [refs[1 + 3 * b : 4 + 3 * b] for b in range(n)]
    out_ref, hid = refs[1 + 3 * n :]
    unit = w[0][0].shape[1]
    for b, (g, u, _) in enumerate(w):
        both = jnp.dot(
            x_ref[...], jnp.concatenate([g[...], u[...]], axis=1), preferred_element_type=F32
        )
        hid[:, b * unit : (b + 1) * unit] = (
            jax.nn.gelu(both[:, :unit], approximate=True) * both[:, unit:]
        ).astype(BF)
    cols = 512

    @pl.loop(0, out_ref.shape[1] // cols)
    def _(k):
        at = pl.ds(pl.multiple_of(k * cols, cols), cols)
        down = jnp.concatenate([d[:, at] for _, _, d in w], axis=0)
        out_ref[:, at] = jnp.dot(hid[...], down, preferred_element_type=F32).astype(BF)


def ffn(x, weights):
    n = len(weights)
    rows, d = x.shape
    unit = weights[0][0].shape[1]
    vmem = pl.BlockSpec(memory_space=pltpu.VMEM)
    return pl.pallas_call(
        ffn_kernel,
        in_specs=[vmem] * (1 + 3 * n),
        out_specs=vmem,
        out_shape=jax.ShapeDtypeStruct((rows, d), BF),
        scratch_shapes=[pltpu.VMEM((rows, n * unit), BF)],
        compiler_params=params(24),
        cost_estimate=cost(8),
        name="ffn",
    )(x, *[a for block in weights for a in block])


def finish_kernel(parts_ref, stream_ref, out_ref):
    total = parts_ref[0].astype(F32)
    for k in range(1, parts_ref.shape[0]):
        total += parts_ref[k].astype(F32)
    out_ref[...] = (stream_ref[...] + total).astype(BF)


def finish(parts, stream):
    vmem = pl.BlockSpec(memory_space=pltpu.VMEM)
    return pl.pallas_call(
        finish_kernel,
        in_specs=[vmem, vmem],
        out_specs=vmem,
        out_shape=jax.ShapeDtypeStruct(stream.shape, BF),
        compiler_params=params(4),
        cost_estimate=cost(2),
        name="finish",
    )(parts, stream)


def join_kernel(mine_ref, *refs):
    out_ref = refs[4]
    rows = refs[0].shape[0]
    m = mine_ref[0]
    core, side = lax.rem(m, 2), m // 2
    for k, ref in enumerate(refs[:4]):
        c = 1 - core if k % 2 else core
        z = 1 - side if k >= 2 else side
        first = pl.multiple_of((2 * z + c) * rows, rows)
        out_ref[pl.ds(first, rows), :] = ref[...]


def join(mine, parts):
    rows, d = parts[0].shape
    spec = pl.BlockSpec((rows, d), lambda i, *_: (0, 0))
    return pl.pallas_call(
        join_kernel,
        grid_spec=pltpu.PrefetchScalarGridSpec(
            num_scalar_prefetch=1,
            grid=(1,),
            in_specs=[spec] * 4,
            out_specs=pl.BlockSpec((4 * rows, d), lambda i, *_: (0, 0)),
        ),
        out_shape=jax.ShapeDtypeStruct((4 * rows, d), parts[0].dtype),
        compiler_params=params(4),
        cost_estimate=cost(1),
        name="join",
    )(mine, *parts)


def assemble_kernel(mine_ref, *refs):
    out_ref = refs[6]
    m = mine_ref[0]
    core, side = lax.rem(m, 2), m // 2
    for c, (a, z, b) in ((core, refs[:3]), (1 - core, refs[3:6])):
        quarter, rest = a.shape[1], b.shape[1]
        for ref, first in (
            (a, (2 * side + c) * quarter),
            (z, (2 * (1 - side) + c) * quarter),
            (b, 4 * quarter + c * rest),
        ):
            rows = ref.shape[1]
            out_ref[:, pl.ds(pl.multiple_of(first, rows), rows), :] = ref[...]


def assemble(mine, parts):
    pages, quarter, width = parts[0].shape
    block = 8
    page_len = 8 * quarter
    return pl.pallas_call(
        assemble_kernel,
        grid_spec=pltpu.PrefetchScalarGridSpec(
            num_scalar_prefetch=1,
            grid=(pages // block,),
            in_specs=[
                pl.BlockSpec((block, p.shape[1], width), lambda i, *_: (i, 0, 0)) for p in parts
            ],
            out_specs=pl.BlockSpec((block, page_len, width), lambda i, *_: (i, 0, 0)),
        ),
        out_shape=jax.ShapeDtypeStruct((pages, page_len, width), parts[0].dtype),
        compiler_params=params(8),
        cost_estimate=cost(6),
        name="assemble",
    )(mine, *parts)


def step(
    page_pool, move_count, send_slots, page_table, history_len, queries, new_entry, residual,
    out_proj, ffn_gain, gate_proj, up_proj, down_proj,
):
    axes = ("dp", "mp")
    n_dp, n_mp = lax.axis_size("dp"), lax.axis_size("mp")
    devices = n_dp * n_mp
    games, heads, hd = queries.shape
    mine = lax.axis_index("mp").reshape(1)
    half = mine % 2
    swap = lambda bit: [(k, k ^ bit) for k in range(devices)]
    send = lambda a, pairs: lax.ppermute(a, axes, pairs)
    core, side, far = swap(1), swap(2), swap(6)
    every = range(devices)
    groups = [
        [k for k in every if k % 2 == c and ((k >> 1) ^ (k >> 2)) % 2 == w]
        for w in range(2)
        for c in range(2)
    ]
    planes = [[k for k in every if k % 8 == z] for z in range(8)]
    peers = len(planes[0])
    exchange = lambda a, who: lax.all_to_all(
        a, axes, 0, 0, tiled=True, axis_index_groups=who
    )

    twist = (mine // 2 + lax.axis_index("dp")) % 2
    plan = (mine, twist, send_slots, move_count.reshape(-1), page_pool)
    out_a = outgoing_pages(True, *plan)
    out_b = outgoing_pages(False, *plan)
    spread_out = lambda a: exchange(a.reshape(n_dp, -1, *a.shape[1:]), groups).reshape(a.shape)
    got_a = spread_out(out_a)
    got_b = spread_out(out_b)
    got_z = send(got_a, side)

    q_mine = (queries.transpose(1, 0, 2) * jnp.asarray(hd**-0.5, BF)).reshape(
        heads * games, hd
    )
    q_peer = send(q_mine, core)
    copies = 2 * heads
    table = jnp.tile(page_table.T, (1, copies))
    lengths = jnp.tile(history_len[None, :], (1, copies))

    weights = (gate_proj, up_proj, down_proj)
    each = lambda ws, pairs: tuple(send(a, pairs) for a in ws)
    side_gate, side_up = send(weights[0], side), send(weights[1], side)
    side_down = send(weights[2], side)
    w_side = (side_gate, side_up, side_down)
    w_core = each(weights, core)
    side_core_gate, side_core_up = send(side_gate, core), send(side_up, core)
    side_core_down = send(side_down, core)
    w_side_core = (side_core_gate, side_core_up, side_core_down)
    far_up = send(weights[1], far)
    far_down, far_gate = send(weights[2], far), send(weights[0], far)
    w_far = (far_gate, far_up, far_down)
    diag_gate = send(w_side[0], far)
    diag_up = send(far_up, side)
    diag_down = send(far_down, side)
    w_diag = (diag_gate, diag_up, diag_down)
    w_far_core = each(w_far, core)
    diag_core_up, diag_core_down = send(diag_up, core), send(diag_down, core)
    diag_core_gate = send(diag_gate, core)
    w_diag_core = (diag_core_gate, diag_core_up, diag_core_down)
    blocks = [
        weights, w_core, w_side, w_side_core, w_far, w_far_core, w_diag, w_diag_core
    ]

    acc, stat, qt = resident(half, q_mine, q_peer, new_entry, table, lengths, page_pool)
    keep, give = moved(mine, qt, table, lengths, acc, stat, got_a, got_z, got_b)
    other = send(give, core)
    got_peer = each((got_a, got_z, got_b), core)
    hold, pass_on = project(mine, keep, other, out_proj, games)
    hold_got = send(pass_on, core)
    side_got = send(hold[1] + hold_got[1], side)
    arrived = assemble(mine, (got_a, got_z, got_b, *got_peer))

    spread, stream = norm(
        mine, hold, hold_got, side_got, residual, ffn_gain.reshape(1, -1), peers
    )
    rows, d = stream.shape
    x = exchange(spread, planes)
    parts = ffn(x.reshape(peers * rows, d), blocks)
    back = exchange(parts.reshape(peers, rows, d), planes)
    quarter = finish(back, stream)
    other_side = send(quarter, side)
    other_core = send(quarter, core)
    other_both = send(other_side, core)
    layer_out = join(mine, (quarter, other_core, other_side, other_both))
    return arrived, layer_out


def solution(mesh):
    in_specs = (
        P("dp", None, None),
        P("dp", None),
        P("dp", None),
        P("dp", None),
        P("dp"),
        P("dp", "mp", None),
        P("dp", None),
        P("dp", None),
        P("mp", None),
        P(),
        P(None, ("dp", "mp")),
        P(None, ("dp", "mp")),
        P(("dp", "mp"), None),
    )
    out_specs = (P("dp", None, None), P("dp", None))
    return jax.shard_map(
        step, mesh=mesh, in_specs=in_specs, out_specs=out_specs, check_vma=False
    )
```
